32 devices in a mesh: fsdp: 32 (over z, y, x, core).
Axes of the slice: x: 2, y: 2, z: 4, core: 2. Of those that a mesh axis runs over, the one named last changes fastest.
Arguments:
- layer_input: bfloat16 [4096, 1536], P('fsdp'), may hold values from -6 to 6
- out_cotangent: bfloat16 [4096, 1536], P('fsdp'), may hold values from -6 to 6
- lengths: int32 [32, 1], P('fsdp'), may hold values from 0 to 128, as said below
- norm_attn: bfloat16 [1536], P('fsdp'), may hold values from 0.5 to 1.5
- w_query: bfloat16 [1536, 1536], P('fsdp'), may hold values from -2 to 2
- w_key: bfloat16 [1536, 768], P('fsdp'), may hold values from -2 to 2
- w_value: bfloat16 [1536, 768], P('fsdp'), may hold values from -0.15625 to 0.15625
- w_out: bfloat16 [1536, 1536], P('fsdp'), may hold values from -1.25 to 1.25
- norm_mlp: bfloat16 [1536], P('fsdp'), may hold values from 0.5 to 1.5
- w_gate: bfloat16 [1536, 4096], P('fsdp'), may hold values from -0.15625 to 0.15625
- w_up: bfloat16 [1536, 4096], P('fsdp'), may hold values from -0.15625 to 0.15625
- w_down: bfloat16 [4096, 1536], P('fsdp'), may hold values from -0.1875 to 0.1875
Outputs:
- layer_output: bfloat16 [4096, 1536], P('fsdp')
- grad_input: float32 [4096, 1536], P('fsdp')
- grad_norm_attn: float32 [1536], P('fsdp')
- grad_w_query: float32 [1536, 1536], P('fsdp')
- grad_w_key: float32 [1536, 768], P('fsdp')
- grad_w_value: float32 [1536, 768], P('fsdp')
- grad_w_out: float32 [1536, 1536], P('fsdp')
- grad_norm_mlp: float32 [1536], P('fsdp')
- grad_w_gate: float32 [1536, 4096], P('fsdp')
- grad_w_up: float32 [1536, 4096], P('fsdp')
- grad_w_down: float32 [4096, 1536], P('fsdp')
The draws below stay inside these ranges and needn't reach their ends.
Inputs may be any that keep to these rules, and one draw needn't show every extreme that they name: Row d lists the lengths of device d's sequences in slot order; every row has a first sequence, zeros come only after all sequences, and each sequence takes whole blocks of 128 slots, at most 1 block a row. Some row holds a single sequence of length 128.
All inputs are finite; a program needn't handle non-finite values.
Results may differ from the reference program's by a relative error of at most 0.014.
The reference program's roundings to bfloat16 on the way count: a program that leaves them out, or rounds other values in their place, can miss the bound.
Values may be sent and summed in bfloat16 or wider, within the bound.
A program may use at most 320 MiB of HBM per device.

```python
import math
import jax
import jax.numpy as jnp
from jax import lax

D = 1536
HEADS = 16
KV_HEADS = 8
HEAD = 96
FF = 4096
BLOCK = 128
BLOCKS_DEV = 1
TOKENS = 4096
KVD = 768
N_FSDP = 32


def attention_pair(key):
    query_base = jax.random.normal(jax.random.fold_in(key, 11), (D, D), jnp.float32) * D ** (-0.5)
    key_noise = jax.random.normal(jax.random.fold_in(key, 12), (D, KV_HEADS * HEAD), jnp.float32) * D ** (-0.5)
    key_weight = key_noise
    return (jnp.clip(query_base, -2.0, 2.0), jnp.clip(key_weight, -2.0, 2.0))


def draw_w_query(key, part):
    return attention_pair(key)[0].astype(jnp.bfloat16)


def draw_w_key(key, part):
    return attention_pair(key)[1].astype(jnp.bfloat16)


def draw_lengths(key, part):
    row_count = N_FSDP
    blocks = BLOCKS_DEV
    used_blocks = jax.random.randint(jax.random.fold_in(key, 1), (row_count,), (blocks + 1) // 2, blocks + 1)
    cut_bits = jax.random.randint(jax.random.fold_in(key, 2), (row_count, blocks), 0, 2)
    full_row = jax.random.randint(jax.random.fold_in(key, 3), (), 0, row_count)
    is_full = jnp.arange(row_count) == full_row
    used_blocks = jnp.where(is_full, blocks, used_blocks)
    block_index = jnp.arange(blocks)
    new_start = (block_index[None, :] == 0) | (cut_bits == 1) & (block_index[None, :] < used_blocks[:, None]) & jnp.logical_not(is_full)[:, None]
    sequence_of = jnp.cumsum(new_start.astype(jnp.int32), axis=1) - 1
    in_use = block_index[None, :] < used_blocks[:, None]
    block_counts = jnp.sum(((sequence_of[:, :, None] == block_index[None, None, :]) & in_use[:, :, None]).astype(jnp.int32), axis=1)
    last_fill = jax.random.randint(jax.random.fold_in(key, 4), (row_count, blocks), 1, BLOCK + 1)
    last_fill = jnp.where(is_full[:, None], BLOCK, last_fill)
    return jnp.where(block_counts > 0, (block_counts - 1) * BLOCK + last_fill, 0).astype(jnp.int32)


def block_levels(own_key, shape, cuts, least, largest):
    def one(dim, shards_of):
        heights = jax.random.uniform(jax.random.fold_in(jax.random.fold_in(own_key, 6), dim), (shards_of,), jnp.float32, least / len(cuts), largest / len(cuts))
        return jnp.repeat(jnp.exp(heights), shape[dim] // shards_of).reshape((-1,) + (1,) * (len(shape) - dim - 1))

    loudness = one(*cuts[0])
    for cut in cuts[1:]:
        loudness = loudness * one(*cut)
    return loudness


def noise(key, dims, width, limit, cuts=(), held_as=jnp.bfloat16):
    array = jax.random.normal(key, dims, jnp.float32) * width
    if len(cuts) > 0:
        array = block_levels(key, dims, cuts, -0.22, 0.18) * array
    return jnp.clip(array, min=-limit, max=limit).astype(held_as)


def setup_inputs(seed: int = 0) -> dict:
    keys = jax.random.split(jax.random.key(seed), 13)
    layer_input = noise(keys[0], (TOKENS, D), 1.0, 6.0, ((0, 32),))
    out_cotangent = noise(keys[1], (TOKENS, D), 1.0, 6.0, ((0, 32),))
    lengths = draw_lengths(jax.random.fold_in(keys[12], 71), 0)
    norm_attn = jnp.clip(1.0 + 0.1 * jax.random.normal(keys[3], (D,), jnp.float32), 0.5, 1.5).astype(jnp.bfloat16)
    w_query = draw_w_query(jax.random.fold_in(keys[12], 71), 0)
    w_key = draw_w_key(jax.random.fold_in(keys[12], 71), 0)
    w_value = noise(keys[6], (D, KVD), D ** -0.5, 0.15625, ((0, 32),))
    w_out = noise(keys[7], (D, D), (D // 64) ** -0.5, 1.25, ((0, 32),))
    norm_mlp = jnp.clip(1.0 + 0.1 * jax.random.normal(keys[8], (D,), jnp.float32), 0.5, 1.5).astype(jnp.bfloat16)
    w_gate = noise(keys[9], (D, FF), D ** -0.5, 0.15625, ((0, 32),))
    w_up = noise(keys[10], (D, FF), D ** -0.5, 0.15625, ((0, 32),))
    w_down = noise(keys[11], (FF, D), (FF // 4) ** -0.5, 0.1875, ((0, 32),))
    return {"layer_input": layer_input, "out_cotangent": out_cotangent, "lengths": lengths, "norm_attn": norm_attn, "w_query": w_query, "w_key": w_key, "w_value": w_value, "w_out": w_out, "norm_mlp": norm_mlp, "w_gate": w_gate, "w_up": w_up, "w_down": w_down}


eps_norm = 1e-05
rope_theta = 100000.0
highest = lax.Precision.HIGHEST

@jax.custom_vjp
def low(v):
    return lax.optimization_barrier(v.astype(jnp.bfloat16)).astype(jnp.float32)

@jax.custom_vjp
def low_back(v):
    return v

def low_keep(v):
    return (low(v), None)

def low_pass(kept, grad):
    return (grad,)

def back_keep(v):
    return (v, None)

def back_low(kept, grad):
    return (low(grad),)
low.defvjp(low_keep, low_pass)
low_back.defvjp(back_keep, back_low)

def slot_layout(lengths_row):
    slot_count = BLOCK * BLOCKS_DEV
    blocks_used = (lengths_row + BLOCK - 1) // BLOCK
    first_block = jnp.cumsum(blocks_used) - blocks_used
    slot_index = jnp.arange(slot_count, dtype=jnp.int32)
    block_of = slot_index // BLOCK
    inside = (block_of[:, None] >= first_block[None, :]) & (block_of[:, None] < (first_block + blocks_used)[None, :])
    seq_index = jnp.arange(BLOCKS_DEV, dtype=jnp.int32)
    present = jnp.any(inside, axis=1)
    owner_seq = jnp.where(present, lax.optimization_barrier(jnp.sum(jnp.where(inside, seq_index[None, :], 0), axis=1)), -1)
    start_slot = lax.optimization_barrier(jnp.sum(jnp.where(inside, first_block[None, :], 0), axis=1)) * BLOCK
    seq_length = lax.optimization_barrier(jnp.sum(jnp.where(inside, lengths_row[None, :], 0), axis=1))
    position = slot_index - start_slot
    live_slot = present & (position < seq_length)
    visible = (owner_seq[:, None] == owner_seq[None, :]) & (slot_index[None, :] <= slot_index[:, None]) & live_slot[:, None] & live_slot[None, :]
    return (position, live_slot, visible)

def rope_tables(position):
    half_width = HEAD // 2
    exponent = jnp.arange(half_width, dtype=jnp.float32) * (2.0 / HEAD)
    inverse = jnp.exp(-math.log(rope_theta) * exponent)
    angles = position.astype(jnp.float32)[:, None] * inverse[None, :]
    cosine_tab = jnp.concatenate([jnp.cos(angles), jnp.cos(angles)], axis=-1)
    sine_tab = jnp.concatenate([jnp.sin(angles), jnp.sin(angles)], axis=-1)
    return (cosine_tab, sine_tab)

def rotate_half(tensor):
    half_width = tensor.shape[-1] // 2
    return jnp.concatenate([-tensor[..., half_width:], tensor[..., :half_width]], axis=-1)

def rms_scale(values, gain_vec):
    return values * lax.rsqrt(lax.optimization_barrier(jnp.mean(values * values, axis=-1, keepdims=True)) + eps_norm) * gain_vec

def layer_forward(inputs, norm_attn, w_query, w_key, w_value, w_out, norm_mlp, w_gate, w_up, w_down, cosine_tab, sine_tab, visible, live_slot):
    group_devices = visible.shape[0]
    slot_count = visible.shape[1]
    group_size = HEADS // KV_HEADS
    score_scale = 1.0 / math.sqrt(HEAD)
    normed = low(rms_scale(inputs, norm_attn))
    queries = low_back(jnp.dot(normed, w_query, precision=highest))
    keys_proj = low_back(jnp.dot(normed, w_key, precision=highest))
    values_proj = low(low_back(jnp.dot(normed, w_value, precision=highest)))
    query_heads = queries.reshape(group_devices, slot_count, KV_HEADS, group_size, HEAD)
    key_heads = keys_proj.reshape(group_devices, slot_count, KV_HEADS, HEAD)
    q_rot = low(query_heads * cosine_tab[:, :, None, None, :] + rotate_half(query_heads) * sine_tab[:, :, None, None, :])
    k_rot = low(key_heads * cosine_tab[:, :, None, :] + rotate_half(key_heads) * sine_tab[:, :, None, :])
    value_heads = values_proj.reshape(group_devices, slot_count, KV_HEADS, HEAD)
    scores = low_back(jnp.einsum('gikrd,gjkd->gkrij', q_rot, k_rot, precision=highest) * score_scale)
    scores = jnp.where(visible[:, None, None, :, :], scores, -1e+30)
    weights = jax.nn.softmax(scores, axis=-1) * live_slot[:, None, None, :, None].astype(jnp.float32)
    mixed_heads = jnp.einsum('gkrij,gjkd->gikrd', low(weights), value_heads, precision=highest)
    attended = low(low_back(mixed_heads.reshape(group_devices * slot_count, HEADS * HEAD)))
    residual = inputs + low_back(jnp.dot(attended, w_out, precision=highest))
    normed_mlp = low(rms_scale(residual, norm_mlp))
    gate_proj = low_back(jnp.dot(normed_mlp, w_gate, precision=highest))
    up_proj = low_back(jnp.dot(normed_mlp, w_up, precision=highest))
    hidden = low(jax.nn.silu(gate_proj) * up_proj)
    return residual + low_back(jnp.dot(hidden, w_down, precision=highest))

def reference(layer_input, out_cotangent, lengths, norm_attn, w_query, w_key, w_value, w_out, norm_mlp, w_gate, w_up, w_down):
    group_devices = math.gcd(N_FSDP, 4)
    step_count = N_FSDP // group_devices
    slot_count = BLOCK * BLOCKS_DEV
    parameters = tuple((weight.astype(jnp.float32) for weight in (norm_attn, w_query, w_key, w_value, w_out, norm_mlp, w_gate, w_up, w_down)))
    inputs_all = layer_input.reshape(step_count, group_devices * slot_count, D)
    cotangent_all = out_cotangent.reshape(step_count, group_devices * slot_count, D)
    lengths_all = lengths.reshape(step_count, group_devices, BLOCKS_DEV)

    def one_step(totals, pieces):
        inputs, cotangent, lengths_group = pieces
        position, live_slot, visible = jax.vmap(slot_layout)(lengths_group)
        cosine_tab, sine_tab = jax.vmap(rope_tables)(position)

        def apply_layer(inputs_float, *weights):
            return layer_forward(inputs_float, *weights, cosine_tab, sine_tab, visible, live_slot)
        output, pullback = jax.vjp(apply_layer, inputs.astype(jnp.float32), *parameters)
        live_rows = live_slot.reshape(group_devices * slot_count)[:, None]
        gradients = pullback(jnp.where(live_rows, cotangent.astype(jnp.float32), 0.0))
        totals = tuple((running + fresh for running, fresh in zip(totals, gradients[1:])))
        return (totals, (output.astype(jnp.bfloat16), gradients[0]))
    initial = tuple((jnp.zeros(weight.shape, jnp.float32) for weight in parameters))
    totals, (outputs, input_grads) = lax.scan(one_step, initial, (inputs_all, cotangent_all, lengths_all))
    return (outputs.reshape(TOKENS, D), input_grads.reshape(TOKENS, D), totals[0], totals[1], totals[2], totals[3], totals[4], totals[5], totals[6], totals[7], totals[8])
```

```python
import functools
import math

import jax
import jax.numpy as jnp
from jax import lax
from jax.experimental import pallas as pl
from jax.experimental.pallas import tpu as pltpu
from jax.sharding import PartitionSpec as P

HEADS = 16
KV_HEADS = 8
HEAD = 96
LANES = 128
CUBE = 8
COLORS = 3

eps_norm = 1e-05
rope_theta = 100000.0
masked_score = -1e30
score_scale = 1.0 / math.sqrt(HEAD)


bf16 = jnp.bfloat16
f32 = jnp.float32


def rope_tables(slot_count):
    half_width = HEAD // 2
    exponent = jnp.arange(half_width, dtype=f32) * (2.0 / HEAD)
    inverse = jnp.exp(-math.log(rope_theta) * exponent)
    angles = jnp.arange(slot_count, dtype=jnp.int32).astype(f32)[:, None] * inverse[None, :]
    pad = jnp.zeros((slot_count, LANES - HEAD), f32)
    cosine_tab = jnp.concatenate([jnp.cos(angles), jnp.cos(angles), pad], axis=-1)
    sine_tab = jnp.concatenate([jnp.sin(angles), jnp.sin(angles), pad], axis=-1)
    return cosine_tab, sine_tab


def rms_parts(values):
    inverse_rms = lax.rsqrt(jnp.mean(values * values, axis=-1, keepdims=True) + eps_norm)
    return values * inverse_rms, inverse_rms


def rms_back(grad_normed, unit_rows, inverse_rms, gain_vec):
    scaled = grad_normed * gain_vec
    return inverse_rms * (scaled - unit_rows * jnp.mean(scaled * unit_rows, axis=-1, keepdims=True))


def contract_last(left_side, right_side):
    return lax.dot_general(
        left_side, right_side, (((1,), (1,)), ((), ())), preferred_element_type=f32
    )


def contract_first(left_side, right_side):
    return lax.dot_general(
        left_side, right_side, (((0,), (0,)), ((), ())), preferred_element_type=f32
    )


def matmul(left_side, right_side):
    return jnp.dot(left_side, right_side, preferred_element_type=f32)


def _rot_half(t, lane):
    return jnp.where(
        lane < HEAD // 2, -pltpu.roll(t, LANES - HEAD // 2, 1), pltpu.roll(t, HEAD // 2, 1)
    )


def _rope(t, cos, sin, lane):
    return t * cos + _rot_half(t, lane) * sin


def _unrope(t, cos, sin, lane):
    return t * cos - _rot_half(t, lane) * sin


def _wide(v):
    return jnp.concatenate([v, jnp.zeros_like(v)], axis=1)


def _weights(length, q, k, visible, live):
    scores = jnp.where(visible, contract_last(q, k) * score_scale, masked_score)
    exponent = jnp.exp(scores - jnp.max(scores, axis=-1, keepdims=True))
    return jnp.where(live, exponent / jnp.sum(exponent, axis=-1, keepdims=True), 0.0)


def _masks(length, slots):
    row = lax.broadcasted_iota(jnp.int32, (slots, slots), 0)
    col = lax.broadcasted_iota(jnp.int32, (slots, slots), 1)
    live = row < length
    return (col <= row) & live & (col < length), live


def attend_kernel(len_ref, qkv_ref, cos_ref, sin_ref, o_ref):
    length = len_ref[pl.program_id(0)]
    slots = qkv_ref.shape[0]
    visible, live = _masks(length, slots)
    lane = lax.broadcasted_iota(jnp.int32, (slots, LANES), 1)
    cos, sin = cos_ref[...], sin_ref[...]
    k = _rope(qkv_ref[:, 2 * LANES : 3 * LANES], cos, sin, lane).astype(bf16)
    v = qkv_ref[:, 3 * LANES :]
    v_wide = _wide(v)
    mixed = None
    for h in range(2):
        q = _rope(qkv_ref[:, h * LANES : (h + 1) * LANES], cos, sin, lane).astype(bf16)
        weights = _weights(length, q, k, visible, live).astype(bf16)
        v_h = v_wide if h == 0 else pltpu.roll(v_wide, HEAD, 1)
        part = matmul(weights, v_h.astype(bf16))
        mixed = part if mixed is None else mixed + part
    o_ref[...] = mixed.astype(bf16)


def attend_back_kernel(len_ref, qkv_ref, do_ref, cos_ref, sin_ref, out_ref):
    length = len_ref[pl.program_id(0)]
    slots = qkv_ref.shape[0]
    visible, live = _masks(length, slots)
    lane = lax.broadcasted_iota(jnp.int32, (slots, LANES), 1)
    cos, sin = cos_ref[...], sin_ref[...]
    k = _rope(qkv_ref[:, 2 * LANES : 3 * LANES], cos, sin, lane).astype(bf16)
    v_wide = _wide(qkv_ref[:, 3 * LANES :])
    d_o = do_ref[...]
    grad_k = grad_v = None
    for h in range(2):
        q = _rope(qkv_ref[:, h * LANES : (h + 1) * LANES], cos, sin, lane).astype(bf16)
        weights = _weights(length, q, k, visible, live)
        v_h = v_wide if h == 0 else pltpu.roll(v_wide, HEAD, 1)
        grad_weights = contract_last(d_o, v_h.astype(bf16))
        row_inner = jnp.sum(weights * grad_weights, axis=-1, keepdims=True)
        grad_scores = (weights * (grad_weights - row_inner)).astype(bf16)
        grad_q = matmul(grad_scores, k) * score_scale
        out_ref[:, h * LANES : (h + 1) * LANES] = _unrope(grad_q, cos, sin, lane).astype(bf16)
        part_k = contract_first(grad_scores, q) * score_scale
        part_v = contract_first(weights.astype(bf16), d_o)
        if h == 1:
            part_v = pltpu.roll(part_v, 2 * LANES - HEAD, 1)
        part_v = part_v[:, :LANES]
        grad_k = part_k if grad_k is None else grad_k + part_k
        grad_v = part_v if grad_v is None else grad_v + part_v
    out_ref[:, 2 * LANES : 3 * LANES] = _unrope(grad_k, cos, sin, lane).astype(bf16)
    out_ref[:, 3 * LANES :] = jnp.where(lane < HEAD, grad_v, 0.0).astype(bf16)


def attend(lengths, qkv, cos, sin):
    blocks, slots, width = qkv.shape
    table = pl.BlockSpec((slots, LANES), lambda s, ln: (0, 0))
    return pl.pallas_call(
        attend_kernel,
        out_shape=jax.ShapeDtypeStruct((blocks, slots, 2 * LANES), bf16),
        grid_spec=pltpu.PrefetchScalarGridSpec(
            num_scalar_prefetch=1,
            grid=(blocks,),
            in_specs=[pl.BlockSpec((None, slots, width), lambda s, ln: (s, 0, 0)), table, table],
            out_specs=pl.BlockSpec((None, slots, 2 * LANES), lambda s, ln: (s, 0, 0)),
        ),
        cost_estimate=pl.CostEstimate(
            flops=blocks * 8 * slots * slots * LANES, bytes_accessed=blocks * slots * width * 6,
            transcendentals=blocks * 2 * slots * slots,
        ),
    )(lengths, qkv, cos, sin)


def attend_back(lengths, qkv, d_o, cos, sin):
    blocks, slots, width = qkv.shape
    table = pl.BlockSpec((slots, LANES), lambda s, ln: (0, 0))
    return pl.pallas_call(
        attend_back_kernel,
        out_shape=jax.ShapeDtypeStruct((blocks, slots, width), bf16),
        grid_spec=pltpu.PrefetchScalarGridSpec(
            num_scalar_prefetch=1,
            grid=(blocks,),
            in_specs=[
                pl.BlockSpec((None, slots, width), lambda s, ln: (s, 0, 0)),
                pl.BlockSpec((None, slots, 2 * LANES), lambda s, ln: (s, 0, 0)),
                table,
                table,
            ],
            out_specs=pl.BlockSpec((None, slots, width), lambda s, ln: (s, 0, 0)),
        ),
        cost_estimate=pl.CostEstimate(
            flops=blocks * 24 * slots * slots * LANES, bytes_accessed=blocks * slots * width * 8,
            transcendentals=blocks * 2 * slots * slots,
        ),
    )(lengths, qkv, d_o, cos, sin)


def per_device(
    n,
    layer_input,
    out_cotangent,
    lengths,
    norm_attn,
    w_query,
    w_key,
    w_value,
    w_out,
    norm_mlp,
    w_gate,
    w_up,
    w_down,
):
    cubes = n // (2 * CUBE)
    slots, width = layer_input.shape
    rows = w_query.shape[0]
    down_rows = w_down.shape[0]
    q_cols, kv_cols = w_query.shape[1] // CUBE, w_key.shape[1] // CUBE
    me = lax.axis_index("fsdp")
    core, place, cube = me % 2, (me // 2) % CUBE, me // (2 * CUBE)

    def swap(array, bits):
        return lax.ppermute(array, "fsdp", [(i, i ^ bits) for i in range(n)])

    def cube_gather(block):
        part = block.shape[1] // COLORS
        columns = []
        for color in range(COLORS):
            order = [(color + i) % 3 for i in range(3)]
            held, names = block[None, :, color * part : (color + 1) * part], [0]
            for bit in order:
                held = jnp.concatenate([held, swap(held, 2 << bit)], axis=0)
                names = names + [name ^ (1 << bit) for name in names]
            columns.append((held, names))
        return jnp.stack(
            [
                jnp.concatenate([held[names.index(s)] for held, names in columns], axis=1)
                for s in range(CUBE)
            ]
        )

    def cube_scatter(blocks):
        part = blocks.shape[2] // COLORS
        columns = []
        for color in range(COLORS):
            order = [(color + i) % 3 for i in range(3)]
            held = {s: blocks[s, :, color * part : (color + 1) * part] for s in range(CUBE)}
            for bit in order:
                send = [s for s in held if s & (1 << bit)]
                got = swap(jnp.stack([held[s] for s in send]), 2 << bit)
                for i, s in enumerate(send):
                    held[s ^ (1 << bit)] = held[s ^ (1 << bit)] + got[i]
                    del held[s]
            columns.append(held[0])
        return jnp.concatenate(columns, axis=1)

    def cube_exchange(blocks):
        return jnp.stack([blocks[0]] + [swap(blocks[s], 2 * s) for s in range(1, CUBE)])

    relative = jnp.arange(CUBE, dtype=jnp.int32) ^ place

    def by_place(blocks):
        return jnp.take(blocks, relative, axis=0, indices_are_sorted=False, unique_indices=True)

    def group_gather(block):
        held = jnp.stack([block] + [swap(block, 2 * CUBE * s) for s in range(1, cubes)])
        return jnp.stack([held, swap(held, 1)])

    owner = jnp.arange(n, dtype=jnp.int32)
    from_me = owner ^ me
    owner_entry = ((from_me % 2) * cubes + from_me // (2 * CUBE)) * CUBE + (from_me // 2) % CUBE
    pair = jnp.arange(2 * cubes, dtype=jnp.int32)
    pair_entry = ((pair % 2) ^ core) * cubes + ((pair // 2) ^ cube)

    def all_rows(block):
        held = group_gather(block).reshape(n, *block.shape[1:])
        return jnp.take(held, owner_entry, axis=0, unique_indices=True)

    small = jnp.concatenate(
        [norm_attn, norm_mlp, lengths[0].astype(bf16), jnp.zeros((LANES - 2 * rows - 1,), bf16)]
    )[None]
    bit = 1
    while bit < n:
        small = jnp.concatenate([small, swap(small, bit)], axis=0)
        bit *= 2
    cube_lengths = small[0 : 2 * CUBE : 2, 2 * rows].astype(jnp.int32)
    gains = jnp.take(small, from_me, axis=0)
    gain_attn = gains[:, :rows].reshape(width).astype(f32)
    gain_mlp = gains[:, rows : 2 * rows].reshape(width).astype(f32)
    cos, sin = rope_tables(slots)

    x_all = cube_gather(layer_input)
    own_qkv = jnp.concatenate(
        [
            w_query.reshape(rows, CUBE, q_cols),
            w_key.reshape(rows, CUBE, kv_cols),
            w_value.reshape(rows, CUBE, kv_cols),
        ],
        axis=2,
    ).transpose(1, 0, 2)
    w_qkv = all_rows(cube_exchange(by_place(own_qkv))).reshape(width, q_cols + 2 * kv_cols)
    w_qkv = jnp.pad(
        w_qkv.reshape(width, 4, HEAD), ((0, 0), (0, 0), (0, LANES - HEAD))
    ).reshape(width, 4 * LANES)

    out_held = jnp.stack([w_out] + [swap(w_out, 2 * CUBE * s) for s in range(1, cubes)])
    out_held = out_held.reshape(1, cubes, rows, width)
    for bit in range(3):
        out_held = jnp.concatenate([out_held, swap(out_held, 2 << bit)], axis=0)
    out_held = jnp.stack([out_held, swap(out_held, 1)])
    out_entry = ((from_me % 2) * CUBE + (from_me // 2) % CUBE) * cubes + from_me // (2 * CUBE)
    full_out = jnp.take(out_held.reshape(n, rows, width), out_entry, axis=0, unique_indices=True)
    full_out = jnp.pad(
        full_out.reshape(CUBE, q_cols, width), ((0, 0), (0, 2 * LANES - q_cols), (0, 0))
    ).reshape(CUBE * 2 * LANES, width)

    ff_cols = 2 * cubes * down_rows

    def by_hidden(weight):
        split = weight.reshape(rows, cubes, CUBE, 2, down_rows)
        return split.transpose(2, 0, 1, 3, 4).reshape(CUBE, rows, ff_cols)

    own_gate_up = jnp.concatenate([by_hidden(w_gate), by_hidden(w_up)], axis=2)
    w_gate_up = all_rows(cube_exchange(by_place(own_gate_up))).reshape(width, 2 * ff_cols)
    down_held = group_gather(w_down).reshape(2 * cubes, down_rows, width)
    down = jnp.take(down_held, pair_entry, axis=0, unique_indices=True).reshape(ff_cols, width)

    live = jnp.arange(slots, dtype=jnp.int32)[:, None] < lengths[0, 0]
    cotangent = jnp.where(live, out_cotangent, jnp.zeros_like(out_cotangent))
    g_all = cube_gather(cotangent).reshape(CUBE * slots, width)

    inputs = layer_input.astype(f32)
    unit_all, _ = rms_parts(x_all.reshape(CUBE * slots, width).astype(f32))
    normed_all = (unit_all * gain_attn).astype(bf16)
    qkv = matmul(normed_all, w_qkv).reshape(CUBE, slots, 4 * LANES)
    mixed = attend(cube_lengths, qkv, cos, sin)
    attended = by_place(cube_exchange(mixed)).transpose(1, 0, 2).reshape(slots, CUBE * 2 * LANES)
    residual = inputs + matmul(attended, full_out)
    unit_mlp, inv_mlp = rms_parts(residual)
    normed_mlp = cube_gather((unit_mlp * gain_mlp).astype(bf16)).reshape(CUBE * slots, width)

    gate_up = matmul(normed_mlp, w_gate_up)
    gate, up = gate_up[:, :ff_cols], gate_up[:, ff_cols:]
    sigmoid_gate = jax.nn.sigmoid(gate)
    hidden = (gate * sigmoid_gate * up).astype(bf16)
    grad_hidden = contract_last(g_all, down)
    grad_gate = (grad_hidden * up * sigmoid_gate * (1.0 + gate * (1.0 - sigmoid_gate))).astype(bf16)
    grad_up = (grad_hidden * gate * sigmoid_gate).astype(bf16)
    grad_gate_up = jnp.concatenate([grad_gate, grad_up], axis=1)
    grad_normed_mlp = cube_scatter(
        contract_last(grad_gate_up, w_gate_up).reshape(CUBE, slots, width)
    )
    grad_resid = cotangent.astype(f32) + rms_back(grad_normed_mlp, unit_mlp, inv_mlp, gain_mlp)
    grad_resid_low = grad_resid.astype(bf16)

    grad_attended = contract_last(grad_resid_low, full_out).astype(bf16)
    grad_blocks = by_place(grad_attended.reshape(slots, CUBE, 2 * LANES).transpose(1, 0, 2))
    grad_mixed = cube_exchange(grad_blocks)
    grad_qkv = attend_back(cube_lengths, qkv, grad_mixed, cos, sin).reshape(
        CUBE * slots, 4 * LANES
    )

    def low_sum(blocks):
        total = blocks[0]
        for s in range(1, CUBE):
            total = total + swap(blocks[s].astype(bf16), 2 * s).astype(f32)
        return total

    output = (
        residual + low_sum(matmul(hidden, down).reshape(CUBE, slots, width))
    ).astype(bf16)
    grad_normed = low_sum(contract_last(grad_qkv, w_qkv).reshape(CUBE, slots, width))
    unit_attn, inv_attn = rms_parts(inputs)
    grad_input = grad_resid + rms_back(grad_normed, unit_attn, inv_attn, gain_attn)

    def group_sum(blocks, core_axis):
        pick = functools.partial(
            lax.dynamic_index_in_dim, axis=core_axis + 1, keepdims=False
        )
        pair_total = pick(blocks, core) + swap(pick(blocks, 1 - core), 1)
        total = lax.dynamic_index_in_dim(pair_total, cube, axis=0, keepdims=False)
        for s in range(1, cubes):
            send = lax.dynamic_index_in_dim(pair_total, cube ^ s, axis=0, keepdims=False)
            total = total + swap(send.astype(bf16), 2 * CUBE * s).astype(f32)
        return total

    grad_down = group_sum(
        contract_first(hidden, g_all).reshape(cubes, 2, down_rows, width), 0
    )

    def to_owners(partial):
        cols = partial.shape[1]
        total = group_sum(partial.reshape(cubes, CUBE, 2, rows, cols), 1)
        return by_place(cube_exchange(by_place(total.astype(bf16)))).astype(f32)

    grad_gu = to_owners(contract_first(normed_mlp, grad_gate_up))

    def hidden_back(block):
        return block.reshape(CUBE, rows, cubes, 2, down_rows).transpose(1, 2, 0, 3, 4).reshape(
            rows, cubes * CUBE * 2 * down_rows
        )

    grad_w_gate, grad_w_up = hidden_back(grad_gu[:, :, :ff_cols]), hidden_back(grad_gu[:, :, ff_cols:])

    grad_w = to_owners(contract_first(normed_all, grad_qkv))
    grad_heads = grad_w.reshape(CUBE, rows, 4, LANES)[:, :, :, :HEAD].transpose(1, 2, 0, 3)
    grad_w_query = grad_heads[:, :2].transpose(0, 2, 1, 3).reshape(rows, CUBE * q_cols)
    grad_w_key = grad_heads[:, 2].reshape(rows, CUBE * kv_cols)
    grad_w_value = grad_heads[:, 3].reshape(rows, CUBE * kv_cols)

    resid_low_all = cube_gather(grad_resid_low).reshape(CUBE * slots, width)
    grad_out_part = contract_first(mixed.reshape(CUBE * slots, 2 * LANES), resid_low_all)[:q_cols]
    grad_out_sum = group_sum(grad_out_part.reshape(cubes, 2, rows, width), 0)
    moves = [
        (2 * CUBE * g + 2 * t + c, 2 * cubes * t + 2 * g + c)
        for g in range(cubes)
        for t in range(CUBE)
        for c in range(2)
    ]
    grad_w_out = lax.ppermute(grad_out_sum.astype(bf16), "fsdp", moves).astype(f32)

    def gain_grad(gain, pairs):
        total = sum(jnp.sum(weight.astype(f32) * grad, axis=1) for weight, grad in pairs)
        return total / gain.astype(f32)

    gain_attn_grad = gain_grad(
        norm_attn, [(w_query, grad_w_query), (w_key, grad_w_key), (w_value, grad_w_value)]
    )
    gain_mlp_grad = gain_grad(norm_mlp, [(w_gate, grad_w_gate), (w_up, grad_w_up)])
    return (
        output,
        grad_input,
        gain_attn_grad,
        grad_w_query,
        grad_w_key,
        grad_w_value,
        grad_w_out,
        gain_mlp_grad,
        grad_w_gate,
        grad_w_up,
        grad_down,
    )


def solution(mesh):
    rows, vec = P("fsdp", None), P("fsdp")
    return jax.shard_map(
        functools.partial(per_device, mesh.shape["fsdp"]),
        mesh=mesh,
        in_specs=(rows, rows, rows, vec, rows, rows, rows, rows, vec, rows, rows, rows),
        out_specs=(rows, rows, vec, rows, rows, rows, rows, vec, rows, rows, rows),
        check_vma=False,
    )
```

```python
import functools
import math

import jax
import jax.numpy as jnp
from jax import lax
from jax.experimental import pallas as pl
from jax.experimental.pallas import tpu as pltpu
from jax.sharding import PartitionSpec as P

HEADS = 16
KV_HEADS = 8
HEAD = 96
LANES = 128
CUBE = 8
COLORS = 3

eps_norm = 1e-05
rope_theta = 100000.0
masked_score = -1e30
score_scale = 1.0 / math.sqrt(HEAD)


bf16 = jnp.bfloat16
f32 = jnp.float32


def rope_tables(slot_count):
    half_width = HEAD // 2
    exponent = jnp.arange(half_width, dtype=f32) * (2.0 / HEAD)
    inverse = jnp.exp(-math.log(rope_theta) * exponent)
    angles = jnp.arange(slot_count, dtype=jnp.int32).astype(f32)[:, None] * inverse[None, :]
    pad = jnp.zeros((slot_count, LANES - HEAD), f32)
    cosine_tab = jnp.concatenate([jnp.cos(angles), jnp.cos(angles), pad], axis=-1)
    sine_tab = jnp.concatenate([jnp.sin(angles), jnp.sin(angles), pad], axis=-1)
    return cosine_tab, sine_tab


def rms_parts(values):
    inverse_rms = lax.rsqrt(jnp.mean(values * values, axis=-1, keepdims=True) + eps_norm)
    return values * inverse_rms, inverse_rms


def rms_back(grad_normed, unit_rows, inverse_rms, gain_vec):
    scaled = grad_normed * gain_vec
    return inverse_rms * (scaled - unit_rows * jnp.mean(scaled * unit_rows, axis=-1, keepdims=True))


def contract_last(left_side, right_side):
    return lax.dot_general(
        left_side, right_side, (((1,), (1,)), ((), ())), preferred_element_type=f32
    )


def contract_first(left_side, right_side):
    return lax.dot_general(
        left_side, right_side, (((0,), (0,)), ((), ())), preferred_element_type=f32
    )


def matmul(left_side, right_side):
    return jnp.dot(left_side, right_side, preferred_element_type=f32)


def _rot_half(t, lane):
    return jnp.where(
        lane < HEAD // 2, -pltpu.roll(t, LANES - HEAD // 2, 1), pltpu.roll(t, HEAD // 2, 1)
    )


def _rope(t, cos, sin, lane):
    return t * cos + _rot_half(t, lane) * sin


def _unrope(t, cos, sin, lane):
    return t * cos - _rot_half(t, lane) * sin


def _wide(v):
    return jnp.concatenate([v, jnp.zeros_like(v)], axis=1)


def _weights(length, q, k, visible, live):
    scores = jnp.where(visible, contract_last(q, k) * score_scale, masked_score)
    exponent = jnp.exp(scores - jnp.max(scores, axis=-1, keepdims=True))
    return jnp.where(live, exponent / jnp.sum(exponent, axis=-1, keepdims=True), 0.0)


def _masks(length, slots):
    row = lax.broadcasted_iota(jnp.int32, (slots, slots), 0)
    col = lax.broadcasted_iota(jnp.int32, (slots, slots), 1)
    live = row < length
    return (col <= row) & live & (col < length), live


def attend_kernel(len_ref, qkv_ref, cos_ref, sin_ref, o_ref):
    length = len_ref[pl.program_id(0)]
    slots = qkv_ref.shape[0]
    visible, live = _masks(length, slots)
    lane = lax.broadcasted_iota(jnp.int32, (slots, LANES), 1)
    cos, sin = cos_ref[...], sin_ref[...]
    k = _rope(qkv_ref[:, 2 * LANES : 3 * LANES], cos, sin, lane).astype(bf16)
    v = qkv_ref[:, 3 * LANES :]
    v_wide = _wide(v)
    mixed = None
    for h in range(2):
        q = _rope(qkv_ref[:, h * LANES : (h + 1) * LANES], cos, sin, lane).astype(bf16)
        weights = _weights(length, q, k, visible, live).astype(bf16)
        v_h = v_wide if h == 0 else pltpu.roll(v_wide, HEAD, 1)
        part = matmul(weights, v_h.astype(bf16))
        mixed = part if mixed is None else mixed + part
    o_ref[...] = mixed.astype(bf16)


def attend_back_kernel(len_ref, qkv_ref, do_ref, cos_ref, sin_ref, out_ref):
    length = len_ref[pl.program_id(0)]
    slots = qkv_ref.shape[0]
    visible, live = _masks(length, slots)
    lane = lax.broadcasted_iota(jnp.int32, (slots, LANES), 1)
    cos, sin = cos_ref[...], sin_ref[...]
    k = _rope(qkv_ref[:, 2 * LANES : 3 * LANES], cos, sin, lane).astype(bf16)
    v_wide = _wide(qkv_ref[:, 3 * LANES :])
    d_o = do_ref[...]
    grad_k = grad_v = None
    for h in range(2):
        q = _rope(qkv_ref[:, h * LANES : (h + 1) * LANES], cos, sin, lane).astype(bf16)
        weights = _weights(length, q, k, visible, live)
        v_h = v_wide if h == 0 else pltpu.roll(v_wide, HEAD, 1)
        grad_weights = contract_last(d_o, v_h.astype(bf16))
        row_inner = jnp.sum(weights * grad_weights, axis=-1, keepdims=True)
        grad_scores = (weights * (grad_weights - row_inner)).astype(bf16)
        grad_q = matmul(grad_scores, k) * score_scale
        out_ref[:, h * LANES : (h + 1) * LANES] = _unrope(grad_q, cos, sin, lane).astype(bf16)
        part_k = contract_first(grad_scores, q) * score_scale
        part_v = contract_first(weights.astype(bf16), d_o)
        if h == 1:
            part_v = pltpu.roll(part_v, 2 * LANES - HEAD, 1)
        part_v = part_v[:, :LANES]
        grad_k = part_k if grad_k is None else grad_k + part_k
        grad_v = part_v if grad_v is None else grad_v + part_v
    out_ref[:, 2 * LANES : 3 * LANES] = _unrope(grad_k, cos, sin, lane).astype(bf16)
    out_ref[:, 3 * LANES :] = jnp.where(lane < HEAD, grad_v, 0.0).astype(bf16)


def attend(lengths, qkv, cos, sin):
    blocks, slots, width = qkv.shape
    table = pl.BlockSpec((slots, LANES), lambda s, ln: (0, 0))
    return pl.pallas_call(
        attend_kernel,
        out_shape=jax.ShapeDtypeStruct((blocks, slots, 2 * LANES), bf16),
        grid_spec=pltpu.PrefetchScalarGridSpec(
            num_scalar_prefetch=1,
            grid=(blocks,),
            in_specs=[pl.BlockSpec((None, slots, width), lambda s, ln: (s, 0, 0)), table, table],
            out_specs=pl.BlockSpec((None, slots, 2 * LANES), lambda s, ln: (s, 0, 0)),
        ),
        cost_estimate=pl.CostEstimate(
            flops=blocks * 8 * slots * slots * LANES, bytes_accessed=blocks * slots * width * 6,
            transcendentals=blocks * 2 * slots * slots,
        ),
    )(lengths, qkv, cos, sin)


def attend_back(lengths, qkv, d_o, cos, sin):
    blocks, slots, width = qkv.shape
    table = pl.BlockSpec((slots, LANES), lambda s, ln: (0, 0))
    return pl.pallas_call(
        attend_back_kernel,
        out_shape=jax.ShapeDtypeStruct((blocks, slots, width), bf16),
        grid_spec=pltpu.PrefetchScalarGridSpec(
            num_scalar_prefetch=1,
            grid=(blocks,),
            in_specs=[
                pl.BlockSpec((None, slots, width), lambda s, ln: (s, 0, 0)),
                pl.BlockSpec((None, slots, 2 * LANES), lambda s, ln: (s, 0, 0)),
                table,
                table,
            ],
            out_specs=pl.BlockSpec((None, slots, width), lambda s, ln: (s, 0, 0)),
        ),
        cost_estimate=pl.CostEstimate(
            flops=blocks * 24 * slots * slots * LANES, bytes_accessed=blocks * slots * width * 8,
            transcendentals=blocks * 2 * slots * slots,
        ),
    )(lengths, qkv, d_o, cos, sin)


class Mail:
    def __init__(self, me, send_sems, recv_sems):
        self.me, self.send_sems, self.recv_sems = me, send_sems, recv_sems
        self.count, self.all = 0, []

    def peer(self, bits):
        device, bit = self.me, 1
        while bit <= bits:
            if bits & bit:
                device = device + bit * (1 - 2 * ((self.me // bit) % 2))
            bit *= 2
        return device

    def send(self, src, dst, bits):
        copy = pltpu.make_async_remote_copy(
            src_ref=src,
            dst_ref=dst,
            send_sem=self.send_sems.at[self.count],
            recv_sem=self.recv_sems.at[self.count],
            device_id=(self.peer(bits),),
            device_id_type=pl.DeviceIdType.MESH,
        )
        self.count += 1
        copy.start()
        self.all.append(copy)
        return copy

    def finish(self):
        for copy in self.all:
            copy.wait_send()


def xor_place(t, s):
    total = 0
    for bit in (1, 2, 4):
        total = total + bit * (((t // bit) % 2 + (s // bit) % 2) % 2)
    return total


def gather_start(mail, all_ref, own):
    part = all_ref.shape[2] // COLORS
    cps = {}
    for color in range(COLORS):
        cols = pl.ds(color * part, part)
        for i in range(3):
            bit = 1 << ((color + i) % 3)
            cps[color, bit] = mail.send(own.at[:, cols], all_ref.at[bit, :, cols], 2 * bit)
    return cps


def gather_forward(mail, all_ref, cps, stage):
    part = all_ref.shape[2] // COLORS
    for color in range(COLORS):
        cols = pl.ds(color * part, part)
        b1, b2, b3 = [1 << ((color + i) % 3) for i in range(3)]
        moves = {0: [(b1, (b2, b3))], 1: [(b2, (b3,)), (b1 ^ b2, (b3,))]}[stage]
        for slot, bits in moves:
            cps[color, slot].wait_recv()
            for bit in bits:
                cps[color, slot ^ bit] = mail.send(
                    all_ref.at[slot, :, cols], all_ref.at[slot ^ bit, :, cols], 2 * bit
                )


def gather_finish(cps):
    for color in range(COLORS):
        b1, b2, b3 = [1 << ((color + i) % 3) for i in range(3)]
        for slot in (b3, b1 ^ b3, b2 ^ b3, b1 ^ b2 ^ b3):
            cps[color, slot].wait_recv()


def forward_kernel(
    n, x_ref, small_ref, pack_ref, wo_ref, gu_ref, wd_ref, g_ref, cos_ref, sin_ref,
    h1_all, qkv_all, mixed_all, slots_ref, resid_ref, h2_all, g_all, wqkv, wout, wgu, wdown, gains,
    x_all, small_got, send_sems, recv_sems, local_sems,
):
    cubes = n // (2 * CUBE)
    me = lax.axis_index("fsdp")
    core, place, cube = me % 2, (me // 2) % CUBE, me // (2 * CUBE)
    pz, py, px = place // 4, (place // 2) % 2, place % 2
    mail = Mail(me, send_sems, recv_sems)
    slots, width = x_ref.shape
    rows = wo_ref.shape[0]
    peers = [2 * s for s in range(1, CUBE)] + [1] + [2 * CUBE * s for s in range(1, cubes)]

    barrier = pltpu.get_barrier_semaphore()
    for bits in peers:
        pl.semaphore_signal(
            barrier, inc=1, device_id=(mail.peer(bits),), device_id_type=pl.DeviceIdType.MESH
        )
    pl.semaphore_wait(barrier, len(peers))

    local = [
        pltpu.make_async_copy(pack_ref.at[place], wqkv.at[cube, place, core], local_sems.at[0]),
        pltpu.make_async_copy(gu_ref.at[place], wgu.at[cube, place, core], local_sems.at[1]),
        pltpu.make_async_copy(wd_ref, wdown.at[cube, core], local_sems.at[2]),
        pltpu.make_async_copy(wo_ref, wout.at[cube, pz, py, px, core], local_sems.at[3]),
        pltpu.make_async_copy(g_ref, g_all.at[0], local_sems.at[4]),
        pltpu.make_async_copy(x_ref, x_all.at[0], local_sems.at[5]),
        pltpu.make_async_copy(small_ref, gains, local_sems.at[6]),
    ]
    for copy in local:
        copy.start()

    pack_cps = [
        mail.send(pack_ref.at[xor_place(place, s)], wqkv.at[cube, place, core], 2 * s)
        for s in range(1, CUBE)
    ]
    x_cps = gather_start(mail, x_all, x_ref)
    wo_cps = [
        mail.send(wo_ref, wout.at[cube, pz, py, px, core], 2 * CUBE * s) for s in range(1, cubes)
    ]

    local[6].wait()
    bit, i = 1, 0
    while bit < n:
        copy = mail.send(gains, small_got.at[i], bit)
        mail.all.pop()
        copy.wait()
        gains[...] += small_got[i]
        bit, i = 2 * bit, i + 1

    local[0].wait()
    for copy in pack_cps:
        copy.wait_recv()
    pack_cps = [
        mail.send(wqkv.at[cube, :, core], wqkv.at[cube, :, core], 2 * CUBE * s)
        for s in range(1, cubes)
    ]
    core_cps = [mail.send(wqkv.at[cube, :, core], wqkv.at[cube, :, core], 1)]

    gather_forward(mail, x_all, x_cps, 0)
    gu_cps = [
        mail.send(gu_ref.at[xor_place(place, s)], wgu.at[cube, place, core], 2 * s)
        for s in range(1, CUBE)
    ]
    wd_cps = [mail.send(wd_ref, wdown.at[cube, core], 2 * CUBE * s) for s in range(1, cubes)]
    for s, copy in enumerate(pack_cps, 1):
        copy.wait_recv()
        there = mail.peer(2 * CUBE * s) // (2 * CUBE)
        core_cps.append(mail.send(wqkv.at[there, :, core], wqkv.at[there, :, core], 1))
    gather_forward(mail, x_all, x_cps, 1)
    local[3].wait()
    for copy in wo_cps:
        copy.wait_recv()
    wo_x = mail.send(
        wout.at[:, pz, py, px, core], wout.at[:, pz, py, px, core], 8
    )
    gather_finish(x_cps)
    for copy in core_cps:
        copy.wait_recv()
    local[5].wait()

    gain_attn = gains[0:1, :]
    gain_mlp = gains[1:2, :]
    lengths = gains[2:3, :]
    row = lax.broadcasted_iota(jnp.int32, (slots, slots), 0)
    col = lax.broadcasted_iota(jnp.int32, (slots, slots), 1)
    lane = lax.broadcasted_iota(jnp.int32, (slots, LANES), 1)
    device = lax.broadcasted_iota(jnp.int32, lengths.shape, 1)

    def attention(s, carry):
        values = x_all[s].astype(f32)
        normed = (rms_parts(values)[0] * gain_attn).astype(bf16)
        h1_all[s] = normed
        qkv_all[s] = matmul(normed, wqkv[...].reshape(width, 4 * LANES))
        there = 2 * CUBE * cube + 2 * xor_place(place, s) + core
        length = jnp.sum(jnp.where(device == there, lengths, 0.0), axis=1, keepdims=True)
        live = row.astype(f32) < length
        visible = (col <= row) & live
        cos, sin = cos_ref[...], sin_ref[...]
        k = _rope(qkv_all[s, :, 2 * LANES : 3 * LANES], cos, sin, lane).astype(bf16)
        v_wide = _wide(qkv_all[s, :, 3 * LANES :])
        mixed = None
        for h in range(2):
            q = _rope(qkv_all[s, :, h * LANES : (h + 1) * LANES], cos, sin, lane).astype(bf16)
            weights = _weights(None, q, k, visible, live).astype(bf16)
            v_h = v_wide if h == 0 else pltpu.roll(v_wide, HEAD, 1)
            part = matmul(weights, v_h.astype(bf16))
            mixed = part if mixed is None else mixed + part
        mixed_all[s] = mixed.astype(bf16)
        return carry

    lax.fori_loop(0, CUBE, attention, 0)
    o_cps = [
        mail.send(mixed_all.at[s], slots_ref.at[place], 2 * s) for s in range(1, CUBE)
    ]
    slots_ref[place] = mixed_all[0]

    wo_x.wait_recv()
    wo_y = mail.send(wout.at[:, :, py, px, core], wout.at[:, :, py, px, core], 4)
    local[1].wait()
    for copy in gu_cps:
        copy.wait_recv()
    gu_cube = [
        mail.send(wgu.at[cube, :, core], wgu.at[cube, :, core], 2 * CUBE * s)
        for s in range(1, cubes)
    ]
    wo_y.wait_recv()
    wo_z = mail.send(wout.at[:, :, :, px, core], wout.at[:, :, :, px, core], 2)
    wo_z.wait_recv()
    wo_c = mail.send(wout.at[:, :, :, :, core], wout.at[:, :, :, :, core], 1)
    for copy in o_cps:
        copy.wait_recv()
    wide = []
    zero = jnp.zeros((slots, LANES), f32)
    for j in range(CUBE // 2):
        low = jnp.concatenate([slots_ref[2 * j].astype(f32), zero], axis=1)
        high = jnp.concatenate([slots_ref[2 * j + 1].astype(f32), zero], axis=1)
        wide.append((low + pltpu.roll(high, 2 * HEAD, 1)).astype(bf16))
    attended = jnp.concatenate(wide, axis=1)
    wo_c.wait_recv()
    step = 256
    for j in range(width // step):
        cols = slice(j * step, (j + 1) * step)
        weight = wout[:, :, :, :, :, :, cols].reshape(width, step)
        resid_ref[:, cols] = x_ref[:, cols].astype(f32) + matmul(attended, weight)
    h2_all[0] = (rms_parts(resid_ref[...])[0] * gain_mlp).astype(bf16)
    h2_cps = gather_start(mail, h2_all, h2_all.at[0])
    gather_forward(mail, h2_all, h2_cps, 0)
    gather_forward(mail, h2_all, h2_cps, 1)

    local[2].wait()
    for copy in wd_cps:
        copy.wait_recv()
    last = [mail.send(wdown.at[:, core], wdown.at[:, core], 1)]
    for copy in gu_cube:
        copy.wait_recv()
    last.append(mail.send(wgu.at[:, :, core], wgu.at[:, :, core], 1))
    local[4].wait()
    g_cps = gather_start(mail, g_all, g_ref)
    gather_forward(mail, g_all, g_cps, 0)
    gather_forward(mail, g_all, g_cps, 1)
    gather_finish(g_cps)
    gather_finish(h2_cps)
    for copy in last:
        copy.wait_recv()
    mail.finish()


def per_device_any(
    n,
    layer_input,
    out_cotangent,
    lengths,
    norm_attn,
    w_query,
    w_key,
    w_value,
    w_out,
    norm_mlp,
    w_gate,
    w_up,
    w_down,
):
    cubes = n // (2 * CUBE)
    slots, width = layer_input.shape
    rows = w_query.shape[0]
    down_rows = w_down.shape[0]
    q_cols, kv_cols = w_query.shape[1] // CUBE, w_key.shape[1] // CUBE
    me = lax.axis_index("fsdp")
    core, place, cube = me % 2, (me // 2) % CUBE, me // (2 * CUBE)

    def swap(array, bits):
        return lax.ppermute(array, "fsdp", [(i, i ^ bits) for i in range(n)])

    def cube_gather(block):
        part = block.shape[1] // COLORS
        columns = []
        for color in range(COLORS):
            order = [(color + i) % 3 for i in range(3)]
            held, names = block[None, :, color * part : (color + 1) * part], [0]
            for bit in order:
                held = jnp.concatenate([held, swap(held, 2 << bit)], axis=0)
                names = names + [name ^ (1 << bit) for name in names]
            columns.append((held, names))
        return jnp.stack(
            [
                jnp.concatenate([held[names.index(s)] for held, names in columns], axis=1)
                for s in range(CUBE)
            ]
        )

    def cube_scatter(blocks):
        part = blocks.shape[2] // COLORS
        columns = []
        for color in range(COLORS):
            order = [(color + i) % 3 for i in range(3)]
            held = {s: blocks[s, :, color * part : (color + 1) * part] for s in range(CUBE)}
            for bit in order:
                send = [s for s in held if s & (1 << bit)]
                got = swap(jnp.stack([held[s] for s in send]), 2 << bit)
                for i, s in enumerate(send):
                    held[s ^ (1 << bit)] = held[s ^ (1 << bit)] + got[i]
                    del held[s]
            columns.append(held[0])
        return jnp.concatenate(columns, axis=1)

    def cube_exchange(blocks):
        return jnp.stack([blocks[0]] + [swap(blocks[s], 2 * s) for s in range(1, CUBE)])

    relative = jnp.arange(CUBE, dtype=jnp.int32) ^ place

    def by_place(blocks):
        return jnp.take(blocks, relative, axis=0, indices_are_sorted=False, unique_indices=True)

    def group_gather(block):
        held = jnp.stack([block] + [swap(block, 2 * CUBE * s) for s in range(1, cubes)])
        return jnp.stack([held, swap(held, 1)])

    owner = jnp.arange(n, dtype=jnp.int32)
    from_me = owner ^ me
    owner_entry = ((from_me % 2) * cubes + from_me // (2 * CUBE)) * CUBE + (from_me // 2) % CUBE
    pair = jnp.arange(2 * cubes, dtype=jnp.int32)
    pair_entry = ((pair % 2) ^ core) * cubes + ((pair // 2) ^ cube)

    def all_rows(block):
        held = group_gather(block).reshape(n, *block.shape[1:])
        return jnp.take(held, owner_entry, axis=0, unique_indices=True)

    small = jnp.concatenate(
        [norm_attn, norm_mlp, lengths[0].astype(bf16), jnp.zeros((LANES - 2 * rows - 1,), bf16)]
    )[None]
    bit = 1
    while bit < n:
        small = jnp.concatenate([small, swap(small, bit)], axis=0)
        bit *= 2
    cube_lengths = small[0 : 2 * CUBE : 2, 2 * rows].astype(jnp.int32)
    gains = jnp.take(small, from_me, axis=0)
    gain_attn = gains[:, :rows].reshape(width).astype(f32)
    gain_mlp = gains[:, rows : 2 * rows].reshape(width).astype(f32)
    cos, sin = rope_tables(slots)

    x_all = cube_gather(layer_input)
    own_qkv = jnp.concatenate(
        [
            w_query.reshape(rows, CUBE, q_cols),
            w_key.reshape(rows, CUBE, kv_cols),
            w_value.reshape(rows, CUBE, kv_cols),
        ],
        axis=2,
    ).transpose(1, 0, 2)
    w_qkv = all_rows(cube_exchange(by_place(own_qkv))).reshape(width, q_cols + 2 * kv_cols)
    w_qkv = jnp.pad(
        w_qkv.reshape(width, 4, HEAD), ((0, 0), (0, 0), (0, LANES - HEAD))
    ).reshape(width, 4 * LANES)

    out_held = jnp.stack([w_out] + [swap(w_out, 2 * CUBE * s) for s in range(1, cubes)])
    out_held = out_held.reshape(1, cubes, rows, width)
    for bit in range(3):
        out_held = jnp.concatenate([out_held, swap(out_held, 2 << bit)], axis=0)
    out_held = jnp.stack([out_held, swap(out_held, 1)])
    out_entry = ((from_me % 2) * CUBE + (from_me // 2) % CUBE) * cubes + from_me // (2 * CUBE)
    full_out = jnp.take(out_held.reshape(n, rows, width), out_entry, axis=0, unique_indices=True)
    full_out = jnp.pad(
        full_out.reshape(CUBE, q_cols, width), ((0, 0), (0, 2 * LANES - q_cols), (0, 0))
    ).reshape(CUBE * 2 * LANES, width)

    ff_cols = 2 * cubes * down_rows

    def by_hidden(weight):
        split = weight.reshape(rows, cubes, CUBE, 2, down_rows)
        return split.transpose(2, 0, 1, 3, 4).reshape(CUBE, rows, ff_cols)

    own_gate_up = jnp.concatenate([by_hidden(w_gate), by_hidden(w_up)], axis=2)
    w_gate_up = all_rows(cube_exchange(by_place(own_gate_up))).reshape(width, 2 * ff_cols)
    down_held = group_gather(w_down).reshape(2 * cubes, down_rows, width)
    down = jnp.take(down_held, pair_entry, axis=0, unique_indices=True).reshape(ff_cols, width)

    live = jnp.arange(slots, dtype=jnp.int32)[:, None] < lengths[0, 0]
    cotangent = jnp.where(live, out_cotangent, jnp.zeros_like(out_cotangent))
    g_all = cube_gather(cotangent).reshape(CUBE * slots, width)

    inputs = layer_input.astype(f32)
    unit_all, _ = rms_parts(x_all.reshape(CUBE * slots, width).astype(f32))
    normed_all = (unit_all * gain_attn).astype(bf16)
    qkv = matmul(normed_all, w_qkv).reshape(CUBE, slots, 4 * LANES)
    mixed = attend(cube_lengths, qkv, cos, sin)
    attended = by_place(cube_exchange(mixed)).transpose(1, 0, 2).reshape(slots, CUBE * 2 * LANES)
    residual = inputs + matmul(attended, full_out)
    unit_mlp, inv_mlp = rms_parts(residual)
    normed_mlp = cube_gather((unit_mlp * gain_mlp).astype(bf16)).reshape(CUBE * slots, width)

    gate_up = matmul(normed_mlp, w_gate_up)
    gate, up = gate_up[:, :ff_cols], gate_up[:, ff_cols:]
    sigmoid_gate = jax.nn.sigmoid(gate)
    hidden = (gate * sigmoid_gate * up).astype(bf16)
    grad_hidden = contract_last(g_all, down)
    grad_gate = (grad_hidden * up * sigmoid_gate * (1.0 + gate * (1.0 - sigmoid_gate))).astype(bf16)
    grad_up = (grad_hidden * gate * sigmoid_gate).astype(bf16)
    grad_gate_up = jnp.concatenate([grad_gate, grad_up], axis=1)
    grad_normed_mlp = cube_scatter(
        contract_last(grad_gate_up, w_gate_up).reshape(CUBE, slots, width)
    )
    grad_resid = cotangent.astype(f32) + rms_back(grad_normed_mlp, unit_mlp, inv_mlp, gain_mlp)
    grad_resid_low = grad_resid.astype(bf16)

    grad_attended = contract_last(grad_resid_low, full_out).astype(bf16)
    grad_blocks = by_place(grad_attended.reshape(slots, CUBE, 2 * LANES).transpose(1, 0, 2))
    grad_mixed = cube_exchange(grad_blocks)
    grad_qkv = attend_back(cube_lengths, qkv, grad_mixed, cos, sin).reshape(
        CUBE * slots, 4 * LANES
    )

    def low_sum(blocks):
        total = blocks[0]
        for s in range(1, CUBE):
            total = total + swap(blocks[s].astype(bf16), 2 * s).astype(f32)
        return total

    output = (
        residual + low_sum(matmul(hidden, down).reshape(CUBE, slots, width))
    ).astype(bf16)
    grad_normed = low_sum(contract_last(grad_qkv, w_qkv).reshape(CUBE, slots, width))
    unit_attn, inv_attn = rms_parts(inputs)
    grad_input = grad_resid + rms_back(grad_normed, unit_attn, inv_attn, gain_attn)

    def group_sum(blocks, core_axis):
        pick = functools.partial(
            lax.dynamic_index_in_dim, axis=core_axis + 1, keepdims=False
        )
        pair_total = pick(blocks, core) + swap(pick(blocks, 1 - core), 1)
        total = lax.dynamic_index_in_dim(pair_total, cube, axis=0, keepdims=False)
        for s in range(1, cubes):
            send = lax.dynamic_index_in_dim(pair_total, cube ^ s, axis=0, keepdims=False)
            total = total + swap(send.astype(bf16), 2 * CUBE * s).astype(f32)
        return total

    grad_down = group_sum(
        contract_first(hidden, g_all).reshape(cubes, 2, down_rows, width), 0
    )

    def to_owners(partial):
        cols = partial.shape[1]
        total = group_sum(partial.reshape(cubes, CUBE, 2, rows, cols), 1)
        return by_place(cube_exchange(by_place(total.astype(bf16)))).astype(f32)

    grad_gu = to_owners(contract_first(normed_mlp, grad_gate_up))

    def hidden_back(block):
        return block.reshape(CUBE, rows, cubes, 2, down_rows).transpose(1, 2, 0, 3, 4).reshape(
            rows, cubes * CUBE * 2 * down_rows
        )

    grad_w_gate, grad_w_up = hidden_back(grad_gu[:, :, :ff_cols]), hidden_back(grad_gu[:, :, ff_cols:])

    grad_w = to_owners(contract_first(normed_all, grad_qkv))
    grad_heads = grad_w.reshape(CUBE, rows, 4, LANES)[:, :, :, :HEAD].transpose(1, 2, 0, 3)
    grad_w_query = grad_heads[:, :2].transpose(0, 2, 1, 3).reshape(rows, CUBE * q_cols)
    grad_w_key = grad_heads[:, 2].reshape(rows, CUBE * kv_cols)
    grad_w_value = grad_heads[:, 3].reshape(rows, CUBE * kv_cols)

    resid_low_all = cube_gather(grad_resid_low).reshape(CUBE * slots, width)
    grad_out_part = contract_first(mixed.reshape(CUBE * slots, 2 * LANES), resid_low_all)[:q_cols]
    grad_out_sum = group_sum(grad_out_part.reshape(cubes, 2, rows, width), 0)
    moves = [
        (2 * CUBE * g + 2 * t + c, 2 * cubes * t + 2 * g + c)
        for g in range(cubes)
        for t in range(CUBE)
        for c in range(2)
    ]
    grad_w_out = lax.ppermute(grad_out_sum.astype(bf16), "fsdp", moves).astype(f32)

    def gain_grad(gain, pairs):
        total = sum(jnp.sum(weight.astype(f32) * grad, axis=1) for weight, grad in pairs)
        return total / gain.astype(f32)

    gain_attn_grad = gain_grad(
        norm_attn, [(w_query, grad_w_query), (w_key, grad_w_key), (w_value, grad_w_value)]
    )
    gain_mlp_grad = gain_grad(norm_mlp, [(w_gate, grad_w_gate), (w_up, grad_w_up)])
    return (
        output,
        grad_input,
        gain_attn_grad,
        grad_w_query,
        grad_w_key,
        grad_w_value,
        grad_w_out,
        gain_mlp_grad,
        grad_w_gate,
        grad_w_up,
        grad_down,
    )


def per_device_fast(
    n,
    layer_input,
    out_cotangent,
    lengths,
    norm_attn,
    w_query,
    w_key,
    w_value,
    w_out,
    norm_mlp,
    w_gate,
    w_up,
    w_down,
):
    cubes = n // (2 * CUBE)
    slots, width = layer_input.shape
    rows = w_query.shape[0]
    down_rows = w_down.shape[0]
    q_cols, kv_cols = w_query.shape[1] // CUBE, w_key.shape[1] // CUBE
    me = lax.axis_index("fsdp")
    core, place, cube = me % 2, (me // 2) % CUBE, me // (2 * CUBE)

    def swap(array, bits):
        return lax.ppermute(array, "fsdp", [(i, i ^ bits) for i in range(n)])

    def cube_gather(block):
        part = block.shape[1] // COLORS
        columns = []
        for color in range(COLORS):
            order = [(color + i) % 3 for i in range(3)]
            held, names = block[None, :, color * part : (color + 1) * part], [0]
            for bit in order:
                held = jnp.concatenate([held, swap(held, 2 << bit)], axis=0)
                names = names + [name ^ (1 << bit) for name in names]
            columns.append((held, names))
        return jnp.stack(
            [
                jnp.concatenate([held[names.index(s)] for held, names in columns], axis=1)
                for s in range(CUBE)
            ]
        )

    def cube_scatter(blocks):
        part = blocks.shape[2] // COLORS
        columns = []
        for color in range(COLORS):
            order = [(color + i) % 3 for i in range(3)]
            held = {s: blocks[s, :, color * part : (color + 1) * part] for s in range(CUBE)}
            for bit in order:
                send = [s for s in held if s & (1 << bit)]
                got = swap(jnp.stack([held[s] for s in send]), 2 << bit)
                for i, s in enumerate(send):
                    held[s ^ (1 << bit)] = held[s ^ (1 << bit)] + got[i]
                    del held[s]
            columns.append(held[0])
        return jnp.concatenate(columns, axis=1)

    def cube_exchange(blocks):
        return jnp.stack([blocks[0]] + [swap(blocks[s], 2 * s) for s in range(1, CUBE)])

    relative = jnp.arange(CUBE, dtype=jnp.int32) ^ place

    def by_place(blocks):
        return jnp.take(blocks, relative, axis=0, indices_are_sorted=False, unique_indices=True)

    def group_gather(block):
        held = jnp.stack([block] + [swap(block, 2 * CUBE * s) for s in range(1, cubes)])
        return jnp.stack([held, swap(held, 1)])

    owner = jnp.arange(n, dtype=jnp.int32)
    from_me = owner ^ me
    owner_entry = ((from_me % 2) * cubes + from_me // (2 * CUBE)) * CUBE + (from_me // 2) % CUBE
    pair = jnp.arange(2 * cubes, dtype=jnp.int32)
    pair_entry = ((pair % 2) ^ core) * cubes + ((pair // 2) ^ cube)

    def all_rows(block):
        held = group_gather(block).reshape(n, *block.shape[1:])
        return jnp.take(held, owner_entry, axis=0, unique_indices=True)

    def lanes(values, start):
        return lax.dynamic_update_slice(jnp.zeros((width,), f32), values.astype(f32), (start,))

    small = jnp.stack(
        [lanes(norm_attn, me * rows), lanes(norm_mlp, me * rows), lanes(lengths[0], me)]
        + [jnp.zeros((width,), f32)] * 5
    )
    cos, sin = rope_tables(slots)
    own_qkv = jnp.concatenate(
        [
            w_query.reshape(rows, CUBE, 2, HEAD),
            w_key.reshape(rows, CUBE, 1, HEAD),
            w_value.reshape(rows, CUBE, 1, HEAD),
        ],
        axis=2,
    )
    own_qkv = jnp.pad(own_qkv, ((0, 0), (0, 0), (0, 0), (0, LANES - HEAD)))
    own_qkv = own_qkv.reshape(rows, CUBE, 4 * LANES).transpose(1, 0, 2)
    ff_cols = 2 * cubes * down_rows

    def by_hidden(weight):
        split = weight.reshape(rows, cubes, CUBE, 2, down_rows)
        return split.transpose(2, 0, 1, 3, 4).reshape(CUBE, rows, ff_cols)

    own_gate_up = jnp.concatenate([by_hidden(w_gate), by_hidden(w_up)], axis=2)
    live = jnp.arange(slots, dtype=jnp.int32)[:, None] < lengths[0, 0]
    cotangent = jnp.where(live, out_cotangent, jnp.zeros_like(out_cotangent))
    inputs = layer_input.astype(f32)

    every = pl.BlockSpec(memory_space=pltpu.VMEM)
    hbm = pl.BlockSpec(memory_space=pl.ANY)
    shapes = [
        ((CUBE, slots, width), bf16),
        ((CUBE, slots, 4 * LANES), f32),
        ((CUBE, slots, 2 * LANES), bf16),
        ((CUBE, slots, 2 * LANES), bf16),
        ((slots, width), f32),
        ((CUBE, slots, width), bf16),
        ((CUBE, slots, width), bf16),
        ((cubes, CUBE, 2, rows, 4 * LANES), bf16),
        ((cubes, 2, 2, 2, 2, rows, width), bf16),
        ((cubes, CUBE, 2, rows, 2 * ff_cols), bf16),
        ((cubes, 2, down_rows, width), bf16),
        ((8, width), f32),
    ]
    messages = 160
    (
        normed_all, qkv, mixed, _, residual, normed_mlp, g_all, w_qkv, full_out, w_gate_up, down,
        gains,
    ) = pl.pallas_call(
        functools.partial(forward_kernel, n),
        out_shape=[jax.ShapeDtypeStruct(*shape) for shape in shapes],
        in_specs=[every, hbm, hbm, hbm, hbm, hbm, every, every, every],
        out_specs=[every] * len(shapes),
        scratch_shapes=[
            pltpu.VMEM((CUBE, slots, width), bf16),
            pltpu.VMEM((n.bit_length() - 1, 8, width), f32),
            pltpu.SemaphoreType.DMA((messages,)),
            pltpu.SemaphoreType.DMA((messages,)),
            pltpu.SemaphoreType.DMA((8,)),
        ],
        compiler_params=pltpu.CompilerParams(
            collective_id=0, has_side_effects=True, vmem_limit_bytes=62 * 1024 * 1024
        ),
    )(layer_input, small, own_qkv, w_out, own_gate_up, w_down, cotangent, cos, sin)
    gain_attn, gain_mlp = gains[0], gains[1]
    there = 2 * CUBE * cube + 2 * relative + core
    cube_lengths = jnp.take(gains[2], there).astype(jnp.int32)
    normed_all = normed_all.reshape(CUBE * slots, width)
    normed_mlp = normed_mlp.reshape(CUBE * slots, width)
    g_all = g_all.reshape(CUBE * slots, width)
    w_qkv = w_qkv.reshape(width, 4 * LANES)
    full_out = full_out.reshape(width, width)
    w_gate_up = w_gate_up.reshape(width, 2 * ff_cols)
    down = down.reshape(ff_cols, width)
    unit_mlp, inv_mlp = rms_parts(residual)

    gate_up = matmul(normed_mlp, w_gate_up)
    gate, up = gate_up[:, :ff_cols], gate_up[:, ff_cols:]
    sigmoid_gate = jax.nn.sigmoid(gate)
    hidden = (gate * sigmoid_gate * up).astype(bf16)
    grad_hidden = contract_last(g_all, down)
    grad_gate = (grad_hidden * up * sigmoid_gate * (1.0 + gate * (1.0 - sigmoid_gate))).astype(bf16)
    grad_up = (grad_hidden * gate * sigmoid_gate).astype(bf16)
    grad_gate_up = jnp.concatenate([grad_gate, grad_up], axis=1)
    grad_normed_mlp = cube_scatter(
        contract_last(grad_gate_up, w_gate_up).reshape(CUBE, slots, width)
    )
    grad_resid = cotangent.astype(f32) + rms_back(grad_normed_mlp, unit_mlp, inv_mlp, gain_mlp)
    grad_resid_low = grad_resid.astype(bf16)

    grad_attended = contract_last(grad_resid_low, full_out).astype(bf16)
    grad_blocks = jnp.pad(
        by_place(grad_attended.reshape(slots, CUBE, q_cols).transpose(1, 0, 2)),
        ((0, 0), (0, 0), (0, 2 * LANES - q_cols)),
    )
    grad_mixed = cube_exchange(grad_blocks)
    grad_qkv = attend_back(cube_lengths, qkv, grad_mixed, cos, sin).reshape(
        CUBE * slots, 4 * LANES
    )

    def low_sum(blocks):
        total = blocks[0]
        for s in range(1, CUBE):
            total = total + swap(blocks[s].astype(bf16), 2 * s).astype(f32)
        return total

    output = (
        residual + low_sum(matmul(hidden, down).reshape(CUBE, slots, width))
    ).astype(bf16)
    grad_normed = low_sum(contract_last(grad_qkv, w_qkv).reshape(CUBE, slots, width))
    unit_attn, inv_attn = rms_parts(inputs)
    grad_input = grad_resid + rms_back(grad_normed, unit_attn, inv_attn, gain_attn)

    def group_sum(blocks, core_axis):
        pick = functools.partial(
            lax.dynamic_index_in_dim, axis=core_axis + 1, keepdims=False
        )
        pair_total = pick(blocks, core) + swap(pick(blocks, 1 - core), 1)
        total = lax.dynamic_index_in_dim(pair_total, cube, axis=0, keepdims=False)
        for s in range(1, cubes):
            send = lax.dynamic_index_in_dim(pair_total, cube ^ s, axis=0, keepdims=False)
            total = total + swap(send.astype(bf16), 2 * CUBE * s).astype(f32)
        return total

    grad_down = group_sum(
        contract_first(hidden, g_all).reshape(cubes, 2, down_rows, width), 0
    )

    def to_owners(partial):
        cols = partial.shape[1]
        total = group_sum(partial.reshape(cubes, CUBE, 2, rows, cols), 1)
        return by_place(cube_exchange(by_place(total.astype(bf16)))).astype(f32)

    grad_gu = to_owners(contract_first(normed_mlp, grad_gate_up))

    def hidden_back(block):
        return block.reshape(CUBE, rows, cubes, 2, down_rows).transpose(1, 2, 0, 3, 4).reshape(
            rows, cubes * CUBE * 2 * down_rows
        )

    grad_w_gate, grad_w_up = hidden_back(grad_gu[:, :, :ff_cols]), hidden_back(grad_gu[:, :, ff_cols:])

    grad_w = to_owners(contract_first(normed_all, grad_qkv))
    grad_heads = grad_w.reshape(CUBE, rows, 4, LANES)[:, :, :, :HEAD].transpose(1, 2, 0, 3)
    grad_w_query = grad_heads[:, :2].transpose(0, 2, 1, 3).reshape(rows, CUBE * q_cols)
    grad_w_key = grad_heads[:, 2].reshape(rows, CUBE * kv_cols)
    grad_w_value = grad_heads[:, 3].reshape(rows, CUBE * kv_cols)

    resid_low_all = cube_gather(grad_resid_low).reshape(CUBE * slots, width)
    grad_out_part = contract_first(mixed.reshape(CUBE * slots, 2 * LANES), resid_low_all)[:q_cols]
    grad_out_sum = group_sum(grad_out_part.reshape(cubes, 2, rows, width), 0)
    moves = [
        (2 * CUBE * g + 2 * t + c, 2 * cubes * t + 2 * g + c)
        for g in range(cubes)
        for t in range(CUBE)
        for c in range(2)
    ]
    grad_w_out = lax.ppermute(grad_out_sum.astype(bf16), "fsdp", moves).astype(f32)

    def gain_grad(gain, pairs):
        total = sum(jnp.sum(weight.astype(f32) * grad, axis=1) for weight, grad in pairs)
        return total / gain.astype(f32)

    gain_attn_grad = gain_grad(
        norm_attn, [(w_query, grad_w_query), (w_key, grad_w_key), (w_value, grad_w_value)]
    )
    gain_mlp_grad = gain_grad(norm_mlp, [(w_gate, grad_w_gate), (w_up, grad_w_up)])
    return (
        output,
        grad_input,
        gain_attn_grad,
        grad_w_query,
        grad_w_key,
        grad_w_value,
        grad_w_out,
        gain_mlp_grad,
        grad_w_gate,
        grad_w_up,
        grad_down,
    )


def solution(mesh):
    n = mesh.shape["fsdp"]
    rows, vec = P("fsdp", None), P("fsdp")
    per_device = per_device_fast if n == 4 * CUBE else per_device_any
    return jax.shard_map(
        functools.partial(per_device, n),
        mesh=mesh,
        in_specs=(rows, rows, rows, vec, rows, rows, rows, rows, vec, rows, rows, rows),
        out_specs=(rows, rows, vec, rows, rows, rows, rows, vec, rows, rows, rows),
        check_vma=False,
    )
```

```python
import functools
import math

import jax
import jax.numpy as jnp
from jax import lax
from jax.experimental import pallas as pl
from jax.experimental.pallas import tpu as pltpu
from jax.sharding import PartitionSpec as P

HEADS = 16
KV_HEADS = 8
HEAD = 96
LANES = 128
CUBE = 8
COLORS = 3

eps_norm = 1e-05
rope_theta = 100000.0
masked_score = -1e30
score_scale = 1.0 / math.sqrt(HEAD)


bf16 = jnp.bfloat16
f32 = jnp.float32


def rope_tables(slot_count):
    half_width = HEAD // 2
    exponent = jnp.arange(half_width, dtype=f32) * (2.0 / HEAD)
    inverse = jnp.exp(-math.log(rope_theta) * exponent)
    angles = jnp.arange(slot_count, dtype=jnp.int32).astype(f32)[:, None] * inverse[None, :]
    pad = jnp.zeros((slot_count, LANES - HEAD), f32)
    cosine_tab = jnp.concatenate([jnp.cos(angles), jnp.cos(angles), pad], axis=-1)
    sine_tab = jnp.concatenate([jnp.sin(angles), jnp.sin(angles), pad], axis=-1)
    return cosine_tab, sine_tab


def rms_parts(values):
    inverse_rms = lax.rsqrt(jnp.mean(values * values, axis=-1, keepdims=True) + eps_norm)
    return values * inverse_rms, inverse_rms


def rms_back(grad_normed, unit_rows, inverse_rms, gain_vec):
    scaled = grad_normed * gain_vec
    return inverse_rms * (scaled - unit_rows * jnp.mean(scaled * unit_rows, axis=-1, keepdims=True))


def contract_last(left_side, right_side):
    return lax.dot_general(
        left_side, right_side, (((1,), (1,)), ((), ())), preferred_element_type=f32
    )


def contract_first(left_side, right_side):
    return lax.dot_general(
        left_side, right_side, (((0,), (0,)), ((), ())), preferred_element_type=f32
    )


def matmul(left_side, right_side):
    return jnp.dot(left_side, right_side, preferred_element_type=f32)


def _rot_half(t, lane):
    return jnp.where(
        lane < HEAD // 2, -pltpu.roll(t, LANES - HEAD // 2, 1), pltpu.roll(t, HEAD // 2, 1)
    )


def _rope(t, cos, sin, lane):
    return t * cos + _rot_half(t, lane) * sin


def _unrope(t, cos, sin, lane):
    return t * cos - _rot_half(t, lane) * sin


def _wide(v):
    return jnp.concatenate([v, jnp.zeros_like(v)], axis=1)


def _weights(q, k, visible, live):
    scores = jnp.where(visible, contract_last(q, k) * score_scale, masked_score)
    exponent = jnp.exp(scores - jnp.max(scores, axis=-1, keepdims=True))
    return jnp.where(live, exponent / jnp.sum(exponent, axis=-1, keepdims=True), 0.0)


def _masks(length, slots):
    row = lax.broadcasted_iota(jnp.int32, (slots, slots), 0)
    col = lax.broadcasted_iota(jnp.int32, (slots, slots), 1)
    live = row < length
    return (col <= row) & live & (col < length), live


def attend_kernel(len_ref, qkv_ref, cos_ref, sin_ref, o_ref):
    length = len_ref[pl.program_id(0)]
    slots = qkv_ref.shape[0]
    visible, live = _masks(length, slots)
    lane = lax.broadcasted_iota(jnp.int32, (slots, LANES), 1)
    cos, sin = cos_ref[...], sin_ref[...]
    k = _rope(qkv_ref[:, 2 * LANES : 3 * LANES], cos, sin, lane).astype(bf16)
    v = qkv_ref[:, 3 * LANES :]
    v_wide = _wide(v)
    mixed = None
    for h in range(2):
        q = _rope(qkv_ref[:, h * LANES : (h + 1) * LANES], cos, sin, lane).astype(bf16)
        weights = _weights(q, k, visible, live).astype(bf16)
        v_h = v_wide if h == 0 else pltpu.roll(v_wide, HEAD, 1)
        part = matmul(weights, v_h.astype(bf16))
        mixed = part if mixed is None else mixed + part
    o_ref[...] = mixed.astype(bf16)


def attend_back_kernel(len_ref, qkv_ref, do_ref, cos_ref, sin_ref, out_ref):
    length = len_ref[pl.program_id(0)]
    slots = qkv_ref.shape[0]
    visible, live = _masks(length, slots)
    lane = lax.broadcasted_iota(jnp.int32, (slots, LANES), 1)
    cos, sin = cos_ref[...], sin_ref[...]
    k = _rope(qkv_ref[:, 2 * LANES : 3 * LANES], cos, sin, lane).astype(bf16)
    v_wide = _wide(qkv_ref[:, 3 * LANES :])
    d_o = do_ref[...]
    grad_k = grad_v = None
    for h in range(2):
        q = _rope(qkv_ref[:, h * LANES : (h + 1) * LANES], cos, sin, lane).astype(bf16)
        weights = _weights(q, k, visible, live)
        v_h = v_wide if h == 0 else pltpu.roll(v_wide, HEAD, 1)
        grad_weights = contract_last(d_o, v_h.astype(bf16))
        row_inner = jnp.sum(weights * grad_weights, axis=-1, keepdims=True)
        grad_scores = (weights * (grad_weights - row_inner)).astype(bf16)
        grad_q = matmul(grad_scores, k) * score_scale
        out_ref[:, h * LANES : (h + 1) * LANES] = _unrope(grad_q, cos, sin, lane).astype(bf16)
        part_k = contract_first(grad_scores, q) * score_scale
        part_v = contract_first(weights.astype(bf16), d_o)
        if h == 1:
            part_v = pltpu.roll(part_v, 2 * LANES - HEAD, 1)
        part_v = part_v[:, :LANES]
        grad_k = part_k if grad_k is None else grad_k + part_k
        grad_v = part_v if grad_v is None else grad_v + part_v
    out_ref[:, 2 * LANES : 3 * LANES] = _unrope(grad_k, cos, sin, lane).astype(bf16)
    out_ref[:, 3 * LANES :] = jnp.where(lane < HEAD, grad_v, 0.0).astype(bf16)


def attend(lengths, qkv, cos, sin):
    blocks, slots, width = qkv.shape
    table = pl.BlockSpec((slots, LANES), lambda s, ln: (0, 0))
    return pl.pallas_call(
        attend_kernel,
        out_shape=jax.ShapeDtypeStruct((blocks, slots, 2 * LANES), bf16),
        grid_spec=pltpu.PrefetchScalarGridSpec(
            num_scalar_prefetch=1,
            grid=(blocks,),
            in_specs=[pl.BlockSpec((None, slots, width), lambda s, ln: (s, 0, 0)), table, table],
            out_specs=pl.BlockSpec((None, slots, 2 * LANES), lambda s, ln: (s, 0, 0)),
        ),
        cost_estimate=pl.CostEstimate(
            flops=blocks * 8 * slots * slots * LANES, bytes_accessed=blocks * slots * width * 6,
            transcendentals=blocks * 2 * slots * slots,
        ),
    )(lengths, qkv, cos, sin)


def attend_back(lengths, qkv, d_o, cos, sin):
    blocks, slots, width = qkv.shape
    table = pl.BlockSpec((slots, LANES), lambda s, ln: (0, 0))
    return pl.pallas_call(
        attend_back_kernel,
        out_shape=jax.ShapeDtypeStruct((blocks, slots, width), bf16),
        grid_spec=pltpu.PrefetchScalarGridSpec(
            num_scalar_prefetch=1,
            grid=(blocks,),
            in_specs=[
                pl.BlockSpec((None, slots, width), lambda s, ln: (s, 0, 0)),
                pl.BlockSpec((None, slots, 2 * LANES), lambda s, ln: (s, 0, 0)),
                table,
                table,
            ],
            out_specs=pl.BlockSpec((None, slots, width), lambda s, ln: (s, 0, 0)),
        ),
        cost_estimate=pl.CostEstimate(
            flops=blocks * 24 * slots * slots * LANES, bytes_accessed=blocks * slots * width * 8,
            transcendentals=blocks * 2 * slots * slots,
        ),
    )(lengths, qkv, d_o, cos, sin)


class Mail:
    def __init__(self, n, send_sems, recv_sems):
        self.me = lax.axis_index("fsdp")
        self.send_sems, self.recv_sems = send_sems, recv_sems
        self.count, self.open = 0, []
        self.peers = {bits: self._peer(bits) for bits in range(1, n)}

    def _peer(self, bits):
        device, bit = self.me, 1
        while bit <= bits:
            if bits & bit:
                device = device + bit * (1 - 2 * ((self.me // bit) % 2))
            bit *= 2
        return device

    def enter(self, bits_list):
        barrier = pltpu.get_barrier_semaphore()
        for bits in bits_list:
            pl.semaphore_signal(
                barrier,
                inc=1,
                device_id=(self.peers[bits],),
                device_id_type=pl.DeviceIdType.MESH,
            )
        pl.semaphore_wait(barrier, len(bits_list))

    def make(self, src, dst, bits):
        copy = pltpu.make_async_remote_copy(
            src_ref=src,
            dst_ref=dst,
            send_sem=self.send_sems.at[self.count],
            recv_sem=self.recv_sems.at[self.count],
            device_id=(self.peers[bits],),
            device_id_type=pl.DeviceIdType.MESH,
        )
        self.count += 1
        self.open.append(copy)
        return copy

    def send(self, src, dst, bits):
        copy = self.make(src, dst, bits)
        copy.start()
        return copy

    def sent(self, copies):
        for copy in copies:
            copy.wait_send()
            self.open = [other for other in self.open if other is not copy]


def take(copies):
    for copy in copies:
        copy.wait_recv()


def xor_place(t, s):
    total = 0
    for bit in (1, 2, 4):
        total = total + bit * (((t // bit) % 2 + (s // bit) % 2) % 2)
    return total


def color_bits(color):
    return [1 << ((color + i) % 3) for i in range(3)]


class Gather:
    def __init__(self, mail, all_ref, own):
        self.mail, self.copies, self.stages = mail, {}, [[], [], []]
        part = all_ref.shape[2] // COLORS
        for i in range(3):
            for color in range(COLORS):
                cols = pl.ds(color * part, part)
                bit = color_bits(color)[i]
                self._make(0, color, bit, own.at[:, cols], all_ref.at[bit, :, cols], bit)
        for color in range(COLORS):
            cols = pl.ds(color * part, part)
            b1, b2, b3 = color_bits(color)
            for stage, slot, bit in (
                (1, b1, b2), (1, b1, b3), (2, b2, b3), (2, b1 ^ b2, b3)
            ):
                src, dst = all_ref.at[slot, :, cols], all_ref.at[slot ^ bit, :, cols]
                self._make(stage, color, slot ^ bit, src, dst, bit)
        for copy in self.stages[0]:
            copy.start()

    def _make(self, stage, color, slot, src, dst, bit):
        self.copies[color, slot] = self.mail.make(src, dst, 2 * bit)
        self.stages[stage].append(self.copies[color, slot])

    def forward(self, stage):
        for color in range(COLORS):
            b1, b2, b3 = color_bits(color)
            for slot in ((b1,), (b2, b1 ^ b2))[stage - 1]:
                self.copies[color, slot].wait_recv()
        for copy in self.stages[stage]:
            copy.start()

    def sent(self):
        self.mail.sent(self.copies.values())

    def near(self):
        for color in range(COLORS):
            self.copies[color, color_bits(color)[2]].wait_recv()

    def far(self):
        for color in range(COLORS):
            b1, b2, b3 = color_bits(color)
            for slot in (b1 ^ b3, b2 ^ b3, 7):
                self.copies[color, slot].wait_recv()


class Scatter:
    def __init__(self, mail, ref, got):
        self.mail, self.ref, self.got, self.copies = mail, ref, got, {}
        self.part = ref.shape[2] // COLORS

    def send(self, color, s):
        bit = [b for b in color_bits(color) if s & b][0]
        cols = pl.ds(color * self.part, self.part)
        self.copies[color, s] = self.mail.send(
            self.ref.at[s, :, cols], self.got.at[s, :, cols], 2 * bit
        )

    def start(self, entries):
        for s in entries:
            for color in range(COLORS):
                if s & color_bits(color)[0]:
                    self.send(color, s)

    def add(self, color, s):
        bit = [b for b in color_bits(color) if s & b][0]
        cols = slice(color * self.part, (color + 1) * self.part)
        self.copies[color, s].wait_recv()
        total = self.ref[s ^ bit, :, cols].astype(f32) + self.got[s, :, cols].astype(f32)
        self.ref[s ^ bit, :, cols] = total.astype(self.ref.dtype)

    def second(self):
        for color in range(COLORS):
            b1, b2, b3 = color_bits(color)
            for rest in (b2, b2 ^ b3):
                self.add(color, b1 ^ rest)
                self.send(color, rest)

    def third(self):
        for color in range(COLORS):
            b1, b2, b3 = color_bits(color)
            self.add(color, b1 ^ b3)
            self.add(color, b2 ^ b3)
            self.send(color, b3)

    def last(self):
        for color in range(COLORS):
            b1, b2, b3 = color_bits(color)
            for s in (b1, b2, b3):
                self.add(color, s)


def lanes_at(values, start, width):
    low = start // LANES * LANES
    high = min(values.shape[1], -(-(start + width) // LANES) * LANES)
    window = values[:, low:high]
    if start > low:
        window = pltpu.roll(window, (high - low) - (start - low), 1)
    return window


def spread(values, width, shift):
    missing = width - values.shape[1]
    if missing > 0:
        values = jnp.concatenate(
            [values, jnp.zeros((values.shape[0], missing), values.dtype)], axis=1
        )
    return pltpu.roll(values, shift, 1) if shift else values


def clear_from(values, lane_count):
    lane = lax.broadcasted_iota(jnp.int32, values.shape, 1)
    return jnp.where(lane < lane_count, values, 0.0)


def heads_of(qkv):
    return [lanes_at(qkv, HEAD * j, HEAD)[:, :LANES] for j in range(4)]


def block_masks(slots, length):
    row = lax.broadcasted_iota(jnp.int32, (slots, slots), 0)
    col = lax.broadcasted_iota(jnp.int32, (slots, slots), 1)
    live = row.astype(f32) < length
    return (col <= row) & live, live


def lane_value(values, index):
    lane = lax.broadcasted_iota(jnp.int32, values.shape, 1)
    return jnp.sum(jnp.where(lane == index, values, 0.0), axis=1, keepdims=True)


def forward_kernel(
    n, x_ref, g_in, len_ref, small_ref, wq_ref, wk_ref, wv_ref, wo_ref, wg_ref, wu_ref, wd_ref,
    cos_ref, sin_ref,
    h1_all, qkv_all, mixed_all, resid, h2_all, wqkv, gains, dx1, dx1_low, d_o, gu_low, wd_grad,
    g_own, pack, gu_pack, wout, wgu, wdown, g_all, small_got, o_slots, hidden, dgu, dh2, got,
    gu_grad, gu_got, gu_send, gu_far, wd_part, wd_got, wd_send, wd_far,
    send_sems, recv_sems, local_sems,
):
    cubes = n // (2 * CUBE)
    mail = Mail(n, send_sems, recv_sems)
    me = mail.me
    core, place, cube = me % 2, (me // 2) % CUBE, me // (2 * CUBE)
    pz, py, px = place // 4, (place // 2) % 2, place % 2
    other_core, other = 1 - core, 1 - cube
    slots, width = x_ref.shape
    rows, down_rows = wo_ref.shape[0], wd_ref.shape[0]
    units = hidden.shape[2]
    far_bits = 2 * CUBE
    mail.enter([2 * s for s in range(1, CUBE)] + [1, far_bits])

    x_mail = Gather(mail, h1_all, x_ref)
    local = [
        pltpu.make_async_copy(wd_ref, wdown.at[cube, core], local_sems.at[0]),
        pltpu.make_async_copy(wo_ref, wout.at[cube, pz, py, px, core], local_sems.at[1]),
    ]
    for copy in local:
        copy.start()
    gains[...] = small_ref[...]
    small_cps = mail.send(small_ref, small_got.at[0], 1)

    query, key, value = (ref[...].astype(f32) for ref in (wq_ref, wk_ref, wv_ref))
    for t in range(CUBE):
        whole = 4 * HEAD
        parts = (
            spread(clear_from(lanes_at(query, 2 * HEAD * t, 2 * HEAD), 2 * HEAD), whole, 0)
            + spread(clear_from(lanes_at(key, HEAD * t, HEAD), HEAD), whole, 2 * HEAD)
            + spread(clear_from(lanes_at(value, HEAD * t, HEAD), HEAD), whole, 3 * HEAD)
        )
        pack[t] = parts.astype(bf16)
    wqkv[cube, place, core] = pack[place]
    pack_cps = [
        mail.send(pack.at[xor_place(place, s)], wqkv.at[cube, place, core], 2 * s)
        for s in range(1, CUBE)
    ]
    wo_cps = mail.send(wo_ref, wout.at[cube, pz, py, px, core], far_bits)

    for t in range(CUBE):
        for i in range(2 * cubes):
            start = (((i // 2) * CUBE + t) * 2 + i % 2) * down_rows
            cols = slice(start, start + down_rows)
            gu_pack[t, :, i * down_rows : (i + 1) * down_rows] = wg_ref[:, cols]
            gu_pack[t, :, units + i * down_rows : units + (i + 1) * down_rows] = wu_ref[:, cols]
    wgu[cube, place, core] = gu_pack[place]
    row = lax.broadcasted_iota(jnp.int32, (slots, width), 0)
    g_own[...] = jnp.where(row < len_ref[0, 0], g_in[...].astype(f32), 0.0).astype(bf16)
    g_all[0] = g_own[...]

    for i in range(1, n.bit_length() - 1):
        small_cps.wait_recv()
        mail.sent([small_cps])
        gains[...] += small_got[i - 1]
        small_cps = mail.send(gains, small_got.at[i], 1 << i)
    take(pack_cps)
    pack_far = mail.send(wqkv.at[cube, :, core], wqkv.at[cube, :, core], far_bits)
    pack_core = [mail.send(wqkv.at[cube, :, core], wqkv.at[cube, :, core], 1)]
    x_mail.forward(1)
    small_cps.wait_recv()
    mail.sent([small_cps])
    gains[...] += small_got[n.bit_length() - 2]
    gu_cps = [
        mail.send(gu_pack.at[xor_place(place, s)], wgu.at[cube, place, core], 2 * s)
        for s in range(1, CUBE)
    ]
    x_mail.forward(2)
    local[1].wait()
    wo_cps.wait_recv()
    wo_z = mail.send(wout.at[:, pz, py, px, core], wout.at[:, pz, py, px, core], 8)
    g_mail = Gather(mail, g_all, g_own)
    pack_far.wait_recv()
    pack_core.append(mail.send(wqkv.at[other, :, core], wqkv.at[other, :, core], 1))
    x_mail.near()
    x_mail.far()
    take(pack_core)
    x_mail.sent()
    h1_all[0] = x_ref[...]
    gain_attn, gain_mlp, lengths = gains[0:1, :], gains[1:2, :], gains[2:3, :]

    wo_y = mail.make(wout.at[:, :, py, px, core], wout.at[:, :, py, px, core], 4)
    wo_x = mail.make(wout.at[:, :, :, px, core], wout.at[:, :, :, px, core], 2)
    wo_c = mail.make(wout.at[:, :, :, :, core], wout.at[:, :, :, :, core], 1)
    gu_out = mail.make(wgu.at[cube, :, core], wgu.at[cube, :, core], far_bits)
    wd_out = mail.make(wd_ref, wdown.at[cube, core], far_bits)

    def attention(s, carry):
        values = h1_all[s].astype(f32)
        normed = (rms_parts(values)[0] * gain_attn).astype(bf16)
        h1_all[s] = normed
        qkv_all[s] = matmul(normed, wqkv[...].reshape(width, 4 * HEAD))
        there = far_bits * cube + 2 * xor_place(place, s) + core
        visible, live = block_masks(slots, lane_value(lengths, there))
        lane = lax.broadcasted_iota(jnp.int32, (slots, LANES), 1)
        cos, sin = cos_ref[...], sin_ref[...]
        q0, q1, k, v = heads_of(qkv_all[s])
        k = _rope(k, cos, sin, lane).astype(bf16)
        v_wide = _wide(clear_from(v, HEAD))
        mixed = None
        for h, q in enumerate((q0, q1)):
            q = _rope(q, cos, sin, lane).astype(bf16)
            weights = _weights(q, k, visible, live).astype(bf16)
            v_h = pltpu.roll(v_wide, HEAD, 1) if h else v_wide
            part = matmul(weights, v_h.astype(bf16))
            mixed = part if mixed is None else mixed + part
        mixed_all[s] = mixed.astype(bf16)

        @pl.when(s == 0)
        def _():
            wo_z.wait_recv()
            wo_y.start()

        @pl.when(s == 1)
        def _():
            take(gu_cps)
            gu_out.start()

        @pl.when(s == 2)
        def _():
            wd_out.start()
            g_mail.forward(1)

        @pl.when(s == 4)
        def _():
            wo_y.wait_recv()
            wo_x.start()

        @pl.when(s == 5)
        def _():
            g_mail.forward(2)

        @pl.when(s == 7)
        def _():
            wo_x.wait_recv()
            wo_c.start()

        return carry

    lax.fori_loop(0, CUBE, attention, 0)

    o_cps = [mail.send(mixed_all.at[s], o_slots.at[place], 2 * s) for s in range(1, CUBE)]
    o_slots[place] = mixed_all[0]
    local[0].wait()
    wd_out.wait_recv()
    wd_core = mail.send(wdown.at[:, core], wdown.at[:, core], 1)
    take(o_cps)
    wide = []
    for j in range(CUBE // 2):
        low = spread(o_slots[2 * j].astype(f32), 3 * LANES, 0)
        high = spread(o_slots[2 * j + 1].astype(f32), 3 * LANES, 2 * HEAD)
        wide.append((low + high).astype(bf16))
    attended = jnp.concatenate(wide, axis=1)
    wo_c.wait_recv()
    step = 256
    for j in range(width // step):
        cols = slice(j * step, (j + 1) * step)
        weight = wout[:, :, :, :, :, :, cols].reshape(width, step)
        resid[:, cols] = x_ref[:, cols].astype(f32) + matmul(attended, weight)
    h2_all[0] = (rms_parts(resid[...])[0] * gain_mlp).astype(bf16)
    h2_mail = Gather(mail, h2_all, h2_all.at[0])
    g_mail.near()
    g_mail.far()
    h2_mail.forward(1)
    wd_core.wait_recv()
    gu_out.wait_recv()
    gu_core = mail.send(wgu.at[:, :, core], wgu.at[:, :, core], 1)
    h2_mail.forward(2)
    h2_mail.near()
    gu_core.wait_recv()

    def blocks(ref, group, cols=slice(None)):
        return jnp.concatenate([ref[s, :, cols] for s in group], axis=0)

    back = Scatter(mail, dh2, got)

    def feed_forward(group):
        step = 256
        for j in range(units // step):
            cols, up_cols = slice(j * step, (j + 1) * step), slice(units + j * step, units + (j + 1) * step)
            lhs = blocks(h2_all, group)
            gate = matmul(lhs, wgu[:, :, :, :, cols].reshape(width, step))
            up = matmul(lhs, wgu[:, :, :, :, up_cols].reshape(width, step))
            down = wdown[...].reshape(units, width)[cols]
            grad_hidden = contract_last(blocks(g_all, group), down)
            sigmoid_gate = jax.nn.sigmoid(gate)
            silu = gate * sigmoid_gate
            hid = (silu * up).astype(bf16)
            d_gate = (
                grad_hidden * up * sigmoid_gate * (1.0 + gate * (1.0 - sigmoid_gate))
            ).astype(bf16)
            d_up = (grad_hidden * silu).astype(bf16)
            for i, s in enumerate(group):
                part = slice(i * slots, (i + 1) * slots)
                hidden[s, :, cols] = hid[part]
                dgu[s, :, cols] = d_gate[part]
                dgu[s, :, up_cols] = d_up[part]
        for j in range(2):
            part = width // 2
            grad = contract_last(blocks(dgu, group), wgu[j].reshape(part, 2 * units))
            for i, s in enumerate(group):
                dh2[s, :, j * part : (j + 1) * part] = grad[i * slots : (i + 1) * slots]
        back.start(group)

    feed_forward((0, 1, 2, 4))
    h2_mail.far()
    feed_forward((3, 5, 6, 7))

    d_all = dgu[...].reshape(CUBE * slots, 2 * units)
    chunk = width // 4
    for j in range(4):
        lhs = h2_all[:, :, j * chunk : (j + 1) * chunk].reshape(CUBE * slots, chunk)
        gu_grad[j // 2, j % 2] = contract_first(lhs, d_all).reshape(gu_grad.shape[2:])
    gu_cps = mail.send(gu_grad.at[:, :, :, other_core], gu_got, 1)
    hid_all = hidden[...].reshape(CUBE * slots, units)
    for j in range(4):
        cols = slice(j * chunk, (j + 1) * chunk)
        g_cols = g_all[:, :, cols].reshape(CUBE * slots, chunk)
        wd_part[:, :, :, cols] = contract_first(hid_all, g_cols).reshape(cubes, 2, down_rows, chunk)
    wd_cps = mail.send(wd_part.at[:, other_core], wd_got, 1)
    back.second()
    gu_cps.wait_recv()
    gu_send[...] = (gu_grad[other, :, :, core] + gu_got[other]).astype(bf16)
    gu_cps = mail.send(gu_send, gu_far, far_bits)
    wd_cps.wait_recv()
    wd_send[...] = (wd_part[other, core] + wd_got[other]).astype(bf16)
    wd_cps = mail.send(wd_send, wd_far, far_bits)
    back.third()
    h2_mail.sent()
    for i in range(2):
        half = slice(i * CUBE // 2, (i + 1) * CUBE // 2)
        lhs = hidden[half].reshape(CUBE // 2 * slots, units)
        part = matmul(lhs, wdown[...].reshape(units, width))
        h2_all[half] = part.reshape(CUBE // 2, slots, width).astype(bf16)
    back.last()

    unit, inverse = rms_parts(resid[...])
    dx1[...] = g_own[...].astype(f32) + rms_back(dh2[0], unit, inverse, gain_mlp)
    dx1_low[...] = dx1[...].astype(bf16)
    low = dx1_low[...]
    for t in range(CUBE):
        weight = wout[t // 4, (t // 2) % 2, t % 2].reshape(2 * HEAD, width)
        d_o[t] = spread(contract_last(low, weight), 2 * LANES, 0).astype(bf16)
    gu_cps.wait_recv()
    gu_low[...] = (
        gu_grad[cube, :, :, core] + gu_got[cube] + gu_far[...].astype(f32)
    ).astype(bf16)
    wd_cps.wait_recv()
    wd_grad[...] = wd_part[cube, core] + wd_got[cube] + wd_far[...].astype(f32)
    mail.sent(mail.open)


def per_device_any(
    n,
    layer_input,
    out_cotangent,
    lengths,
    norm_attn,
    w_query,
    w_key,
    w_value,
    w_out,
    norm_mlp,
    w_gate,
    w_up,
    w_down,
):
    cubes = n // (2 * CUBE)
    slots, width = layer_input.shape
    rows = w_query.shape[0]
    down_rows = w_down.shape[0]
    q_cols, kv_cols = w_query.shape[1] // CUBE, w_key.shape[1] // CUBE
    me = lax.axis_index("fsdp")
    core, place, cube = me % 2, (me // 2) % CUBE, me // (2 * CUBE)

    def swap(array, bits):
        return lax.ppermute(array, "fsdp", [(i, i ^ bits) for i in range(n)])

    def cube_gather(block):
        part = block.shape[1] // COLORS
        columns = []
        for color in range(COLORS):
            order = [(color + i) % 3 for i in range(3)]
            held, names = block[None, :, color * part : (color + 1) * part], [0]
            for bit in order:
                held = jnp.concatenate([held, swap(held, 2 << bit)], axis=0)
                names = names + [name ^ (1 << bit) for name in names]
            columns.append((held, names))
        return jnp.stack(
            [
                jnp.concatenate([held[names.index(s)] for held, names in columns], axis=1)
                for s in range(CUBE)
            ]
        )

    def cube_scatter(blocks):
        part = blocks.shape[2] // COLORS
        columns = []
        for color in range(COLORS):
            order = [(color + i) % 3 for i in range(3)]
            held = {s: blocks[s, :, color * part : (color + 1) * part] for s in range(CUBE)}
            for bit in order:
                send = [s for s in held if s & (1 << bit)]
                got = swap(jnp.stack([held[s] for s in send]), 2 << bit)
                for i, s in enumerate(send):
                    held[s ^ (1 << bit)] = held[s ^ (1 << bit)] + got[i]
                    del held[s]
            columns.append(held[0])
        return jnp.concatenate(columns, axis=1)

    def cube_exchange(blocks):
        return jnp.stack([blocks[0]] + [swap(blocks[s], 2 * s) for s in range(1, CUBE)])

    relative = jnp.arange(CUBE, dtype=jnp.int32) ^ place

    def by_place(blocks):
        return jnp.take(blocks, relative, axis=0, indices_are_sorted=False, unique_indices=True)

    def group_gather(block):
        held = jnp.stack([block] + [swap(block, 2 * CUBE * s) for s in range(1, cubes)])
        return jnp.stack([held, swap(held, 1)])

    owner = jnp.arange(n, dtype=jnp.int32)
    from_me = owner ^ me
    owner_entry = ((from_me % 2) * cubes + from_me // (2 * CUBE)) * CUBE + (from_me // 2) % CUBE
    pair = jnp.arange(2 * cubes, dtype=jnp.int32)
    pair_entry = ((pair % 2) ^ core) * cubes + ((pair // 2) ^ cube)

    def all_rows(block):
        held = group_gather(block).reshape(n, *block.shape[1:])
        return jnp.take(held, owner_entry, axis=0, unique_indices=True)

    small = jnp.concatenate(
        [norm_attn, norm_mlp, lengths[0].astype(bf16), jnp.zeros((LANES - 2 * rows - 1,), bf16)]
    )[None]
    bit = 1
    while bit < n:
        small = jnp.concatenate([small, swap(small, bit)], axis=0)
        bit *= 2
    cube_lengths = small[0 : 2 * CUBE : 2, 2 * rows].astype(jnp.int32)
    gains = jnp.take(small, from_me, axis=0)
    gain_attn = gains[:, :rows].reshape(width).astype(f32)
    gain_mlp = gains[:, rows : 2 * rows].reshape(width).astype(f32)
    cos, sin = rope_tables(slots)

    x_all = cube_gather(layer_input)
    own_qkv = jnp.concatenate(
        [
            w_query.reshape(rows, CUBE, q_cols),
            w_key.reshape(rows, CUBE, kv_cols),
            w_value.reshape(rows, CUBE, kv_cols),
        ],
        axis=2,
    ).transpose(1, 0, 2)
    w_qkv = all_rows(cube_exchange(by_place(own_qkv))).reshape(width, q_cols + 2 * kv_cols)
    w_qkv = jnp.pad(
        w_qkv.reshape(width, 4, HEAD), ((0, 0), (0, 0), (0, LANES - HEAD))
    ).reshape(width, 4 * LANES)

    out_held = jnp.stack([w_out] + [swap(w_out, 2 * CUBE * s) for s in range(1, cubes)])
    out_held = out_held.reshape(1, cubes, rows, width)
    for bit in range(3):
        out_held = jnp.concatenate([out_held, swap(out_held, 2 << bit)], axis=0)
    out_held = jnp.stack([out_held, swap(out_held, 1)])
    out_entry = ((from_me % 2) * CUBE + (from_me // 2) % CUBE) * cubes + from_me // (2 * CUBE)
    full_out = jnp.take(out_held.reshape(n, rows, width), out_entry, axis=0, unique_indices=True)
    full_out = jnp.pad(
        full_out.reshape(CUBE, q_cols, width), ((0, 0), (0, 2 * LANES - q_cols), (0, 0))
    ).reshape(CUBE * 2 * LANES, width)

    ff_cols = 2 * cubes * down_rows

    def by_hidden(weight):
        split = weight.reshape(rows, cubes, CUBE, 2, down_rows)
        return split.transpose(2, 0, 1, 3, 4).reshape(CUBE, rows, ff_cols)

    own_gate_up = jnp.concatenate([by_hidden(w_gate), by_hidden(w_up)], axis=2)
    w_gate_up = all_rows(cube_exchange(by_place(own_gate_up))).reshape(width, 2 * ff_cols)
    down_held = group_gather(w_down).reshape(2 * cubes, down_rows, width)
    down = jnp.take(down_held, pair_entry, axis=0, unique_indices=True).reshape(ff_cols, width)

    live = jnp.arange(slots, dtype=jnp.int32)[:, None] < lengths[0, 0]
    cotangent = jnp.where(live, out_cotangent, jnp.zeros_like(out_cotangent))
    g_all = cube_gather(cotangent).reshape(CUBE * slots, width)

    inputs = layer_input.astype(f32)
    unit_all, _ = rms_parts(x_all.reshape(CUBE * slots, width).astype(f32))
    normed_all = (unit_all * gain_attn).astype(bf16)
    qkv = matmul(normed_all, w_qkv).reshape(CUBE, slots, 4 * LANES)
    mixed = attend(cube_lengths, qkv, cos, sin)
    attended = by_place(cube_exchange(mixed)).transpose(1, 0, 2).reshape(slots, CUBE * 2 * LANES)
    residual = inputs + matmul(attended, full_out)
    unit_mlp, inv_mlp = rms_parts(residual)
    normed_mlp = cube_gather((unit_mlp * gain_mlp).astype(bf16)).reshape(CUBE * slots, width)

    gate_up = matmul(normed_mlp, w_gate_up)
    gate, up = gate_up[:, :ff_cols], gate_up[:, ff_cols:]
    sigmoid_gate = jax.nn.sigmoid(gate)
    hidden = (gate * sigmoid_gate * up).astype(bf16)
    grad_hidden = contract_last(g_all, down)
    grad_gate = (grad_hidden * up * sigmoid_gate * (1.0 + gate * (1.0 - sigmoid_gate))).astype(bf16)
    grad_up = (grad_hidden * gate * sigmoid_gate).astype(bf16)
    grad_gate_up = jnp.concatenate([grad_gate, grad_up], axis=1)
    grad_normed_mlp = cube_scatter(
        contract_last(grad_gate_up, w_gate_up).reshape(CUBE, slots, width)
    )
    grad_resid = cotangent.astype(f32) + rms_back(grad_normed_mlp, unit_mlp, inv_mlp, gain_mlp)
    grad_resid_low = grad_resid.astype(bf16)

    grad_attended = contract_last(grad_resid_low, full_out).astype(bf16)
    grad_blocks = by_place(grad_attended.reshape(slots, CUBE, 2 * LANES).transpose(1, 0, 2))
    grad_mixed = cube_exchange(grad_blocks)
    grad_qkv = attend_back(cube_lengths, qkv, grad_mixed, cos, sin).reshape(
        CUBE * slots, 4 * LANES
    )

    def low_sum(blocks):
        total = blocks[0]
        for s in range(1, CUBE):
            total = total + swap(blocks[s].astype(bf16), 2 * s).astype(f32)
        return total

    output = (
        residual + low_sum(matmul(hidden, down).reshape(CUBE, slots, width))
    ).astype(bf16)
    grad_normed = low_sum(contract_last(grad_qkv, w_qkv).reshape(CUBE, slots, width))
    unit_attn, inv_attn = rms_parts(inputs)
    grad_input = grad_resid + rms_back(grad_normed, unit_attn, inv_attn, gain_attn)

    def group_sum(blocks, core_axis):
        pick = functools.partial(
            lax.dynamic_index_in_dim, axis=core_axis + 1, keepdims=False
        )
        pair_total = pick(blocks, core) + swap(pick(blocks, 1 - core), 1)
        total = lax.dynamic_index_in_dim(pair_total, cube, axis=0, keepdims=False)
        for s in range(1, cubes):
            send = lax.dynamic_index_in_dim(pair_total, cube ^ s, axis=0, keepdims=False)
            total = total + swap(send.astype(bf16), 2 * CUBE * s).astype(f32)
        return total

    grad_down = group_sum(
        contract_first(hidden, g_all).reshape(cubes, 2, down_rows, width), 0
    )

    def to_owners(partial):
        cols = partial.shape[1]
        total = group_sum(partial.reshape(cubes, CUBE, 2, rows, cols), 1)
        return by_place(cube_exchange(by_place(total.astype(bf16)))).astype(f32)

    grad_gu = to_owners(contract_first(normed_mlp, grad_gate_up))

    def hidden_back(block):
        return block.reshape(CUBE, rows, cubes, 2, down_rows).transpose(1, 2, 0, 3, 4).reshape(
            rows, cubes * CUBE * 2 * down_rows
        )

    grad_w_gate, grad_w_up = hidden_back(grad_gu[:, :, :ff_cols]), hidden_back(grad_gu[:, :, ff_cols:])

    grad_w = to_owners(contract_first(normed_all, grad_qkv))
    grad_heads = grad_w.reshape(CUBE, rows, 4, LANES)[:, :, :, :HEAD].transpose(1, 2, 0, 3)
    grad_w_query = grad_heads[:, :2].transpose(0, 2, 1, 3).reshape(rows, CUBE * q_cols)
    grad_w_key = grad_heads[:, 2].reshape(rows, CUBE * kv_cols)
    grad_w_value = grad_heads[:, 3].reshape(rows, CUBE * kv_cols)

    resid_low_all = cube_gather(grad_resid_low).reshape(CUBE * slots, width)
    grad_out_part = contract_first(mixed.reshape(CUBE * slots, 2 * LANES), resid_low_all)[:q_cols]
    grad_out_sum = group_sum(grad_out_part.reshape(cubes, 2, rows, width), 0)
    moves = [
        (2 * CUBE * g + 2 * t + c, 2 * cubes * t + 2 * g + c)
        for g in range(cubes)
        for t in range(CUBE)
        for c in range(2)
    ]
    grad_w_out = lax.ppermute(grad_out_sum.astype(bf16), "fsdp", moves).astype(f32)

    def gain_grad(gain, pairs):
        total = sum(jnp.sum(weight.astype(f32) * grad, axis=1) for weight, grad in pairs)
        return total / gain.astype(f32)

    gain_attn_grad = gain_grad(
        norm_attn, [(w_query, grad_w_query), (w_key, grad_w_key), (w_value, grad_w_value)]
    )
    gain_mlp_grad = gain_grad(norm_mlp, [(w_gate, grad_w_gate), (w_up, grad_w_up)])
    return (
        output,
        grad_input,
        gain_attn_grad,
        grad_w_query,
        grad_w_key,
        grad_w_value,
        grad_w_out,
        gain_mlp_grad,
        grad_w_gate,
        grad_w_up,
        grad_down,
    )


def per_device_fast(
    n,
    layer_input,
    out_cotangent,
    lengths,
    norm_attn,
    w_query,
    w_key,
    w_value,
    w_out,
    norm_mlp,
    w_gate,
    w_up,
    w_down,
):
    cubes = n // (2 * CUBE)
    slots, width = layer_input.shape
    rows = w_query.shape[0]
    down_rows = w_down.shape[0]
    q_cols, kv_cols = w_query.shape[1] // CUBE, w_key.shape[1] // CUBE
    me = lax.axis_index("fsdp")
    core, place, cube = me % 2, (me // 2) % CUBE, me // (2 * CUBE)

    def swap(array, bits):
        return lax.ppermute(array, "fsdp", [(i, i ^ bits) for i in range(n)])

    def cube_gather(block):
        part = block.shape[1] // COLORS
        columns = []
        for color in range(COLORS):
            order = [(color + i) % 3 for i in range(3)]
            held, names = block[None, :, color * part : (color + 1) * part], [0]
            for bit in order:
                held = jnp.concatenate([held, swap(held, 2 << bit)], axis=0)
                names = names + [name ^ (1 << bit) for name in names]
            columns.append((held, names))
        return jnp.stack(
            [
                jnp.concatenate([held[names.index(s)] for held, names in columns], axis=1)
                for s in range(CUBE)
            ]
        )

    def cube_scatter(blocks):
        part = blocks.shape[2] // COLORS
        columns = []
        for color in range(COLORS):
            order = [(color + i) % 3 for i in range(3)]
            held = {s: blocks[s, :, color * part : (color + 1) * part] for s in range(CUBE)}
            for bit in order:
                send = [s for s in held if s & (1 << bit)]
                got = swap(jnp.stack([held[s] for s in send]), 2 << bit)
                for i, s in enumerate(send):
                    held[s ^ (1 << bit)] = held[s ^ (1 << bit)] + got[i]
                    del held[s]
            columns.append(held[0])
        return jnp.concatenate(columns, axis=1)

    def cube_exchange(blocks):
        return jnp.stack([blocks[0]] + [swap(blocks[s], 2 * s) for s in range(1, CUBE)])

    relative = jnp.arange(CUBE, dtype=jnp.int32) ^ place

    def by_place(blocks):
        return jnp.take(blocks, relative, axis=0, indices_are_sorted=False, unique_indices=True)

    def group_gather(block):
        held = jnp.stack([block] + [swap(block, 2 * CUBE * s) for s in range(1, cubes)])
        return jnp.stack([held, swap(held, 1)])

    owner = jnp.arange(n, dtype=jnp.int32)
    from_me = owner ^ me
    owner_entry = ((from_me % 2) * cubes + from_me // (2 * CUBE)) * CUBE + (from_me // 2) % CUBE
    pair = jnp.arange(2 * cubes, dtype=jnp.int32)
    pair_entry = ((pair % 2) ^ core) * cubes + ((pair // 2) ^ cube)

    def all_rows(block):
        held = group_gather(block).reshape(n, *block.shape[1:])
        return jnp.take(held, owner_entry, axis=0, unique_indices=True)

    lane_owner = jnp.arange(width, dtype=jnp.int32)[None] // rows
    small = jnp.where(lane_owner == me, jnp.tile(jnp.stack([norm_attn, norm_mlp]), (1, n)), 0)
    length_row = jnp.where(jnp.arange(width)[None] == me, lengths, 0)
    small = jnp.concatenate(
        [small.astype(f32), length_row.astype(f32), jnp.zeros((5, width), f32)]
    )
    cos, sin = rope_tables(slots)
    units = 2 * cubes * down_rows
    inputs = layer_input.astype(f32)
    live = jnp.arange(slots, dtype=jnp.int32)[:, None] < lengths[0, 0]

    vmem = pl.BlockSpec(memory_space=pltpu.VMEM)
    smem = pl.BlockSpec(memory_space=pltpu.SMEM)
    hbm = pl.BlockSpec(memory_space=pl.ANY)
    qkv_cols = 4 * HEAD
    outs = [
        ((CUBE, slots, width), bf16),
        ((CUBE, slots, qkv_cols), f32),
        ((CUBE, slots, 2 * LANES), bf16),
        ((slots, width), f32),
        ((CUBE, slots, width), bf16),
        ((cubes, CUBE, 2, rows, qkv_cols), bf16),
        ((8, width), f32),
        ((slots, width), f32),
        ((slots, width), bf16),
        ((CUBE, slots, 2 * LANES), bf16),
        ((2, CUBE // 2, rows, 2 * units), bf16),
        ((down_rows, width), f32),
    ]
    gu_half = (cubes, 2, CUBE // 2, rows, 2 * units)
    scratch = [
        ((slots, width), bf16),
        ((CUBE, rows, qkv_cols), bf16),
        ((CUBE, rows, 2 * units), bf16),
        ((cubes, 2, 2, 2, 2, rows, width), bf16),
        ((cubes, CUBE, 2, rows, 2 * units), bf16),
        ((cubes, 2, down_rows, width), bf16),
        ((CUBE, slots, width), bf16),
        ((n.bit_length() - 1, 8, width), f32),
        ((CUBE, slots, 2 * LANES), bf16),
        ((CUBE, slots, units), bf16),
        ((CUBE, slots, 2 * units), bf16),
        ((CUBE, slots, width), f32),
        ((CUBE, slots, width), f32),
        ((cubes, 2, CUBE // 2, 2, rows, 2 * units), f32),
        (gu_half, f32),
        (gu_half[1:], bf16),
        (gu_half[1:], bf16),
        ((cubes, 2, down_rows, width), f32),
        ((cubes, down_rows, width), f32),
        ((down_rows, width), bf16),
        ((down_rows, width), bf16),
    ]
    messages = 160
    (
        normed_all, qkv, mixed, residual, out_part, w_qkv, gains, grad_resid, grad_resid_low, d_o,
        gu_low, grad_down,
    ) = pl.pallas_call(
        functools.partial(forward_kernel, n),
        out_shape=[jax.ShapeDtypeStruct(*shape) for shape in outs],
        in_specs=[vmem, vmem, smem, vmem, vmem, vmem, vmem, hbm, vmem, vmem, hbm, vmem, vmem],
        out_specs=[vmem] * len(outs),
        scratch_shapes=[pltpu.VMEM(*shape) for shape in scratch]
        + [
            pltpu.SemaphoreType.DMA((messages,)),
            pltpu.SemaphoreType.DMA((messages,)),
            pltpu.SemaphoreType.DMA((2,)),
        ],
        compiler_params=pltpu.CompilerParams(
            collective_id=0, has_side_effects=True, vmem_limit_bytes=67043328
        ),
    )(
        layer_input, out_cotangent, lengths, small, w_query, w_key, w_value, w_out, w_gate, w_up,
        w_down, cos, sin,
    )
    gain_attn, gain_mlp = gains[0], gains[1]
    there = 2 * CUBE * cube + 2 * relative + core
    cube_lengths = jnp.take(gains[2], there).astype(jnp.int32)
    normed_all = normed_all.reshape(CUBE * slots, width)
    def padded(a):
        a = a.reshape(*a.shape[:-1], 4, HEAD)
        a = jnp.pad(a, ((0, 0),) * (a.ndim - 1) + ((0, LANES - HEAD),))
        return a.reshape(*a.shape[:-2], 4 * LANES)
    w_qkv = padded(w_qkv.reshape(width, qkv_cols))
    qkv = padded(qkv)
    ff_cols = units

    grad_blocks = by_place(d_o)
    grad_mixed = cube_exchange(grad_blocks)
    grad_qkv = attend_back(cube_lengths, qkv, grad_mixed, cos, sin).reshape(
        CUBE * slots, 4 * LANES
    )

    def low_sum(blocks):
        total = blocks[0]
        for s in range(1, CUBE):
            total = total + swap(blocks[s].astype(bf16), 2 * s).astype(f32)
        return total

    output = (
        residual + low_sum(out_part)
    ).astype(bf16)
    grad_normed = low_sum(contract_last(grad_qkv, w_qkv).reshape(CUBE, slots, width))
    unit_attn, inv_attn = rms_parts(inputs)
    grad_input = grad_resid + rms_back(grad_normed, unit_attn, inv_attn, gain_attn)

    def group_sum(blocks, core_axis):
        pick = functools.partial(
            lax.dynamic_index_in_dim, axis=core_axis + 1, keepdims=False
        )
        pair_total = pick(blocks, core) + swap(pick(blocks, 1 - core), 1)
        total = lax.dynamic_index_in_dim(pair_total, cube, axis=0, keepdims=False)
        for s in range(1, cubes):
            send = lax.dynamic_index_in_dim(pair_total, cube ^ s, axis=0, keepdims=False)
            total = total + swap(send.astype(bf16), 2 * CUBE * s).astype(f32)
        return total

    def to_owners(partial):
        cols = partial.shape[1]
        total = group_sum(partial.reshape(cubes, CUBE, 2, rows, cols), 1)
        return by_place(cube_exchange(by_place(total.astype(bf16)))).astype(f32)

    grad_gu = by_place(cube_exchange(by_place(gu_low.reshape(CUBE, rows, 2 * units)))).astype(f32)

    def hidden_back(block):
        return block.reshape(CUBE, rows, cubes, 2, down_rows).transpose(1, 2, 0, 3, 4).reshape(
            rows, cubes * CUBE * 2 * down_rows
        )

    grad_w_gate, grad_w_up = hidden_back(grad_gu[:, :, :ff_cols]), hidden_back(grad_gu[:, :, ff_cols:])

    grad_w = to_owners(contract_first(normed_all, grad_qkv))
    grad_heads = grad_w.reshape(CUBE, rows, 4, LANES)[:, :, :, :HEAD].transpose(1, 2, 0, 3)
    grad_w_query = grad_heads[:, :2].transpose(0, 2, 1, 3).reshape(rows, CUBE * q_cols)
    grad_w_key = grad_heads[:, 2].reshape(rows, CUBE * kv_cols)
    grad_w_value = grad_heads[:, 3].reshape(rows, CUBE * kv_cols)

    resid_low_all = cube_gather(grad_resid_low).reshape(CUBE * slots, width)
    grad_out_part = contract_first(mixed.reshape(CUBE * slots, 2 * LANES), resid_low_all)[:q_cols]
    grad_out_sum = group_sum(grad_out_part.reshape(cubes, 2, rows, width), 0)
    moves = [
        (2 * CUBE * g + 2 * t + c, 2 * cubes * t + 2 * g + c)
        for g in range(cubes)
        for t in range(CUBE)
        for c in range(2)
    ]
    grad_w_out = lax.ppermute(grad_out_sum.astype(bf16), "fsdp", moves).astype(f32)

    def gain_grad(gain, pairs):
        total = sum(jnp.sum(weight.astype(f32) * grad, axis=1) for weight, grad in pairs)
        return total / gain.astype(f32)

    gain_attn_grad = gain_grad(
        norm_attn, [(w_query, grad_w_query), (w_key, grad_w_key), (w_value, grad_w_value)]
    )
    gain_mlp_grad = gain_grad(norm_mlp, [(w_gate, grad_w_gate), (w_up, grad_w_up)])
    return (
        output,
        grad_input,
        gain_attn_grad,
        grad_w_query,
        grad_w_key,
        grad_w_value,
        grad_w_out,
        gain_mlp_grad,
        grad_w_gate,
        grad_w_up,
        grad_down,
    )


def solution(mesh):
    n = mesh.shape["fsdp"]
    rows, vec = P("fsdp", None), P("fsdp")
    per_device = per_device_fast if n == 4 * CUBE else per_device_any
    return jax.shard_map(
        functools.partial(per_device, n),
        mesh=mesh,
        in_specs=(rows, rows, rows, vec, rows, rows, rows, rows, vec, rows, rows, rows),
        out_specs=(rows, rows, vec, rows, rows, rows, rows, vec, rows, rows, rows),
        check_vma=False,
    )
```

```python
import functools
import math

import jax
import jax.numpy as jnp
from jax import lax
from jax.experimental import pallas as pl
from jax.experimental.pallas import tpu as pltpu
from jax.sharding import PartitionSpec as P

HEADS = 16
KV_HEADS = 8
HEAD = 96
LANES = 128
CUBE = 8
COLORS = 3

eps_norm = 1e-05
rope_theta = 100000.0
masked_score = -1e30
score_scale = 1.0 / math.sqrt(HEAD)


bf16 = jnp.bfloat16
f32 = jnp.float32


def rope_tables(slot_count):
    half_width = HEAD // 2
    exponent = jnp.arange(half_width, dtype=f32) * (2.0 / HEAD)
    inverse = jnp.exp(-math.log(rope_theta) * exponent)
    angles = jnp.arange(slot_count, dtype=jnp.int32).astype(f32)[:, None] * inverse[None, :]
    pad = jnp.zeros((slot_count, LANES - HEAD), f32)
    cosine_tab = jnp.concatenate([jnp.cos(angles), jnp.cos(angles), pad], axis=-1)
    sine_tab = jnp.concatenate([jnp.sin(angles), jnp.sin(angles), pad], axis=-1)
    return cosine_tab, sine_tab


def rms_parts(values):
    inverse_rms = lax.rsqrt(jnp.mean(values * values, axis=-1, keepdims=True) + eps_norm)
    return values * inverse_rms, inverse_rms


def rms_back(grad_normed, unit_rows, inverse_rms, gain_vec):
    scaled = grad_normed * gain_vec
    return inverse_rms * (scaled - unit_rows * jnp.mean(scaled * unit_rows, axis=-1, keepdims=True))


def contract_last(left_side, right_side):
    return lax.dot_general(
        left_side, right_side, (((1,), (1,)), ((), ())), preferred_element_type=f32
    )


def contract_first(left_side, right_side):
    return lax.dot_general(
        left_side, right_side, (((0,), (0,)), ((), ())), preferred_element_type=f32
    )


def matmul(left_side, right_side):
    return jnp.dot(left_side, right_side, preferred_element_type=f32)


def _rot_half(t, lane):
    return jnp.where(
        lane < HEAD // 2, -pltpu.roll(t, LANES - HEAD // 2, 1), pltpu.roll(t, HEAD // 2, 1)
    )


def _rope(t, cos, sin, lane):
    return t * cos + _rot_half(t, lane) * sin


def _unrope(t, cos, sin, lane):
    return t * cos - _rot_half(t, lane) * sin


def _wide(v):
    return jnp.concatenate([v, jnp.zeros_like(v)], axis=1)


def _weights(q, k, visible, live):
    scores = jnp.where(visible, contract_last(q, k) * score_scale, masked_score)
    exponent = jnp.exp(scores - jnp.max(scores, axis=-1, keepdims=True))
    return jnp.where(live, exponent / jnp.sum(exponent, axis=-1, keepdims=True), 0.0)


def _masks(length, slots):
    row = lax.broadcasted_iota(jnp.int32, (slots, slots), 0)
    col = lax.broadcasted_iota(jnp.int32, (slots, slots), 1)
    live = row < length
    return (col <= row) & live & (col < length), live


def attend_kernel(len_ref, qkv_ref, cos_ref, sin_ref, o_ref):
    length = len_ref[pl.program_id(0)]
    slots = qkv_ref.shape[0]
    visible, live = _masks(length, slots)
    lane = lax.broadcasted_iota(jnp.int32, (slots, LANES), 1)
    cos, sin = cos_ref[...], sin_ref[...]
    k = _rope(qkv_ref[:, 2 * LANES : 3 * LANES], cos, sin, lane).astype(bf16)
    v = qkv_ref[:, 3 * LANES :]
    v_wide = _wide(v)
    mixed = None
    for h in range(2):
        q = _rope(qkv_ref[:, h * LANES : (h + 1) * LANES], cos, sin, lane).astype(bf16)
        weights = _weights(q, k, visible, live).astype(bf16)
        v_h = v_wide if h == 0 else pltpu.roll(v_wide, HEAD, 1)
        part = matmul(weights, v_h.astype(bf16))
        mixed = part if mixed is None else mixed + part
    o_ref[...] = mixed.astype(bf16)


def attend_back_kernel(len_ref, qkv_ref, do_ref, cos_ref, sin_ref, out_ref):
    length = len_ref[pl.program_id(0)]
    slots = qkv_ref.shape[0]
    visible, live = _masks(length, slots)
    lane = lax.broadcasted_iota(jnp.int32, (slots, LANES), 1)
    cos, sin = cos_ref[...], sin_ref[...]
    k = _rope(qkv_ref[:, 2 * LANES : 3 * LANES], cos, sin, lane).astype(bf16)
    v_wide = _wide(qkv_ref[:, 3 * LANES :])
    d_o = do_ref[...]
    grad_k = grad_v = None
    for h in range(2):
        q = _rope(qkv_ref[:, h * LANES : (h + 1) * LANES], cos, sin, lane).astype(bf16)
        weights = _weights(q, k, visible, live)
        v_h = v_wide if h == 0 else pltpu.roll(v_wide, HEAD, 1)
        grad_weights = contract_last(d_o, v_h.astype(bf16))
        row_inner = jnp.sum(weights * grad_weights, axis=-1, keepdims=True)
        grad_scores = (weights * (grad_weights - row_inner)).astype(bf16)
        grad_q = matmul(grad_scores, k) * score_scale
        out_ref[:, h * LANES : (h + 1) * LANES] = _unrope(grad_q, cos, sin, lane).astype(bf16)
        part_k = contract_first(grad_scores, q) * score_scale
        part_v = contract_first(weights.astype(bf16), d_o)
        if h == 1:
            part_v = pltpu.roll(part_v, 2 * LANES - HEAD, 1)
        part_v = part_v[:, :LANES]
        grad_k = part_k if grad_k is None else grad_k + part_k
        grad_v = part_v if grad_v is None else grad_v + part_v
    out_ref[:, 2 * LANES : 3 * LANES] = _unrope(grad_k, cos, sin, lane).astype(bf16)
    out_ref[:, 3 * LANES :] = jnp.where(lane < HEAD, grad_v, 0.0).astype(bf16)


def attend(lengths, qkv, cos, sin):
    blocks, slots, width = qkv.shape
    table = pl.BlockSpec((slots, LANES), lambda s, ln: (0, 0))
    return pl.pallas_call(
        attend_kernel,
        out_shape=jax.ShapeDtypeStruct((blocks, slots, 2 * LANES), bf16),
        grid_spec=pltpu.PrefetchScalarGridSpec(
            num_scalar_prefetch=1,
            grid=(blocks,),
            in_specs=[pl.BlockSpec((None, slots, width), lambda s, ln: (s, 0, 0)), table, table],
            out_specs=pl.BlockSpec((None, slots, 2 * LANES), lambda s, ln: (s, 0, 0)),
        ),
        cost_estimate=pl.CostEstimate(
            flops=blocks * 8 * slots * slots * LANES, bytes_accessed=blocks * slots * width * 6,
            transcendentals=blocks * 2 * slots * slots,
        ),
    )(lengths, qkv, cos, sin)


def attend_back(lengths, qkv, d_o, cos, sin):
    blocks, slots, width = qkv.shape
    table = pl.BlockSpec((slots, LANES), lambda s, ln: (0, 0))
    return pl.pallas_call(
        attend_back_kernel,
        out_shape=jax.ShapeDtypeStruct((blocks, slots, width), bf16),
        grid_spec=pltpu.PrefetchScalarGridSpec(
            num_scalar_prefetch=1,
            grid=(blocks,),
            in_specs=[
                pl.BlockSpec((None, slots, width), lambda s, ln: (s, 0, 0)),
                pl.BlockSpec((None, slots, 2 * LANES), lambda s, ln: (s, 0, 0)),
                table,
                table,
            ],
            out_specs=pl.BlockSpec((None, slots, width), lambda s, ln: (s, 0, 0)),
        ),
        cost_estimate=pl.CostEstimate(
            flops=blocks * 24 * slots * slots * LANES, bytes_accessed=blocks * slots * width * 8,
            transcendentals=blocks * 2 * slots * slots,
        ),
    )(lengths, qkv, d_o, cos, sin)


class Mail:
    def __init__(self, n, send_sems, recv_sems):
        self.me = lax.axis_index("fsdp")
        self.send_sems, self.recv_sems = send_sems, recv_sems
        self.count, self.open = 0, []
        self.peers = {bits: self._peer(bits) for bits in range(1, n)}

    def _peer(self, bits):
        device, bit = self.me, 1
        while bit <= bits:
            if bits & bit:
                device = device + bit * (1 - 2 * ((self.me // bit) % 2))
            bit *= 2
        return device

    def enter(self, bits_list, away, others):
        barrier = pltpu.get_barrier_semaphore()

        @pl.when(away)
        def _():
            for device in others:
                pl.semaphore_signal(
                    barrier, inc=1, device_id=(device,), device_id_type=pl.DeviceIdType.MESH
                )

        for bits in bits_list:
            pl.semaphore_signal(
                barrier,
                inc=1,
                device_id=(self.peers[bits],),
                device_id_type=pl.DeviceIdType.MESH,
            )

        @pl.when(away)
        def _():
            pl.semaphore_wait(barrier, len(bits_list) + len(others))

        @pl.when(jnp.logical_not(away))
        def _():
            pl.semaphore_wait(barrier, len(bits_list))

    def make(self, src, dst, bits):
        copy = pltpu.make_async_remote_copy(
            src_ref=src,
            dst_ref=dst,
            send_sem=self.send_sems.at[self.count],
            recv_sem=self.recv_sems.at[self.count],
            device_id=(self.peers[bits],),
            device_id_type=pl.DeviceIdType.MESH,
        )
        self.count += 1
        self.open.append(copy)
        return copy

    def send(self, src, dst, bits):
        copy = self.make(src, dst, bits)
        copy.start()
        return copy

    def sent(self, copies):
        for copy in copies:
            copy.wait_send()
            self.open = [other for other in self.open if other is not copy]


def take(copies):
    for copy in copies:
        copy.wait_recv()


def xor_place(t, s):
    total = 0
    for bit in (1, 2, 4):
        total = total + bit * (((t // bit) % 2 + (s // bit) % 2) % 2)
    return total


def entry(s):
    if isinstance(s, int):
        return {3: 4, 4: 3}.get(s, s)
    return s + (s // 3) % 2 * (1 - s // 4) - (s // 4) * (1 - (s % 4 + 3) // 4)


def color_bits(color):
    return [1 << ((color + i) % 3) for i in range(3)]


class Gather:
    def __init__(self, mail, all_ref, own):
        self.mail, self.copies, self.stages = mail, {}, [[], [], []]
        part = all_ref.shape[2] // COLORS
        for i in range(3):
            for color in range(COLORS):
                cols = pl.ds(color * part, part)
                bit = color_bits(color)[i]
                self._make(0, color, bit, own.at[:, cols], all_ref.at[entry(bit), :, cols], bit)
        for color in range(COLORS):
            cols = pl.ds(color * part, part)
            b1, b2, b3 = color_bits(color)
            for stage, slot, bit in (
                (1, b1, b2), (1, b1, b3), (2, b2, b3), (2, b1 ^ b2, b3)
            ):
                src = all_ref.at[entry(slot), :, cols]
                dst = all_ref.at[entry(slot ^ bit), :, cols]
                self._make(stage, color, slot ^ bit, src, dst, bit)
        for copy in self.stages[0]:
            copy.start()

    def _make(self, stage, color, slot, src, dst, bit):
        self.copies[color, slot] = self.mail.make(src, dst, 2 * bit)
        self.stages[stage].append(self.copies[color, slot])

    def forward(self, stage):
        for color in range(COLORS):
            b1, b2, b3 = color_bits(color)
            for slot in ((b1,), (b2, b1 ^ b2))[stage - 1]:
                self.copies[color, slot].wait_recv()
        for copy in self.stages[stage]:
            copy.start()

    def sent(self):
        self.mail.sent(self.copies.values())

    def near(self):
        for color in range(COLORS):
            self.copies[color, color_bits(color)[2]].wait_recv()

    def far(self):
        for color in range(COLORS):
            b1, b2, b3 = color_bits(color)
            for slot in (b1 ^ b3, b2 ^ b3, 7):
                self.copies[color, slot].wait_recv()


class Scatter:
    def __init__(self, mail, piece, got):
        self.mail, self.piece, self.got, self.copies = mail, piece, got, {}
        for color in range(COLORS):
            for bit in color_bits(color):
                for s in self._stage(color, bit):
                    self.copies[color, s] = mail.make(piece(s, color), got(s, color), 2 * bit)

    def _stage(self, color, bit):
        b1, b2, b3 = color_bits(color)
        if bit == b1:
            return [s for s in range(CUBE) if s & b1]
        return [b2, b2 ^ b3] if bit == b2 else [b3]

    def start(self, entries):
        for s in entries:
            for color in range(COLORS):
                if s & color_bits(color)[0]:
                    self.copies[color, s].start()

    def _add(self, color, s, bit):
        self.copies[color, s].wait_recv()
        here = self.piece(s ^ bit, color)
        here[...] = (here[...].astype(f32) + self.got(s, color)[...].astype(f32)).astype(here.dtype)

    def second(self):
        for color in range(COLORS):
            b1, b2, b3 = color_bits(color)
            for s in (b2, b2 ^ b3):
                self._add(color, b1 ^ s, b1)
                self.copies[color, s].start()

    def third(self):
        for color in range(COLORS):
            b1, b2, b3 = color_bits(color)
            self._add(color, b1 ^ b3, b1)
            self._add(color, b2 ^ b3, b2)
            self.copies[color, b3].start()

    def total(self, color):
        value = self.piece(0, color)[...].astype(f32)
        for s in color_bits(color):
            self.copies[color, s].wait_recv()
            value = value + self.got(s, color)[...].astype(f32)
        return value

    def sent(self):
        self.mail.sent(self.copies.values())


def lanes_at(values, start, width):
    low = start // LANES * LANES
    high = min(values.shape[1], -(-(start + width) // LANES) * LANES)
    window = values[:, low:high]
    if start > low:
        window = pltpu.roll(window, (high - low) - (start - low), 1)
    return window


def spread(values, width, shift):
    missing = width - values.shape[1]
    if missing > 0:
        values = jnp.concatenate(
            [values, jnp.zeros((values.shape[0], missing), values.dtype)], axis=1
        )
    return pltpu.roll(values, shift, 1) if shift else values


def clear_from(values, lane_count):
    lane = lax.broadcasted_iota(jnp.int32, values.shape, 1)
    return jnp.where(lane < lane_count, values, 0.0)


def heads_of(qkv):
    return [lanes_at(qkv, HEAD * j, HEAD)[:, :LANES] for j in range(4)]


def products(weight_ref, grad_ref):
    return weight_ref[...].astype(f32) * grad_ref[...]


def block_masks(slots, length):
    row = lax.broadcasted_iota(jnp.int32, (slots, slots), 0)
    col = lax.broadcasted_iota(jnp.int32, (slots, slots), 1)
    live = row.astype(f32) < length
    return (col <= row) & live, live


def lane_value(values, index):
    lane = lax.broadcasted_iota(jnp.int32, values.shape, 1)
    return jnp.sum(jnp.where(lane == index, values, 0.0), axis=1, keepdims=True)


def layer_kernel(
    n, x_ref, g_in, len_ref, small_ref, wq_ref, wk_ref, wv_ref, wo_ref, wg_ref, wu_ref, wd_ref,
    cos_ref, sin_ref,
    out_ref, grad_in, gq_ref, gk_ref, gv_ref, go_ref, gg_ref, gup_ref, gd_ref, attn_dot, mlp_dot,
    h1_all, qkv_all, mixed_all, resid, h2_all, wqkv, gains,
    wout, wgu, wdown, g_all, o_slots, hidden, dgu, dh2, got,
    gu_grad, gu_got, gu_send, gu_far, wd_part, wd_got, wd_send, wd_far, dqkv, gu_slots,
    qkv_slots, wo_slot,
    send_sems, recv_sems, local_sems, owner_sems, core_ready, far_ready,
):
    cubes = n // (2 * CUBE)
    mail = Mail(n, send_sems, recv_sems)
    me = mail.me
    core, place, cube = me % 2, (me // 2) % CUBE, me // (2 * CUBE)
    pz, py, px = place // 4, (place // 2) % 2, place % 2
    other_core, other = 1 - core, 1 - cube
    slots, width = x_ref.shape
    rows, down_rows = wo_ref.shape[0], wd_ref.shape[0]
    units = hidden.shape[2]
    far_bits = 2 * CUBE
    owner = 2 * cubes * place + 2 * cube + core
    summed_at = far_bits * ((me // 2) % cubes) + 2 * (me // (2 * cubes)) + core
    away = owner != me
    mail.enter([2 * s for s in range(1, CUBE)] + [1, far_bits], away, [owner, summed_at])

    x_mail = Gather(mail, h1_all, x_ref)
    local = [
        pltpu.make_async_copy(wd_ref, wdown.at[cube, core], local_sems.at[0]),
        pltpu.make_async_copy(wo_ref, wout.at[cube, pz, py, px, core], local_sems.at[1]),
    ]
    for copy in local:
        copy.start()
    gains[...] = small_ref[...]
    small_cps = mail.send(small_ref, got.at[0, pl.ds(0, 8)], 1)

    query, key, value = (ref[...].astype(f32) for ref in (wq_ref, wk_ref, wv_ref))
    for t in range(CUBE):
        whole = 4 * HEAD
        parts = (
            spread(clear_from(lanes_at(query, 2 * HEAD * t, 2 * HEAD), 2 * HEAD), whole, 0)
            + spread(clear_from(lanes_at(key, HEAD * t, HEAD), HEAD), whole, 2 * HEAD)
            + spread(clear_from(lanes_at(value, HEAD * t, HEAD), HEAD), whole, 3 * HEAD)
        )
        qkv_slots[t] = parts.astype(bf16)
    wqkv[cube, place, core] = qkv_slots[place]
    pack_cps = [
        mail.send(qkv_slots.at[xor_place(place, s)], wqkv.at[cube, place, core], 2 * s)
        for s in range(1, CUBE)
    ]
    wo_cps = mail.send(wo_ref, wout.at[cube, pz, py, px, core], far_bits)

    for t in range(CUBE):
        for i in range(2 * cubes):
            start = (((i // 2) * CUBE + t) * 2 + i % 2) * down_rows
            cols = slice(start, start + down_rows)
            gu_send[t // 4, t % 4, :, i * down_rows : (i + 1) * down_rows] = wg_ref[:, cols]
            gu_send[t // 4, t % 4, :, units + i * down_rows : units + (i + 1) * down_rows] = wu_ref[:, cols]
    wgu[cube, place, core] = gu_send[place // 4, place % 4]
    row = lax.broadcasted_iota(jnp.int32, (slots, width), 0)
    g_all[0] = jnp.where(row < len_ref[0, 0], g_in[...].astype(f32), 0.0).astype(bf16)

    for i in range(1, n.bit_length() - 1):
        small_cps.wait_recv()
        mail.sent([small_cps])
        gains[...] += got[i - 1, :8]
        small_cps = mail.send(gains, got.at[i, pl.ds(0, 8)], 1 << i)
    take(pack_cps)
    mail.sent(pack_cps)
    pack_far = mail.send(wqkv.at[cube, :, core], wqkv.at[cube, :, core], far_bits)
    pack_core = [mail.send(wqkv.at[cube, :, core], wqkv.at[cube, :, core], 1)]
    x_mail.forward(1)
    small_cps.wait_recv()
    mail.sent([small_cps])
    gains[...] += got[n.bit_length() - 2, :8]
    gu_cps = [
        mail.send(
            gu_send.at[xor_place(place, s) // 4, xor_place(place, s) % 4],
            wgu.at[cube, place, core],
            2 * s,
        )
        for s in range(1, CUBE)
    ]
    x_mail.forward(2)
    local[1].wait()
    wo_cps.wait_recv()
    wo_z = mail.send(wout.at[:, pz, py, px, core], wout.at[:, pz, py, px, core], 8)
    g_mail = Gather(mail, g_all, g_all.at[0])
    pack_far.wait_recv()
    pack_core.append(mail.send(wqkv.at[other, :, core], wqkv.at[other, :, core], 1))
    x_mail.near()
    x_mail.far()
    take(pack_core)
    x_mail.sent()
    h1_all[0] = x_ref[...]
    gain_attn, gain_mlp, lengths = gains[0:1, :], gains[1:2, :], gains[2:3, :]

    wo_y = mail.make(wout.at[:, :, py, px, core], wout.at[:, :, py, px, core], 4)
    wo_x = mail.make(wout.at[:, :, :, px, core], wout.at[:, :, :, px, core], 2)
    wo_c = mail.make(wout.at[:, :, :, :, core], wout.at[:, :, :, :, core], 1)
    gu_out = mail.make(wgu.at[cube, :, core], wgu.at[cube, :, core], far_bits)
    wd_out = mail.make(wd_ref, wdown.at[cube, core], far_bits)

    def attention(s, carry):
        values = h1_all[s].astype(f32)
        normed = (rms_parts(values)[0] * gain_attn).astype(bf16)
        h1_all[s] = normed
        projected = heads_of(matmul(normed, wqkv[...].reshape(width, 4 * HEAD)))
        there = far_bits * cube + 2 * xor_place(place, entry(s)) + core
        visible, live = block_masks(slots, lane_value(lengths, there))
        lane = lax.broadcasted_iota(jnp.int32, (slots, LANES), 1)
        cos, sin = cos_ref[...], sin_ref[...]
        for j in range(3):
            qkv_all[s, :, j * LANES : (j + 1) * LANES] = _rope(projected[j], cos, sin, lane).astype(bf16)
        value = clear_from(projected[3], HEAD)
        qkv_all[s, :, 3 * LANES :] = value.astype(bf16)
        k = qkv_all[s, :, 2 * LANES : 3 * LANES]
        v_wide = _wide(value)
        mixed = None
        for h in range(2):
            q = qkv_all[s, :, h * LANES : (h + 1) * LANES]
            weights = _weights(q, k, visible, live).astype(bf16)
            v_h = pltpu.roll(v_wide, HEAD, 1) if h else v_wide
            part = matmul(weights, v_h.astype(bf16))
            mixed = part if mixed is None else mixed + part
        mixed_all[s] = mixed.astype(bf16)

        @pl.when(s == 0)
        def _():
            wo_z.wait_recv()
            wo_y.start()

        @pl.when(s == 1)
        def _():
            take(gu_cps)
            gu_out.start()

        @pl.when(s == 2)
        def _():
            wd_out.start()
            g_mail.forward(1)

        @pl.when(s == 4)
        def _():
            wo_y.wait_recv()
            wo_x.start()

        @pl.when(s == 5)
        def _():
            g_mail.forward(2)

        @pl.when(s == 7)
        def _():
            wo_x.wait_recv()
            wo_c.start()

        return carry

    lax.fori_loop(0, CUBE, attention, 0)

    o_cps = [mail.send(mixed_all.at[entry(s)], o_slots.at[place], 2 * s) for s in range(1, CUBE)]
    o_slots[place] = mixed_all[0]
    local[0].wait()
    wd_out.wait_recv()
    wd_core = mail.send(wdown.at[:, core], wdown.at[:, core], 1)
    take(o_cps)
    wide = []
    for j in range(CUBE // 2):
        low = spread(o_slots[2 * j].astype(f32), 3 * LANES, 0)
        high = spread(o_slots[2 * j + 1].astype(f32), 3 * LANES, 2 * HEAD)
        wide.append((low + high).astype(bf16))
    attended = jnp.concatenate(wide, axis=1)
    wo_c.wait_recv()
    step = 256
    for j in range(width // step):
        cols = slice(j * step, (j + 1) * step)
        weight = wout[:, :, :, :, :, :, cols].reshape(width, step)
        resid[:, cols] = x_ref[:, cols].astype(f32) + matmul(attended, weight)
    h2_all[0] = (rms_parts(resid[...])[0] * gain_mlp).astype(bf16)
    h2_mail = Gather(mail, h2_all, h2_all.at[0])
    g_mail.near()
    g_mail.far()
    h2_mail.forward(1)
    wd_core.wait_recv()
    gu_out.wait_recv()
    gu_core = mail.send(wgu.at[:, :, core], wgu.at[:, :, core], 1)
    h2_mail.forward(2)
    h2_mail.near()
    gu_core.wait_recv()

    def columns(ref):
        part = width // COLORS
        return lambda s, color: ref.at[entry(s), :, color * part : (color + 1) * part]

    got_columns = columns(got)
    back = Scatter(mail, columns(dh2), lambda s, color: got_columns(entry(s - 1), color))

    def feed_forward(half):
        step = 256
        tokens = CUBE // 2 * slots
        here = slice(half * CUBE // 2, (half + 1) * CUBE // 2)

        def split(values):
            return values.reshape(CUBE // 2, slots, values.shape[1])

        for j in range(units // step):
            cols = slice(j * step, (j + 1) * step)
            up_cols = slice(units + j * step, units + (j + 1) * step)
            lhs = h2_all[here].reshape(tokens, width)
            gate = matmul(lhs, wgu[:, :, :, :, cols].reshape(width, step))
            up = matmul(lhs, wgu[:, :, :, :, up_cols].reshape(width, step))
            down = wdown[...].reshape(units, width)[cols]
            grad_hidden = contract_last(g_all[here].reshape(tokens, width), down)
            sigmoid_gate = jax.nn.sigmoid(gate)
            silu = gate * sigmoid_gate
            hidden[here, :, cols] = split((silu * up).astype(bf16))
            dgu[here, :, cols] = split(
                (grad_hidden * up * sigmoid_gate * (1.0 + gate * (1.0 - sigmoid_gate))).astype(bf16)
            )
            dgu[here, :, up_cols] = split((grad_hidden * silu).astype(bf16))
        for j in range(4):
            part = width // 4
            weight = wgu[j // 2, (j % 2) * (CUBE // 2) : (j % 2 + 1) * (CUBE // 2)]
            grad = contract_last(
                dgu[here].reshape(tokens, 2 * units), weight.reshape(part, 2 * units)
            )
            dh2[here, :, j * part : (j + 1) * part] = split(grad)
        back.start([entry(i) for i in range(half * CUBE // 2, (half + 1) * CUBE // 2)])

    feed_forward(0)
    h2_mail.far()
    feed_forward(1)

    g_mail.sent()
    mail.sent([wo_cps, wo_z, wo_y, wo_x, wo_c])
    d_all = dgu[...].reshape(CUBE * slots, 2 * units)
    chunk = width // 4
    for j in range(4):
        lhs = h2_all[:, :, j * chunk : (j + 1) * chunk].reshape(CUBE * slots, chunk)
        gu_grad[j // 2, j % 2] = contract_first(lhs, d_all).reshape(gu_grad.shape[2:])
    gu_own_cps = gu_cps
    gu_cps = gu_core_cps = mail.send(gu_grad.at[:, :, :, other_core], gu_got, 1)
    hid_all = hidden[...].reshape(CUBE * slots, units)
    for j in range(4):
        cols = slice(j * chunk, (j + 1) * chunk)
        g_cols = g_all[:, :, cols].reshape(CUBE * slots, chunk)
        wd_part[:, :, :, cols] = contract_first(hid_all, g_cols).reshape(cubes, 2, down_rows, chunk)
    wd_cps = wd_core_cps = mail.send(wd_part.at[:, other_core], wd_got, 1)
    back.second()
    gu_cps.wait_recv()
    mail.sent(gu_own_cps)
    gu_send[...] = (gu_grad[other, :, :, core] + gu_got[other]).astype(bf16)
    gu_cps = gu_far_cps = mail.send(gu_send, gu_far, far_bits)
    wd_cps.wait_recv()
    wd_send[...] = (wd_part[other, core] + wd_got[other]).astype(bf16)
    wd_cps = wd_far_cps = mail.send(wd_send, wd_far, far_bits)
    back.third()
    h2_mail.sent()
    for i in range(2):
        half = slice(i * CUBE // 2, (i + 1) * CUBE // 2)
        lhs = hidden[half].reshape(CUBE // 2 * slots, units)
        for j in range(4):
            cols = slice(j * chunk, (j + 1) * chunk)
            part = matmul(lhs, wdown[:, :, :, cols].reshape(units, chunk))
            h2_all[half, :, cols] = part.reshape(CUBE // 2, slots, chunk).astype(bf16)
    unit, inverse = rms_parts(resid[...])
    part = width // COLORS
    for color in range(COLORS):
        dh2[0, :, color * part : (color + 1) * part] = back.total(color)
    grad_in[...] = g_all[0].astype(f32) + rms_back(dh2[0], unit, inverse, gain_mlp)
    low = grad_in[...].astype(bf16)
    g_all[0] = low
    for t in range(CUBE):
        weight = wout[t // 4, (t // 2) % 2, t % 2].reshape(2 * HEAD, width)
        dqkv[t, :, : 2 * LANES] = spread(contract_last(low, weight), 2 * LANES, 0).astype(bf16)
    do_cps = [
        mail.send(dqkv.at[xor_place(place, s), :, pl.ds(0, 2 * LANES)], o_slots.at[entry(s)], 2 * s)
        for s in range(1, CUBE)
    ]
    o_slots[0] = dqkv[place, :, : 2 * LANES]
    low_mail = Gather(mail, g_all, g_all.at[0])

    gu_cps.wait_recv()
    mail.sent([gu_far_cps])
    gu_send[...] = (
        gu_grad[cube, :, :, core] + gu_got[cube] + gu_far[...].astype(f32)
    ).astype(bf16)
    wd_cps.wait_recv()
    gd_ref[...] = wd_part[cube, core] + wd_got[cube] + wd_far[...].astype(f32)
    pl.semaphore_signal(
        core_ready, inc=1, device_id=(mail.peers[1],), device_id_type=pl.DeviceIdType.MESH
    )
    pl.semaphore_signal(
        far_ready, inc=1, device_id=(mail.peers[far_bits],), device_id_type=pl.DeviceIdType.MESH
    )
    take(do_cps)
    mail.sent(do_cps)
    gu_cps = [
        mail.send(
            gu_send.at[xor_place(place, s) // 4, xor_place(place, s) % 4], gu_slots.at[place], 2 * s
        )
        for s in range(1, CUBE)
    ]
    gu_slots[place] = gu_send[place // 4, place % 4]

    cuts = (0, 48, 96, slots)

    def out_got(s, color):
        i = COLORS * s + color
        rows_here = cuts[color + 1] - cuts[color]
        slot = wout.at[i // 16, (i // 8) % 2, (i // 4) % 2, (i // 2) % 2, i % 2]
        return slot.at[pl.ds(0, rows_here)]

    out_mail = Scatter(
        mail, lambda s, color: h2_all.at[entry(s), cuts[color] : cuts[color + 1]], out_got
    )

    def attention_back(s, carry):
        there = far_bits * cube + 2 * xor_place(place, entry(s)) + core
        visible, live = block_masks(slots, lane_value(lengths, there))
        lane = lax.broadcasted_iota(jnp.int32, (slots, LANES), 1)
        cos, sin = cos_ref[...], sin_ref[...]
        k = qkv_all[s, :, 2 * LANES : 3 * LANES]
        v_wide = _wide(qkv_all[s, :, 3 * LANES :].astype(f32))
        grad_o = o_slots[s]
        grad_k = grad_v = total = None
        for h in range(2):
            q = qkv_all[s, :, h * LANES : (h + 1) * LANES]
            weights = _weights(q, k, visible, live)
            v_h = pltpu.roll(v_wide, HEAD, 1) if h else v_wide
            grad_weights = contract_last(grad_o, v_h.astype(bf16))
            row_inner = jnp.sum(weights * grad_weights, axis=-1, keepdims=True)
            grad_scores = (weights * (grad_weights - row_inner)).astype(bf16)
            grad_q = _unrope(matmul(grad_scores, k) * score_scale, cos, sin, lane)
            part_k = contract_first(grad_scores, q) * score_scale
            part_v = contract_first(weights.astype(bf16), grad_o)
            if h:
                part_v = pltpu.roll(part_v, 2 * LANES - HEAD, 1)
            part_v = part_v[:, :LANES]
            grad_q = spread(grad_q, 4 * HEAD, h * HEAD)
            total = grad_q if total is None else total + grad_q
            grad_k = part_k if grad_k is None else grad_k + part_k
            grad_v = part_v if grad_v is None else grad_v + part_v
        total = total + spread(_unrope(grad_k, cos, sin, lane), 4 * HEAD, 2 * HEAD)
        total = total + spread(clear_from(grad_v, HEAD), 4 * HEAD, 3 * HEAD)
        dqkv[s] = total.astype(bf16)

        @pl.when(s == 0)
        def _():
            out_mail.start(range(CUBE))

        @pl.when(s == 1)
        def _():
            low_mail.forward(1)

        @pl.when(s == 5)
        def _():
            low_mail.forward(2)

        return carry

    lax.fori_loop(0, CUBE, attention_back, 0)

    pl.semaphore_wait(core_ready, 1)
    mail.sent([gu_core_cps, wd_core_cps])
    qkv_all_grad = dqkv[...].reshape(CUBE * slots, 4 * HEAD)
    narrow = slice(0, 4 * HEAD)
    for j in range(4):
        lhs = h1_all[:, :, j * chunk : (j + 1) * chunk].reshape(CUBE * slots, chunk)
        gu_grad[j // 2, j % 2, :, :, :, narrow] = contract_first(lhs, qkv_all_grad).reshape(
            CUBE // 2, 2, rows, 4 * HEAD
        )
    qkv_cps = mail.send(
        gu_grad.at[:, :, :, other_core, :, narrow], gu_got.at[:, :, :, :, narrow], 1
    )
    for i in range(2):
        half = slice(i * CUBE // 2, (i + 1) * CUBE // 2)
        lhs = dqkv[half].reshape(CUBE // 2 * slots, 4 * HEAD)
        for j in range(2):
            part = width // 2
            grad = contract_last(lhs, wqkv[j].reshape(part, 4 * HEAD))
            h1_all[half, :, j * part : (j + 1) * part] = grad.reshape(
                CUBE // 2, slots, part
            ).astype(bf16)

    def in_got(s, color):
        part = width // COLORS
        if color == 2:
            return hidden.at[entry(s)]
        return dgu.at[entry(s), :, color * part : (color + 1) * part]

    in_mail = Scatter(mail, columns(h1_all), in_got)
    in_mail.start(range(CUBE))
    qkv_cps.wait_recv()
    pl.semaphore_wait(far_ready, 1)
    mail.sent([*gu_cps, wd_far_cps])
    gu_send[:, :, :, narrow] = (
        gu_grad[other, :, :, core, :, narrow] + gu_got[other, :, :, :, narrow]
    ).astype(bf16)
    qkv_cps = mail.send(
        gu_send.at[:, :, :, narrow], gu_far.at[:, :, :, narrow], far_bits
    )

    low_mail.near()
    low_mail.far()
    mixed = mixed_all[...].reshape(CUBE * slots, 2 * LANES)
    for j in range(4):
        cols = slice(j * chunk, (j + 1) * chunk)
        g_cols = g_all[:, :, cols].reshape(CUBE * slots, chunk)
        wd_part[:, :, :rows, cols] = contract_first(mixed, g_cols)[: 2 * HEAD].reshape(
            cubes, 2, rows, chunk
        )
    wo_cps = mail.send(wd_part.at[:, other_core, pl.ds(0, rows)], wd_got.at[:, pl.ds(0, rows)], 1)
    out_mail.second()
    wo_cps.wait_recv()
    wd_send[:rows] = (wd_part[other, core, :rows] + wd_got[other, :rows]).astype(bf16)
    wo_cps = mail.send(wd_send.at[pl.ds(0, rows)], wd_far.at[pl.ds(0, rows)], far_bits)
    in_mail.second()
    qkv_cps.wait_recv()
    gu_far[:, :, :, narrow] = (
        gu_grad[cube, :, :, core, :, narrow]
        + gu_got[cube, :, :, :, narrow]
        + gu_far[:, :, :, narrow].astype(f32)
    ).astype(bf16)
    qkv_cps = [
        mail.send(
            gu_far.at[xor_place(place, s) // 4, xor_place(place, s) % 4, :, narrow],
            qkv_slots.at[place],
            2 * s,
        )
        for s in range(1, CUBE)
    ]
    qkv_slots[place] = gu_far[place // 4, place % 4, :, narrow]
    wo_cps.wait_recv()
    wd_far[:rows] = (
        wd_part[cube, core, :rows] + wd_got[cube, :rows] + wd_far[:rows].astype(f32)
    ).astype(bf16)
    wo_copy = pltpu.make_async_remote_copy(
        src_ref=wd_far.at[pl.ds(0, rows)],
        dst_ref=wo_slot,
        send_sem=owner_sems.at[0],
        recv_sem=owner_sems.at[1],
        device_id=(owner,),
        device_id_type=pl.DeviceIdType.MESH,
    )

    @pl.when(away)
    def _():
        wo_copy.start()

    @pl.when(owner == me)
    def _():
        wo_slot[...] = wd_far[:rows]

    in_mail.third()
    out_mail.third()

    take(gu_cps)
    for t in range(CUBE):
        for i in range(2 * cubes):
            start = (((i // 2) * CUBE + t) * 2 + i % 2) * down_rows
            cols = slice(start, start + down_rows)
            gg_ref[:, cols] = gu_slots[t, :, i * down_rows : (i + 1) * down_rows].astype(f32)
            gup_ref[:, cols] = gu_slots[
                t, :, units + i * down_rows : units + (i + 1) * down_rows
            ].astype(f32)
    mlp_sum = jnp.sum(wg_ref[...].astype(f32) * gg_ref[...], axis=1, keepdims=True) + jnp.sum(
        wu_ref[...].astype(f32) * gup_ref[...], axis=1, keepdims=True
    )
    mlp_dot[...] = jnp.broadcast_to(mlp_sum, mlp_dot.shape)

    take(qkv_cps)
    whole = 4 * HEAD
    for j in range(CUBE // 2):
        pair = [qkv_slots[2 * j + i].astype(f32) for i in range(2)]
        gq_ref[:, j * whole : (j + 1) * whole] = sum(
            spread(clear_from(values, 2 * HEAD), whole, 2 * HEAD * i)
            for i, values in enumerate(pair)
        )
    for j in range(2):
        four = [qkv_slots[4 * j + i].astype(f32) for i in range(4)]
        for ref, start in ((gk_ref, 2 * HEAD), (gv_ref, 3 * HEAD)):
            ref[:, j * whole : (j + 1) * whole] = sum(
                spread(clear_from(lanes_at(values, start, HEAD), HEAD), whole, HEAD * i)
                for i, values in enumerate(four)
            )
    attn_sum = jnp.sum(products(wq_ref, gq_ref), axis=1, keepdims=True)
    attn_sum = attn_sum + jnp.sum(products(wk_ref, gk_ref), axis=1, keepdims=True)
    attn_sum = attn_sum + jnp.sum(products(wv_ref, gv_ref), axis=1, keepdims=True)
    attn_dot[...] = jnp.broadcast_to(attn_sum, attn_dot.shape)

    @pl.when(away)
    def _():
        wo_copy.wait_recv()
        wo_copy.wait_send()

    go_ref[...] = wo_slot[...].astype(f32)

    unit, inverse = rms_parts(x_ref[...].astype(f32))
    part = width // COLORS
    for color in range(COLORS):
        dh2[0, :, color * part : (color + 1) * part] = in_mail.total(color)
    grad_in[...] += rms_back(dh2[0], unit, inverse, gain_attn)
    for color in range(COLORS):
        here = slice(cuts[color], cuts[color + 1])
        out_ref[here] = (resid[here] + out_mail.total(color)).astype(bf16)
    mail.sent(mail.open)


def per_device_any(
    n,
    layer_input,
    out_cotangent,
    lengths,
    norm_attn,
    w_query,
    w_key,
    w_value,
    w_out,
    norm_mlp,
    w_gate,
    w_up,
    w_down,
):
    cubes = n // (2 * CUBE)
    slots, width = layer_input.shape
    rows = w_query.shape[0]
    down_rows = w_down.shape[0]
    q_cols, kv_cols = w_query.shape[1] // CUBE, w_key.shape[1] // CUBE
    me = lax.axis_index("fsdp")
    core, place, cube = me % 2, (me // 2) % CUBE, me // (2 * CUBE)

    def swap(array, bits):
        return lax.ppermute(array, "fsdp", [(i, i ^ bits) for i in range(n)])

    def cube_gather(block):
        part = block.shape[1] // COLORS
        columns = []
        for color in range(COLORS):
            order = [(color + i) % 3 for i in range(3)]
            held, names = block[None, :, color * part : (color + 1) * part], [0]
            for bit in order:
                held = jnp.concatenate([held, swap(held, 2 << bit)], axis=0)
                names = names + [name ^ (1 << bit) for name in names]
            columns.append((held, names))
        return jnp.stack(
            [
                jnp.concatenate([held[names.index(s)] for held, names in columns], axis=1)
                for s in range(CUBE)
            ]
        )

    def cube_scatter(blocks):
        part = blocks.shape[2] // COLORS
        columns = []
        for color in range(COLORS):
            order = [(color + i) % 3 for i in range(3)]
            held = {s: blocks[s, :, color * part : (color + 1) * part] for s in range(CUBE)}
            for bit in order:
                send = [s for s in held if s & (1 << bit)]
                got = swap(jnp.stack([held[s] for s in send]), 2 << bit)
                for i, s in enumerate(send):
                    held[s ^ (1 << bit)] = held[s ^ (1 << bit)] + got[i]
                    del held[s]
            columns.append(held[0])
        return jnp.concatenate(columns, axis=1)

    def cube_exchange(blocks):
        return jnp.stack([blocks[0]] + [swap(blocks[s], 2 * s) for s in range(1, CUBE)])

    relative = jnp.arange(CUBE, dtype=jnp.int32) ^ place

    def by_place(blocks):
        return jnp.take(blocks, relative, axis=0, indices_are_sorted=False, unique_indices=True)

    def group_gather(block):
        held = jnp.stack([block] + [swap(block, 2 * CUBE * s) for s in range(1, cubes)])
        return jnp.stack([held, swap(held, 1)])

    owner = jnp.arange(n, dtype=jnp.int32)
    from_me = owner ^ me
    owner_entry = ((from_me % 2) * cubes + from_me // (2 * CUBE)) * CUBE + (from_me // 2) % CUBE
    pair = jnp.arange(2 * cubes, dtype=jnp.int32)
    pair_entry = ((pair % 2) ^ core) * cubes + ((pair // 2) ^ cube)

    def all_rows(block):
        held = group_gather(block).reshape(n, *block.shape[1:])
        return jnp.take(held, owner_entry, axis=0, unique_indices=True)

    small = jnp.concatenate(
        [norm_attn, norm_mlp, lengths[0].astype(bf16), jnp.zeros((LANES - 2 * rows - 1,), bf16)]
    )[None]
    bit = 1
    while bit < n:
        small = jnp.concatenate([small, swap(small, bit)], axis=0)
        bit *= 2
    cube_lengths = small[0 : 2 * CUBE : 2, 2 * rows].astype(jnp.int32)
    gains = jnp.take(small, from_me, axis=0)
    gain_attn = gains[:, :rows].reshape(width).astype(f32)
    gain_mlp = gains[:, rows : 2 * rows].reshape(width).astype(f32)
    cos, sin = rope_tables(slots)

    x_all = cube_gather(layer_input)
    own_qkv = jnp.concatenate(
        [
            w_query.reshape(rows, CUBE, q_cols),
            w_key.reshape(rows, CUBE, kv_cols),
            w_value.reshape(rows, CUBE, kv_cols),
        ],
        axis=2,
    ).transpose(1, 0, 2)
    w_qkv = all_rows(cube_exchange(by_place(own_qkv))).reshape(width, q_cols + 2 * kv_cols)
    w_qkv = jnp.pad(
        w_qkv.reshape(width, 4, HEAD), ((0, 0), (0, 0), (0, LANES - HEAD))
    ).reshape(width, 4 * LANES)

    out_held = jnp.stack([w_out] + [swap(w_out, 2 * CUBE * s) for s in range(1, cubes)])
    out_held = out_held.reshape(1, cubes, rows, width)
    for bit in range(3):
        out_held = jnp.concatenate([out_held, swap(out_held, 2 << bit)], axis=0)
    out_held = jnp.stack([out_held, swap(out_held, 1)])
    out_entry = ((from_me % 2) * CUBE + (from_me // 2) % CUBE) * cubes + from_me // (2 * CUBE)
    full_out = jnp.take(out_held.reshape(n, rows, width), out_entry, axis=0, unique_indices=True)
    full_out = jnp.pad(
        full_out.reshape(CUBE, q_cols, width), ((0, 0), (0, 2 * LANES - q_cols), (0, 0))
    ).reshape(CUBE * 2 * LANES, width)

    ff_cols = 2 * cubes * down_rows

    def by_hidden(weight):
        split = weight.reshape(rows, cubes, CUBE, 2, down_rows)
        return split.transpose(2, 0, 1, 3, 4).reshape(CUBE, rows, ff_cols)

    own_gate_up = jnp.concatenate([by_hidden(w_gate), by_hidden(w_up)], axis=2)
    w_gate_up = all_rows(cube_exchange(by_place(own_gate_up))).reshape(width, 2 * ff_cols)
    down_held = group_gather(w_down).reshape(2 * cubes, down_rows, width)
    down = jnp.take(down_held, pair_entry, axis=0, unique_indices=True).reshape(ff_cols, width)

    live = jnp.arange(slots, dtype=jnp.int32)[:, None] < lengths[0, 0]
    cotangent = jnp.where(live, out_cotangent, jnp.zeros_like(out_cotangent))
    g_all = cube_gather(cotangent).reshape(CUBE * slots, width)

    inputs = layer_input.astype(f32)
    unit_all, _ = rms_parts(x_all.reshape(CUBE * slots, width).astype(f32))
    normed_all = (unit_all * gain_attn).astype(bf16)
    qkv = matmul(normed_all, w_qkv).reshape(CUBE, slots, 4 * LANES)
    mixed = attend(cube_lengths, qkv, cos, sin)
    attended = by_place(cube_exchange(mixed)).transpose(1, 0, 2).reshape(slots, CUBE * 2 * LANES)
    residual = inputs + matmul(attended, full_out)
    unit_mlp, inv_mlp = rms_parts(residual)
    normed_mlp = cube_gather((unit_mlp * gain_mlp).astype(bf16)).reshape(CUBE * slots, width)

    gate_up = matmul(normed_mlp, w_gate_up)
    gate, up = gate_up[:, :ff_cols], gate_up[:, ff_cols:]
    sigmoid_gate = jax.nn.sigmoid(gate)
    hidden = (gate * sigmoid_gate * up).astype(bf16)
    grad_hidden = contract_last(g_all, down)
    grad_gate = (grad_hidden * up * sigmoid_gate * (1.0 + gate * (1.0 - sigmoid_gate))).astype(bf16)
    grad_up = (grad_hidden * gate * sigmoid_gate).astype(bf16)
    grad_gate_up = jnp.concatenate([grad_gate, grad_up], axis=1)
    grad_normed_mlp = cube_scatter(
        contract_last(grad_gate_up, w_gate_up).reshape(CUBE, slots, width)
    )
    grad_resid = cotangent.astype(f32) + rms_back(grad_normed_mlp, unit_mlp, inv_mlp, gain_mlp)
    grad_resid_low = grad_resid.astype(bf16)

    grad_attended = contract_last(grad_resid_low, full_out).astype(bf16)
    grad_blocks = by_place(grad_attended.reshape(slots, CUBE, 2 * LANES).transpose(1, 0, 2))
    grad_mixed = cube_exchange(grad_blocks)
    grad_qkv = attend_back(cube_lengths, qkv, grad_mixed, cos, sin).reshape(
        CUBE * slots, 4 * LANES
    )

    def low_sum(blocks):
        total = blocks[0]
        for s in range(1, CUBE):
            total = total + swap(blocks[s].astype(bf16), 2 * s).astype(f32)
        return total

    output = (
        residual + low_sum(matmul(hidden, down).reshape(CUBE, slots, width))
    ).astype(bf16)
    grad_normed = low_sum(contract_last(grad_qkv, w_qkv).reshape(CUBE, slots, width))
    unit_attn, inv_attn = rms_parts(inputs)
    grad_input = grad_resid + rms_back(grad_normed, unit_attn, inv_attn, gain_attn)

    def group_sum(blocks, core_axis):
        pick = functools.partial(
            lax.dynamic_index_in_dim, axis=core_axis + 1, keepdims=False
        )
        pair_total = pick(blocks, core) + swap(pick(blocks, 1 - core), 1)
        total = lax.dynamic_index_in_dim(pair_total, cube, axis=0, keepdims=False)
        for s in range(1, cubes):
            send = lax.dynamic_index_in_dim(pair_total, cube ^ s, axis=0, keepdims=False)
            total = total + swap(send.astype(bf16), 2 * CUBE * s).astype(f32)
        return total

    grad_down = group_sum(
        contract_first(hidden, g_all).reshape(cubes, 2, down_rows, width), 0
    )

    def to_owners(partial):
        cols = partial.shape[1]
        total = group_sum(partial.reshape(cubes, CUBE, 2, rows, cols), 1)
        return by_place(cube_exchange(by_place(total.astype(bf16)))).astype(f32)

    grad_gu = to_owners(contract_first(normed_mlp, grad_gate_up))

    def hidden_back(block):
        return block.reshape(CUBE, rows, cubes, 2, down_rows).transpose(1, 2, 0, 3, 4).reshape(
            rows, cubes * CUBE * 2 * down_rows
        )

    grad_w_gate, grad_w_up = hidden_back(grad_gu[:, :, :ff_cols]), hidden_back(grad_gu[:, :, ff_cols:])

    grad_w = to_owners(contract_first(normed_all, grad_qkv))
    grad_heads = grad_w.reshape(CUBE, rows, 4, LANES)[:, :, :, :HEAD].transpose(1, 2, 0, 3)
    grad_w_query = grad_heads[:, :2].transpose(0, 2, 1, 3).reshape(rows, CUBE * q_cols)
    grad_w_key = grad_heads[:, 2].reshape(rows, CUBE * kv_cols)
    grad_w_value = grad_heads[:, 3].reshape(rows, CUBE * kv_cols)

    resid_low_all = cube_gather(grad_resid_low).reshape(CUBE * slots, width)
    grad_out_part = contract_first(mixed.reshape(CUBE * slots, 2 * LANES), resid_low_all)[:q_cols]
    grad_out_sum = group_sum(grad_out_part.reshape(cubes, 2, rows, width), 0)
    moves = [
        (2 * CUBE * g + 2 * t + c, 2 * cubes * t + 2 * g + c)
        for g in range(cubes)
        for t in range(CUBE)
        for c in range(2)
    ]
    grad_w_out = lax.ppermute(grad_out_sum.astype(bf16), "fsdp", moves).astype(f32)

    def gain_grad(gain, pairs):
        total = sum(jnp.sum(weight.astype(f32) * grad, axis=1) for weight, grad in pairs)
        return total / gain.astype(f32)

    gain_attn_grad = gain_grad(
        norm_attn, [(w_query, grad_w_query), (w_key, grad_w_key), (w_value, grad_w_value)]
    )
    gain_mlp_grad = gain_grad(norm_mlp, [(w_gate, grad_w_gate), (w_up, grad_w_up)])
    return (
        output,
        grad_input,
        gain_attn_grad,
        grad_w_query,
        grad_w_key,
        grad_w_value,
        grad_w_out,
        gain_mlp_grad,
        grad_w_gate,
        grad_w_up,
        grad_down,
    )


def per_device_fast(
    n,
    layer_input,
    out_cotangent,
    lengths,
    norm_attn,
    w_query,
    w_key,
    w_value,
    w_out,
    norm_mlp,
    w_gate,
    w_up,
    w_down,
):
    cubes = n // (2 * CUBE)
    slots, width = layer_input.shape
    rows, down_rows = w_query.shape[0], w_down.shape[0]
    units, qkv_cols = 2 * cubes * down_rows, 4 * HEAD
    me = lax.axis_index("fsdp")
    lane_owner = jnp.arange(width, dtype=jnp.int32)[None] // rows
    small = jnp.where(lane_owner == me, jnp.tile(jnp.stack([norm_attn, norm_mlp]), (1, n)), 0)
    length_row = jnp.where(jnp.arange(width)[None] == me, lengths, 0)
    small = jnp.concatenate(
        [small.astype(f32), length_row.astype(f32), jnp.zeros((5, width), f32)]
    )
    cos, sin = rope_tables(slots)

    vmem = pl.BlockSpec(memory_space=pltpu.VMEM)
    smem = pl.BlockSpec(memory_space=pltpu.SMEM)
    hbm = pl.BlockSpec(memory_space=pl.ANY)
    outs = [
        ((slots, width), bf16),
        ((slots, width), f32),
        ((rows, w_query.shape[1]), f32),
        ((rows, w_key.shape[1]), f32),
        ((rows, w_value.shape[1]), f32),
        ((rows, width), f32),
        ((rows, w_gate.shape[1]), f32),
        ((rows, w_up.shape[1]), f32),
        ((down_rows, width), f32),
        ((rows, LANES), f32),
        ((rows, LANES), f32),
    ]
    half = (2, CUBE // 2, rows, 2 * units)
    scratch = [
        ((CUBE, slots, width), bf16),
        ((CUBE, slots, 4 * LANES), bf16),
        ((CUBE, slots, 2 * LANES), bf16),
        ((slots, width), f32),
        ((CUBE, slots, width), bf16),
        ((cubes, CUBE, 2, rows, qkv_cols), bf16),
        ((8, width), f32),
        ((cubes, 2, 2, 2, 2, rows, width), bf16),
        ((cubes, CUBE, 2, rows, 2 * units), bf16),
        ((cubes, 2, down_rows, width), bf16),
        ((CUBE, slots, width), bf16),
        ((CUBE, slots, 2 * LANES), bf16),
        ((CUBE, slots, units), bf16),
        ((CUBE, slots, 2 * units), bf16),
        ((CUBE, slots, width), f32),
        ((CUBE - 1, slots, width), f32),
        ((cubes, 2, CUBE // 2, 2, rows, 2 * units), f32),
        ((cubes,) + half, f32),
        (half, bf16),
        (half, bf16),
        ((cubes, 2, down_rows, width), f32),
        ((cubes, down_rows, width), f32),
        ((down_rows, width), bf16),
        ((down_rows, width), bf16),
        ((CUBE, slots, qkv_cols), bf16),
        ((CUBE, rows, 2 * units), bf16),
        ((CUBE, rows, qkv_cols), bf16),
        ((rows, width), bf16),
    ]
    messages = 256
    (
        output, grad_input, grad_w_query, grad_w_key, grad_w_value, grad_w_out, grad_w_gate,
        grad_w_up, grad_down, attn_dot, mlp_dot,
    ) = pl.pallas_call(
        functools.partial(layer_kernel, n),
        out_shape=[jax.ShapeDtypeStruct(*shape) for shape in outs],
        in_specs=[vmem, vmem, smem, vmem, vmem, vmem, vmem, hbm, vmem, vmem, hbm, vmem, vmem],
        out_specs=[vmem] * len(outs),
        scratch_shapes=[pltpu.VMEM(*shape) for shape in scratch]
        + [
            pltpu.SemaphoreType.DMA((messages,)),
            pltpu.SemaphoreType.DMA((messages,)),
            pltpu.SemaphoreType.DMA((2,)),
            pltpu.SemaphoreType.DMA((2,)),
            pltpu.SemaphoreType.REGULAR,
            pltpu.SemaphoreType.REGULAR,
        ],
        compiler_params=pltpu.CompilerParams(
            collective_id=0, has_side_effects=True, vmem_limit_bytes=67043328
        ),
    )(
        layer_input, out_cotangent, lengths, small, w_query, w_key, w_value, w_out, w_gate, w_up,
        w_down, cos, sin,
    )
    gain_attn_grad = attn_dot[:, 0] / norm_attn.astype(f32)
    gain_mlp_grad = mlp_dot[:, 0] / norm_mlp.astype(f32)
    return (
        output,
        grad_input,
        gain_attn_grad,
        grad_w_query,
        grad_w_key,
        grad_w_value,
        grad_w_out,
        gain_mlp_grad,
        grad_w_gate,
        grad_w_up,
        grad_down,
    )


def solution(mesh):
    n = mesh.shape["fsdp"]
    rows, vec = P("fsdp", None), P("fsdp")
    per_device = per_device_fast if n == 4 * CUBE else per_device_any
    return jax.shard_map(
        functools.partial(per_device, n),
        mesh=mesh,
        in_specs=(rows, rows, rows, vec, rows, rows, rows, rows, vec, rows, rows, rows),
        out_specs=(rows, rows, vec, rows, rows, rows, rows, vec, rows, rows, rows),
        check_vma=False,
    )
```

```python
import functools
import math

import jax
import jax.numpy as jnp
from jax import lax
from jax.experimental import pallas as pl
from jax.experimental.pallas import tpu as pltpu
from jax.sharding import PartitionSpec as P

HEADS = 16
KV_HEADS = 8
HEAD = 96
LANES = 128
CUBE = 8
COLORS = 3

eps_norm = 1e-05
rope_theta = 100000.0
masked_score = -1e30
score_scale = 1.0 / math.sqrt(HEAD)


bf16 = jnp.bfloat16
f32 = jnp.float32


def rope_tables(slot_count):
    half_width = HEAD // 2
    exponent = jnp.arange(half_width, dtype=f32) * (2.0 / HEAD)
    inverse = jnp.exp(-math.log(rope_theta) * exponent)
    angles = jnp.arange(slot_count, dtype=jnp.int32).astype(f32)[:, None] * inverse[None, :]
    pad = jnp.zeros((slot_count, LANES - HEAD), f32)
    cosine_tab = jnp.concatenate([jnp.cos(angles), jnp.cos(angles), pad], axis=-1)
    sine_tab = jnp.concatenate([jnp.sin(angles), jnp.sin(angles), pad], axis=-1)
    return cosine_tab, sine_tab


def rms_parts(values):
    inverse_rms = lax.rsqrt(jnp.mean(values * values, axis=-1, keepdims=True) + eps_norm)
    return values * inverse_rms, inverse_rms


def rms_back(grad_normed, unit_rows, inverse_rms, gain_vec):
    scaled = grad_normed * gain_vec
    return inverse_rms * (scaled - unit_rows * jnp.mean(scaled * unit_rows, axis=-1, keepdims=True))


def contract_last(left_side, right_side):
    return lax.dot_general(
        left_side, right_side, (((1,), (1,)), ((), ())), preferred_element_type=f32
    )


def contract_first(left_side, right_side):
    return lax.dot_general(
        left_side, right_side, (((0,), (0,)), ((), ())), preferred_element_type=f32
    )


def matmul(left_side, right_side):
    return jnp.dot(left_side, right_side, preferred_element_type=f32)


def _rot_half(t, lane):
    return jnp.where(
        lane < HEAD // 2, -pltpu.roll(t, LANES - HEAD // 2, 1), pltpu.roll(t, HEAD // 2, 1)
    )


def _rope(t, cos, sin, lane):
    return t * cos + _rot_half(t, lane) * sin


def _unrope(t, cos, sin, lane):
    return t * cos - _rot_half(t, lane) * sin


def _wide(v):
    return jnp.concatenate([v, jnp.zeros_like(v)], axis=1)


def _weights(q, k, visible, live):
    scores = jnp.where(visible, contract_last(q, k) * score_scale, masked_score)
    exponent = jnp.exp(scores - jnp.max(scores, axis=-1, keepdims=True))
    return jnp.where(live, exponent / jnp.sum(exponent, axis=-1, keepdims=True), 0.0)


def _masks(length, slots):
    row = lax.broadcasted_iota(jnp.int32, (slots, slots), 0)
    col = lax.broadcasted_iota(jnp.int32, (slots, slots), 1)
    live = row < length
    return (col <= row) & live & (col < length), live


def attend_kernel(len_ref, qkv_ref, cos_ref, sin_ref, o_ref):
    length = len_ref[pl.program_id(0)]
    slots = qkv_ref.shape[0]
    visible, live = _masks(length, slots)
    lane = lax.broadcasted_iota(jnp.int32, (slots, LANES), 1)
    cos, sin = cos_ref[...], sin_ref[...]
    k = _rope(qkv_ref[:, 2 * LANES : 3 * LANES], cos, sin, lane).astype(bf16)
    v = qkv_ref[:, 3 * LANES :]
    v_wide = _wide(v)
    mixed = None
    for h in range(2):
        q = _rope(qkv_ref[:, h * LANES : (h + 1) * LANES], cos, sin, lane).astype(bf16)
        weights = _weights(q, k, visible, live).astype(bf16)
        v_h = v_wide if h == 0 else pltpu.roll(v_wide, HEAD, 1)
        part = matmul(weights, v_h.astype(bf16))
        mixed = part if mixed is None else mixed + part
    o_ref[...] = mixed.astype(bf16)


def attend_back_kernel(len_ref, qkv_ref, do_ref, cos_ref, sin_ref, out_ref):
    length = len_ref[pl.program_id(0)]
    slots = qkv_ref.shape[0]
    visible, live = _masks(length, slots)
    lane = lax.broadcasted_iota(jnp.int32, (slots, LANES), 1)
    cos, sin = cos_ref[...], sin_ref[...]
    k = _rope(qkv_ref[:, 2 * LANES : 3 * LANES], cos, sin, lane).astype(bf16)
    v_wide = _wide(qkv_ref[:, 3 * LANES :])
    d_o = do_ref[...]
    grad_k = grad_v = None
    for h in range(2):
        q = _rope(qkv_ref[:, h * LANES : (h + 1) * LANES], cos, sin, lane).astype(bf16)
        weights = _weights(q, k, visible, live)
        v_h = v_wide if h == 0 else pltpu.roll(v_wide, HEAD, 1)
        grad_weights = contract_last(d_o, v_h.astype(bf16))
        row_inner = jnp.sum(weights * grad_weights, axis=-1, keepdims=True)
        grad_scores = (weights * (grad_weights - row_inner)).astype(bf16)
        grad_q = matmul(grad_scores, k) * score_scale
        out_ref[:, h * LANES : (h + 1) * LANES] = _unrope(grad_q, cos, sin, lane).astype(bf16)
        part_k = contract_first(grad_scores, q) * score_scale
        part_v = contract_first(weights.astype(bf16), d_o)
        if h == 1:
            part_v = pltpu.roll(part_v, 2 * LANES - HEAD, 1)
        part_v = part_v[:, :LANES]
        grad_k = part_k if grad_k is None else grad_k + part_k
        grad_v = part_v if grad_v is None else grad_v + part_v
    out_ref[:, 2 * LANES : 3 * LANES] = _unrope(grad_k, cos, sin, lane).astype(bf16)
    out_ref[:, 3 * LANES :] = jnp.where(lane < HEAD, grad_v, 0.0).astype(bf16)


def attend(lengths, qkv, cos, sin):
    blocks, slots, width = qkv.shape
    table = pl.BlockSpec((slots, LANES), lambda s, ln: (0, 0))
    return pl.pallas_call(
        attend_kernel,
        out_shape=jax.ShapeDtypeStruct((blocks, slots, 2 * LANES), bf16),
        grid_spec=pltpu.PrefetchScalarGridSpec(
            num_scalar_prefetch=1,
            grid=(blocks,),
            in_specs=[pl.BlockSpec((None, slots, width), lambda s, ln: (s, 0, 0)), table, table],
            out_specs=pl.BlockSpec((None, slots, 2 * LANES), lambda s, ln: (s, 0, 0)),
        ),
        cost_estimate=pl.CostEstimate(
            flops=blocks * 8 * slots * slots * LANES, bytes_accessed=blocks * slots * width * 6,
            transcendentals=blocks * 2 * slots * slots,
        ),
    )(lengths, qkv, cos, sin)


def attend_back(lengths, qkv, d_o, cos, sin):
    blocks, slots, width = qkv.shape
    table = pl.BlockSpec((slots, LANES), lambda s, ln: (0, 0))
    return pl.pallas_call(
        attend_back_kernel,
        out_shape=jax.ShapeDtypeStruct((blocks, slots, width), bf16),
        grid_spec=pltpu.PrefetchScalarGridSpec(
            num_scalar_prefetch=1,
            grid=(blocks,),
            in_specs=[
                pl.BlockSpec((None, slots, width), lambda s, ln: (s, 0, 0)),
                pl.BlockSpec((None, slots, 2 * LANES), lambda s, ln: (s, 0, 0)),
                table,
                table,
            ],
            out_specs=pl.BlockSpec((None, slots, width), lambda s, ln: (s, 0, 0)),
        ),
        cost_estimate=pl.CostEstimate(
            flops=blocks * 24 * slots * slots * LANES, bytes_accessed=blocks * slots * width * 8,
            transcendentals=blocks * 2 * slots * slots,
        ),
    )(lengths, qkv, d_o, cos, sin)


GATHER_WIDTHS = (2, 5, 5)
SCATTER_WIDTHS = (5, 4, 3)
OUT_WIDTHS = (6, 4, 2)
LOW_WIDTHS = (1, 5, 6)


class Mail:
    def __init__(self, n, send_sems, recv_sems):
        self.me = lax.axis_index("fsdp")
        self.send_sems, self.recv_sems = send_sems, recv_sems
        self.count, self.open = 0, []
        self.peers = {bits: self._peer(bits) for bits in range(1, n)}

    def _peer(self, bits):
        device, bit = self.me, 1
        while bit <= bits:
            if bits & bit:
                device = device + bit * (1 - 2 * ((self.me // bit) % 2))
            bit *= 2
        return device

    def enter(self, bits_list, away, others):
        barrier = pltpu.get_barrier_semaphore()

        @pl.when(away)
        def _():
            for device in others:
                pl.semaphore_signal(
                    barrier, inc=1, device_id=(device,), device_id_type=pl.DeviceIdType.MESH
                )

        for bits in bits_list:
            pl.semaphore_signal(
                barrier,
                inc=1,
                device_id=(self.peers[bits],),
                device_id_type=pl.DeviceIdType.MESH,
            )

        @pl.when(away)
        def _():
            pl.semaphore_wait(barrier, len(bits_list) + len(others))

        @pl.when(jnp.logical_not(away))
        def _():
            pl.semaphore_wait(barrier, len(bits_list))

    def make(self, src, dst, bits):
        copy = pltpu.make_async_remote_copy(
            src_ref=src,
            dst_ref=dst,
            send_sem=self.send_sems.at[self.count],
            recv_sem=self.recv_sems.at[self.count],
            device_id=(self.peers[bits],),
            device_id_type=pl.DeviceIdType.MESH,
        )
        self.count += 1
        self.open.append(copy)
        return copy

    def send(self, src, dst, bits):
        copy = self.make(src, dst, bits)
        copy.start()
        return copy

    def sent(self, copies):
        for copy in copies:
            copy.wait_send()
            self.open = [other for other in self.open if other is not copy]


def take(copies):
    for copy in copies:
        copy.wait_recv()


def xor_place(t, s):
    total = 0
    for bit in (1, 2, 4):
        total = total + bit * (((t // bit) % 2 + (s // bit) % 2) % 2)
    return total


def entry(s):
    if isinstance(s, int):
        return {3: 4, 4: 3}.get(s, s)
    return s + (s // 3) % 2 * (1 - s // 4) - (s // 4) * (1 - (s % 4 + 3) // 4)


def color_bits(color):
    return [1 << ((color + i) % 3) for i in range(3)]


def columns(ref, widths):
    starts = [sum(widths[:color]) for color in range(COLORS)]
    return lambda s, color: ref.at[
        entry(s), :, pl.ds(starts[color] * LANES, widths[color] * LANES)
    ]


class Gather:
    def __init__(self, mail, piece, absolute=False):
        self.mail, self.copies, self.stages = mail, {}, [[], [], []]

        def make(stage, color, slot, bit):
            dst = piece(slot if absolute else slot ^ bit, color)
            self.copies[color, slot ^ bit] = mail.make(piece(slot, color), dst, 2 * bit)
            self.stages[stage].append(self.copies[color, slot ^ bit])

        for i in range(3):
            for color in range(COLORS):
                make(0, color, 0, color_bits(color)[i])
        for color in range(COLORS):
            b1, b2, b3 = color_bits(color)
            make(1, color, b1, b2)
            make(1, color, b1, b3)
            make(2, color, b2, b3)
            make(2, color, b1 ^ b2, b3)

    def start(self):
        for copy in self.stages[0]:
            copy.start()

    def forward(self, stage):
        for color in range(COLORS):
            b1, b2, b3 = color_bits(color)
            for slot in ((b1,), (b2, b1 ^ b2))[stage - 1]:
                self.copies[color, slot].wait_recv()
        for copy in self.stages[stage]:
            copy.start()

    def sent(self):
        self.mail.sent(self.copies.values())

    def near(self):
        for color in range(COLORS):
            self.copies[color, color_bits(color)[2]].wait_recv()

    def far(self, colors=range(COLORS)):
        for color in colors:
            b1, b2, b3 = color_bits(color)
            for slot in (b1 ^ b3, b2 ^ b3, 7):
                self.copies[color, slot].wait_recv()


class Scatter:
    def __init__(self, mail, piece, got):
        self.mail, self.piece, self.got, self.copies = mail, piece, got, {}
        for color in range(COLORS):
            for bit in color_bits(color):
                for s in self._stage(color, bit):
                    self.copies[color, s] = mail.make(piece(s, color), got(s, color), 2 * bit)

    def _stage(self, color, bit):
        b1, b2, b3 = color_bits(color)
        if bit == b1:
            return [s for s in range(CUBE) if s & b1]
        return [b2, b2 ^ b3] if bit == b2 else [b3]

    def start(self, entries):
        for s in entries:
            for color in range(COLORS):
                if s & color_bits(color)[0]:
                    self.copies[color, s].start()

    def _add(self, color, s, bit):
        self.copies[color, s].wait_recv()
        here = self.piece(s ^ bit, color)
        here[...] = (here[...].astype(f32) + self.got(s, color)[...].astype(f32)).astype(here.dtype)

    def second(self):
        for color in range(COLORS):
            b1, b2, b3 = color_bits(color)
            for s in (b2, b2 ^ b3):
                self._add(color, b1 ^ s, b1)
                self.copies[color, s].start()

    def third(self):
        for color in range(COLORS):
            b1, b2, b3 = color_bits(color)
            self._add(color, b1 ^ b3, b1)
            self._add(color, b2 ^ b3, b2)
            self.copies[color, b3].start()

    def total(self, color):
        value = self.piece(0, color)[...].astype(f32)
        for s in color_bits(color):
            self.copies[color, s].wait_recv()
            value = value + self.got(s, color)[...].astype(f32)
        return value

    def sent(self):
        self.mail.sent(self.copies.values())


def lanes_at(values, start, width):
    low = start // LANES * LANES
    high = min(values.shape[1], -(-(start + width) // LANES) * LANES)
    window = values[:, low:high]
    if start > low:
        window = pltpu.roll(window, (high - low) - (start - low), 1)
    return window


def spread(values, width, shift):
    missing = width - values.shape[1]
    if missing > 0:
        values = jnp.concatenate(
            [values, jnp.zeros((values.shape[0], missing), values.dtype)], axis=1
        )
    return pltpu.roll(values, shift, 1) if shift else values


def clear_from(values, lane_count):
    lane = lax.broadcasted_iota(jnp.int32, values.shape, 1)
    return jnp.where(lane < lane_count, values, 0.0)


def heads_of(qkv):
    return [lanes_at(qkv, HEAD * j, HEAD)[:, :LANES] for j in range(4)]


def block_masks(slots, length):
    row = lax.broadcasted_iota(jnp.int32, (slots, slots), 0)
    col = lax.broadcasted_iota(jnp.int32, (slots, slots), 1)
    live = row.astype(f32) < length
    return (col <= row) & live, live


def lane_value(values, index):
    lane = lax.broadcasted_iota(jnp.int32, values.shape, 1)
    return jnp.sum(jnp.where(lane == index, values, 0.0), axis=1, keepdims=True)


def layer_kernel(
    n, x_ref, g_in, len_ref, small_ref, wq_ref, wk_ref, wv_ref, wo_ref, wg_ref, wu_ref, wd_ref,
    cos_ref, sin_ref,
    out_ref, grad_in, gd_ref, gu_slots, qkv_slots, wo_slot,
    h1_all, qkv_all, mixed_all, resid, h2_all, wqkv, gains,
    wout, wgu, wdown, g_all, o_slots, hidden, dgu, dh2, got,
    gu_grad, gu_got, gu_send, gu_far, wd_part, wd_got, wd_send, wd_far, dqkv,
    send_sems, recv_sems, local_sems, owner_sems, core_ready, far_ready, near_ready,
):
    cubes = n // (2 * CUBE)
    mail = Mail(n, send_sems, recv_sems)
    me = mail.me
    core, place, cube = me % 2, (me // 2) % CUBE, me // (2 * CUBE)
    pz, py, px = place // 4, (place // 2) % 2, place % 2
    other_core, other = 1 - core, 1 - cube
    slots, width = x_ref.shape
    rows, down_rows = wo_ref.shape[0], wd_ref.shape[0]
    units = hidden.shape[2]
    far_bits = 2 * CUBE
    owner = 2 * cubes * place + 2 * cube + core
    summed_at = far_bits * ((me // 2) % cubes) + 2 * (me // (2 * cubes)) + core
    away = owner != me
    mail.enter([2 * s for s in range(1, CUBE)] + [1, far_bits], away, [owner, summed_at])

    def small_at(i, low):
        return got.at[i, pl.ds(low, small_ref.shape[0]), pl.ds(0, LANES)]

    def small_add(copy, i, low):
        copy.wait_recv()
        gains[...] += small_at(i, low)[...]

    small_core = mail.send(small_ref, small_at(0, 32), 1)
    gains[...] = small_ref[...]

    h1_all[0] = x_ref[...]
    local = [
        pltpu.make_async_copy(wd_ref, wdown.at[cube, core], local_sems.at[0]),
        pltpu.make_async_copy(wo_ref, wout.at[cube, pz, py, px, core], local_sems.at[1]),
    ]
    for copy in local:
        copy.start()

    query, key, value = (ref[...].astype(f32) for ref in (wq_ref, wk_ref, wv_ref))
    for t in range(CUBE):
        whole = 4 * HEAD
        parts = (
            spread(clear_from(lanes_at(query, 2 * HEAD * t, 2 * HEAD), 2 * HEAD), whole, 0)
            + spread(clear_from(lanes_at(key, HEAD * t, HEAD), HEAD), whole, 2 * HEAD)
            + spread(clear_from(lanes_at(value, HEAD * t, HEAD), HEAD), whole, 3 * HEAD)
        )
        qkv_slots[t] = parts.astype(bf16)
    wqkv[cube, place, core] = qkv_slots[place]
    pack_cps = [
        mail.send(qkv_slots.at[xor_place(place, s)], wqkv.at[cube, place, core], 2 * s)
        for s in range(1, CUBE)
    ]
    small_core.wait_recv()
    mail.sent([small_core])
    gains[...] += small_at(0, 32)[...]
    small_far = mail.send(gains, small_at(1, 32), far_bits)

    x_mail = Gather(mail, columns(h1_all, GATHER_WIDTHS))
    x_mail.start()

    for t in range(CUBE):
        for i in range(2 * cubes):
            start = (((i // 2) * CUBE + t) * 2 + i % 2) * down_rows
            cols = slice(start, start + down_rows)
            gu_send[t // 4, t % 4, :, i * down_rows : (i + 1) * down_rows] = wg_ref[:, cols]
            gu_send[t // 4, t % 4, :, units + i * down_rows : units + (i + 1) * down_rows] = wu_ref[:, cols]
    wgu[cube, place, core] = gu_send[place // 4, place % 4]
    row = lax.broadcasted_iota(jnp.int32, (slots, width), 0)
    g_all[0] = jnp.where(row < len_ref[0, 0], g_in[...].astype(f32), 0.0).astype(bf16)
    small_far.wait_recv()
    mail.sent([small_far])
    gains[...] += small_at(1, 32)[...]
    small_cps = [mail.send(gains, small_at(s - 1, 0), 2 * s) for s in range(1, CUBE)]
    take(pack_cps)
    mail.sent(pack_cps)
    pack_far = mail.send(wqkv.at[cube, :, core], wqkv.at[cube, :, core], far_bits)
    pack_core = [mail.send(wqkv.at[cube, :, core], wqkv.at[cube, :, core], 1)]
    x_mail.forward(1)
    wo_cps = mail.send(wo_ref, wout.at[cube, pz, py, px, core], far_bits)
    gu_cps = [
        mail.send(
            gu_send.at[xor_place(place, s) // 4, xor_place(place, s) % 4],
            wgu.at[cube, place, core],
            2 * s,
        )
        for s in range(1, CUBE)
    ]
    x_mail.forward(2)
    wd_out = mail.send(wd_ref, wdown.at[cube, core], far_bits)
    take(small_cps)
    mail.sent(small_cps)
    for s in range(1, CUBE):
        gains[...] += small_at(s - 1, 0)[...]
    local[1].wait()
    wo_cps.wait_recv()

    def wo_piece(s, color):
        at = [(p + (s >> i) % 2) % 2 for i, p in ((2, pz), (1, py), (0, px))]
        widths = GATHER_WIDTHS
        start = sum(widths[:color])
        return wout.at[
            :, at[0], at[1], at[2], core, :, pl.ds(start * LANES, widths[color] * LANES)
        ]

    wo_mail = Gather(mail, wo_piece, absolute=True)
    pack_far.wait_recv()
    pack_core.append(mail.send(wqkv.at[other, :, core], wqkv.at[other, :, core], 1))
    x_mail.near()
    x_mail.far()
    wo_mail.start()
    take(pack_core)
    x_mail.sent()

    def row_of(first):
        return jnp.concatenate([gains[first + i : first + i + 1, :] for i in range(width // LANES)], axis=1)

    gain_attn, gain_mlp = row_of(0), row_of(width // LANES)
    lengths = gains[2 * (width // LANES) : 2 * (width // LANES) + 1, :]
    gu_out = mail.make(wgu.at[cube, :, core], wgu.at[cube, :, core], far_bits)

    def attention(s, carry):
        values = h1_all[s].astype(f32)
        normed = (rms_parts(values)[0] * gain_attn).astype(bf16)
        h1_all[s] = normed
        projected = heads_of(matmul(normed, wqkv[...].reshape(width, 4 * HEAD)))
        there = far_bits * cube + 2 * xor_place(place, entry(s)) + core
        visible, live = block_masks(slots, lane_value(lengths, there))
        lane = lax.broadcasted_iota(jnp.int32, (slots, LANES), 1)
        cos, sin = cos_ref[...], sin_ref[...]
        for j in range(3):
            qkv_all[s, :, j * LANES : (j + 1) * LANES] = _rope(projected[j], cos, sin, lane).astype(bf16)
        value = clear_from(projected[3], HEAD)
        qkv_all[s, :, 3 * LANES :] = value.astype(bf16)
        k = qkv_all[s, :, 2 * LANES : 3 * LANES]
        v_wide = _wide(value)
        mixed = None
        for h in range(2):
            q = qkv_all[s, :, h * LANES : (h + 1) * LANES]
            weights = _weights(q, k, visible, live).astype(bf16)
            v_h = pltpu.roll(v_wide, HEAD, 1) if h else v_wide
            part = matmul(weights, v_h.astype(bf16))
            mixed = part if mixed is None else mixed + part
        mixed_all[s] = mixed.astype(bf16)

        @pl.when(s == 4)
        def _():
            take(gu_cps)
            gu_out.start()

        @pl.when(s == 6)
        def _():
            wo_mail.forward(1)

        return carry

    lax.fori_loop(0, CUBE, attention, 0)

    o_cps = [mail.send(mixed_all.at[entry(s)], o_slots.at[place], 2 * s) for s in range(1, CUBE)]
    o_slots[place] = mixed_all[0]
    wo_mail.forward(2)
    local[0].wait()
    wd_out.wait_recv()
    wd_core = mail.send(wdown.at[:, core], wdown.at[:, core], 1)
    take(o_cps)
    g_mail = Gather(mail, columns(g_all, GATHER_WIDTHS))
    g_mail.start()
    wide = []
    for j in range(CUBE // 2):
        low = spread(o_slots[2 * j].astype(f32), 3 * LANES, 0)
        high = spread(o_slots[2 * j + 1].astype(f32), 3 * LANES, 2 * HEAD)
        wide.append((low + high).astype(bf16))
    attended = jnp.concatenate(wide, axis=1)
    wo_mail.near()
    wo_c = []
    for color in range(COLORS):
        wo_mail.far([color])
        start = sum(GATHER_WIDTHS[:color])
        part = wout.at[
            :, :, :, :, core, :, pl.ds(start * LANES, GATHER_WIDTHS[color] * LANES)
        ]
        wo_c.append(mail.send(part, part, 1))
    take(wo_c)
    step = 256
    for j in range(width // step):
        cols = slice(j * step, (j + 1) * step)
        weight = wout[:, :, :, :, :, :, cols].reshape(width, step)
        resid[:, cols] = x_ref[:, cols].astype(f32) + matmul(attended, weight)
    h2_all[0] = (rms_parts(resid[...])[0] * gain_mlp).astype(bf16)
    h2_mail = Gather(mail, columns(h2_all, GATHER_WIDTHS))
    h2_mail.start()
    g_mail.forward(1)
    h2_mail.forward(1)
    g_mail.forward(2)
    gu_out.wait_recv()
    gu_core = mail.send(wgu.at[:, :, core], wgu.at[:, :, core], 1)
    h2_mail.forward(2)
    wd_core.wait_recv()
    gu_core.wait_recv()
    g_mail.near()
    h2_mail.near()

    got_columns = columns(got, SCATTER_WIDTHS)
    back = Scatter(
        mail, columns(dh2, SCATTER_WIDTHS), lambda s, color: got_columns(entry(s - 1), color)
    )

    def feed_forward(half):
        step = 256
        tokens = CUBE // 2 * slots
        here = slice(half * CUBE // 2, (half + 1) * CUBE // 2)

        def split(values):
            return values.reshape(CUBE // 2, slots, values.shape[1])

        for j in range(units // step):
            cols = slice(j * step, (j + 1) * step)
            up_cols = slice(units + j * step, units + (j + 1) * step)
            lhs = h2_all[here].reshape(tokens, width)
            gate = matmul(lhs, wgu[:, :, :, :, cols].reshape(width, step))
            up = matmul(lhs, wgu[:, :, :, :, up_cols].reshape(width, step))
            down = wdown[...].reshape(units, width)[cols]
            grad_hidden = contract_last(g_all[here].reshape(tokens, width), down)
            sigmoid_gate = jax.nn.sigmoid(gate)
            silu = gate * sigmoid_gate
            hidden[here, :, cols] = split((silu * up).astype(bf16))
            dgu[here, :, cols] = split(
                (grad_hidden * up * sigmoid_gate * (1.0 + gate * (1.0 - sigmoid_gate))).astype(bf16)
            )
            dgu[here, :, up_cols] = split((grad_hidden * silu).astype(bf16))
        for j in range(4):
            part = width // 4
            weight = wgu[j // 2, (j % 2) * (CUBE // 2) : (j % 2 + 1) * (CUBE // 2)]
            grad = contract_last(
                dgu[here].reshape(tokens, 2 * units), weight.reshape(part, 2 * units)
            )
            dh2[here, :, j * part : (j + 1) * part] = split(grad)
        back.start([entry(i) for i in range(half * CUBE // 2, (half + 1) * CUBE // 2)])

    feed_forward(0)
    g_mail.far()
    h2_mail.far()
    feed_forward(1)

    g_mail.sent()
    h2_mail.sent()
    wo_mail.sent()
    mail.sent([wo_cps, *wo_c])
    d_all = dgu[...].reshape(CUBE * slots, 2 * units)
    chunk = width // 4
    for j in range(4):
        lhs = h2_all[:, :, j * chunk : (j + 1) * chunk].reshape(CUBE * slots, chunk)
        gu_grad[j // 2, j % 2] = contract_first(lhs, d_all).reshape(gu_grad.shape[2:])
    gu_own_cps = gu_cps
    gu_cps = gu_core_cps = mail.send(gu_grad.at[:, :, :, other_core], gu_got, 1)
    hid_all = hidden[...].reshape(CUBE * slots, units)
    for j in range(4):
        cols = slice(j * chunk, (j + 1) * chunk)
        g_cols = g_all[:, :, cols].reshape(CUBE * slots, chunk)
        wd_part[:, :, :, cols] = contract_first(hid_all, g_cols).reshape(cubes, 2, down_rows, chunk)
    wd_cps = wd_core_cps = mail.send(wd_part.at[:, other_core], wd_got, 1)
    for i in range(2):
        half = slice(i * CUBE // 2, (i + 1) * CUBE // 2)
        lhs = hidden[half].reshape(CUBE // 2 * slots, units)
        for j in range(4):
            cols = slice(j * chunk, (j + 1) * chunk)
            part = matmul(lhs, wdown[:, :, :, cols].reshape(units, chunk))
            h2_all[half, :, cols] = part.reshape(CUBE // 2, slots, chunk).astype(bf16)
    gu_cps.wait_recv()
    mail.sent(gu_own_cps)
    gu_send[...] = (gu_grad[other, :, :, core] + gu_got[other]).astype(bf16)
    gu_cps = gu_far_cps = mail.send(gu_send, gu_far, far_bits)
    wd_cps.wait_recv()
    wd_send[...] = (wd_part[other, core] + wd_got[other]).astype(bf16)
    wd_cps = wd_far_cps = mail.send(wd_send, wd_far, far_bits)

    def out_got(s, color):
        if color == 1:
            return hidden.at[entry(s)]
        start, part = ((0, 768), None, (768, 256))[color]
        return dgu.at[entry(s), :, pl.ds(start, part)]

    out_piece = columns(h2_all, OUT_WIDTHS)
    out_mail = Scatter(mail, out_piece, out_got)
    for bit in (1, 2, 4):
        pl.semaphore_signal(
            near_ready,
            inc=1,
            device_id=(mail.peers[2 * bit],),
            device_id_type=pl.DeviceIdType.MESH,
        )
    back.second()
    pl.semaphore_wait(near_ready, 3)
    out_mail.start(range(CUBE))
    back.third()

    unit, inverse = rms_parts(resid[...])
    for color in range(COLORS):
        columns(dh2, SCATTER_WIDTHS)(0, color)[...] = back.total(color)
    grad_in[...] = g_all[0].astype(f32) + rms_back(dh2[0], unit, inverse, gain_mlp)
    low = grad_in[...].astype(bf16)
    g_all[0] = low
    for t in range(CUBE):
        weight = wout[t // 4, (t // 2) % 2, t % 2].reshape(2 * HEAD, width)
        dqkv[t, :, : 2 * LANES] = spread(contract_last(low, weight), 2 * LANES, 0).astype(bf16)
    do_cps = [
        mail.send(dqkv.at[xor_place(place, s), :, pl.ds(0, 2 * LANES)], o_slots.at[entry(s)], 2 * s)
        for s in range(1, CUBE)
    ]
    o_slots[0] = dqkv[place, :, : 2 * LANES]
    out_mail.second()

    gu_cps.wait_recv()
    mail.sent([gu_far_cps])
    gu_send[...] = (
        gu_grad[cube, :, :, core] + gu_got[cube] + gu_far[...].astype(f32)
    ).astype(bf16)
    wd_cps.wait_recv()
    gd_ref[...] = wd_part[cube, core] + wd_got[cube] + wd_far[...].astype(f32)
    for ready, bits in ((core_ready, 1), (far_ready, far_bits)):
        pl.semaphore_signal(
            ready, inc=1, device_id=(mail.peers[bits],), device_id_type=pl.DeviceIdType.MESH
        )
    gu_cps = [
        mail.send(
            gu_send.at[xor_place(place, s) // 4, xor_place(place, s) % 4], gu_slots.at[place], 2 * s
        )
        for s in range(1, CUBE)
    ]
    gu_slots[place] = gu_send[place // 4, place % 4]
    take(do_cps)
    mail.sent(do_cps)
    low_mail = Gather(mail, columns(g_all, LOW_WIDTHS))
    low_mail.start()

    def attention_back(s, carry):
        there = far_bits * cube + 2 * xor_place(place, entry(s)) + core
        visible, live = block_masks(slots, lane_value(lengths, there))
        lane = lax.broadcasted_iota(jnp.int32, (slots, LANES), 1)
        cos, sin = cos_ref[...], sin_ref[...]
        k = qkv_all[s, :, 2 * LANES : 3 * LANES]
        v_wide = _wide(qkv_all[s, :, 3 * LANES :].astype(f32))
        grad_o = o_slots[s]
        grad_k = grad_v = total = None
        for h in range(2):
            q = qkv_all[s, :, h * LANES : (h + 1) * LANES]
            weights = _weights(q, k, visible, live)
            v_h = pltpu.roll(v_wide, HEAD, 1) if h else v_wide
            grad_weights = contract_last(grad_o, v_h.astype(bf16))
            row_inner = jnp.sum(weights * grad_weights, axis=-1, keepdims=True)
            grad_scores = (weights * (grad_weights - row_inner)).astype(bf16)
            grad_q = _unrope(matmul(grad_scores, k) * score_scale, cos, sin, lane)
            part_k = contract_first(grad_scores, q) * score_scale
            part_v = contract_first(weights.astype(bf16), grad_o)
            if h:
                part_v = pltpu.roll(part_v, 2 * LANES - HEAD, 1)
            part_v = part_v[:, :LANES]
            grad_q = spread(grad_q, 4 * HEAD, h * HEAD)
            total = grad_q if total is None else total + grad_q
            grad_k = part_k if grad_k is None else grad_k + part_k
            grad_v = part_v if grad_v is None else grad_v + part_v
        total = total + spread(_unrope(grad_k, cos, sin, lane), 4 * HEAD, 2 * HEAD)
        total = total + spread(clear_from(grad_v, HEAD), 4 * HEAD, 3 * HEAD)
        dqkv[s] = total.astype(bf16)

        return carry

    lax.fori_loop(0, CUBE, attention_back, 0)
    out_mail.third()

    pl.semaphore_wait(core_ready, 1)
    mail.sent([gu_core_cps, wd_core_cps])
    qkv_all_grad = dqkv[...].reshape(CUBE * slots, 4 * HEAD)
    narrow = slice(0, 4 * HEAD)
    for j in range(4):
        lhs = h1_all[:, :, j * chunk : (j + 1) * chunk].reshape(CUBE * slots, chunk)
        gu_grad[j // 2, j % 2, :, :, :, narrow] = contract_first(lhs, qkv_all_grad).reshape(
            CUBE // 2, 2, rows, 4 * HEAD
        )
    qkv_cps = mail.send(
        gu_grad.at[:, :, :, other_core, :, narrow], gu_got.at[:, :, :, :, narrow], 1
    )
    for i in range(2):
        half = slice(i * CUBE // 2, (i + 1) * CUBE // 2)
        lhs = dqkv[half].reshape(CUBE // 2 * slots, 4 * HEAD)
        for j in range(2):
            part = width // 2
            grad = contract_last(lhs, wqkv[j].reshape(part, 4 * HEAD))
            h1_all[half, :, j * part : (j + 1) * part] = grad.reshape(
                CUBE // 2, slots, part
            ).astype(bf16)

    cuts = (0, 48, 96, slots)

    def in_piece(s, color):
        return h1_all.at[entry(s), pl.ds(cuts[color], cuts[color + 1] - cuts[color])]

    def in_got(s, color):
        i = COLORS * s + color
        slot = wout.at[i // 16, (i // 8) % 2, (i // 4) % 2, (i // 2) % 2, i % 2]
        return slot.at[pl.ds(0, cuts[color + 1] - cuts[color])]

    in_mail = Scatter(mail, in_piece, in_got)
    in_mail.start(range(CUBE))
    qkv_cps.wait_recv()
    pl.semaphore_wait(far_ready, 1)
    mail.sent([*gu_cps, wd_far_cps])
    gu_send[:, :, :, narrow] = (
        gu_grad[other, :, :, core, :, narrow] + gu_got[other, :, :, :, narrow]
    ).astype(bf16)
    qkv_cps = mail.send(
        gu_send.at[:, :, :, narrow], gu_far.at[:, :, :, narrow], far_bits
    )
    low_mail.forward(1)
    low_mail.forward(2)
    in_mail.second()

    low_mail.near()
    low_mail.far()
    mixed = mixed_all[...].reshape(CUBE * slots, 2 * LANES)
    for j in range(4):
        cols = slice(j * chunk, (j + 1) * chunk)
        g_cols = g_all[:, :, cols].reshape(CUBE * slots, chunk)
        wd_part[:, :, :rows, cols] = contract_first(mixed, g_cols)[: 2 * HEAD].reshape(
            cubes, 2, rows, chunk
        )
    wo_cps = mail.send(wd_part.at[:, other_core, pl.ds(0, rows)], wd_got.at[:, pl.ds(0, rows)], 1)
    wo_cps.wait_recv()
    wd_send[:rows] = (wd_part[other, core, :rows] + wd_got[other, :rows]).astype(bf16)
    wo_cps = mail.send(wd_send.at[pl.ds(0, rows)], wd_far.at[pl.ds(0, rows)], far_bits)
    qkv_cps.wait_recv()
    gu_far[:, :, :, narrow] = (
        gu_grad[cube, :, :, core, :, narrow]
        + gu_got[cube, :, :, :, narrow]
        + gu_far[:, :, :, narrow].astype(f32)
    ).astype(bf16)
    qkv_cps = [
        mail.send(
            gu_far.at[xor_place(place, s) // 4, xor_place(place, s) % 4, :, narrow],
            qkv_slots.at[place],
            2 * s,
        )
        for s in range(1, CUBE)
    ]
    qkv_slots[place] = gu_far[place // 4, place % 4, :, narrow]
    in_mail.third()
    wo_cps.wait_recv()
    wd_far[:rows] = (
        wd_part[cube, core, :rows] + wd_got[cube, :rows] + wd_far[:rows].astype(f32)
    ).astype(bf16)
    wo_copy = pltpu.make_async_remote_copy(
        src_ref=wd_far.at[pl.ds(0, rows)],
        dst_ref=wo_slot,
        send_sem=owner_sems.at[0],
        recv_sem=owner_sems.at[1],
        device_id=(owner,),
        device_id_type=pl.DeviceIdType.MESH,
    )

    @pl.when(away)
    def _():
        wo_copy.start()

    @pl.when(owner == me)
    def _():
        wo_slot[...] = wd_far[:rows]

    take(gu_cps)
    take(qkv_cps)

    @pl.when(away)
    def _():
        wo_copy.wait_recv()
        wo_copy.wait_send()

    unit, inverse = rms_parts(x_ref[...].astype(f32))
    for color in range(COLORS):
        dh2[0, cuts[color] : cuts[color + 1]] = in_mail.total(color)
    grad_in[...] += rms_back(dh2[0], unit, inverse, gain_attn)
    for color in range(COLORS):
        low = sum(OUT_WIDTHS[:color]) * LANES
        here = slice(low, low + OUT_WIDTHS[color] * LANES)
        out_ref[:, here] = (resid[:, here] + out_mail.total(color)).astype(bf16)
    mail.sent(mail.open)


def finish_kernel(
    cubes, out_in, grad_in, gd_in, gu_slots, qkv_slots, wo_slot, wq_ref, wk_ref, wv_ref, wg_ref,
    wu_ref, norm_attn_ref, norm_mlp_ref,
    out_ref, grad_ref, attn_ref, gq_ref, gk_ref, gv_ref, go_ref, mlp_ref, gg_ref, gup_ref, gd_ref,
):
    rows, units = wg_ref.shape[0], gu_slots.shape[2] // 2
    down_rows = units // (2 * cubes)
    out_ref[...] = out_in[...]
    grad_ref[...] = grad_in[...]
    gd_ref[...] = gd_in[...]
    go_ref[...] = wo_slot[...].astype(f32)
    for t in range(CUBE):
        for i in range(2 * cubes):
            start = (((i // 2) * CUBE + t) * 2 + i % 2) * down_rows
            cols = slice(start, start + down_rows)
            gg_ref[:, cols] = gu_slots[t, :, i * down_rows : (i + 1) * down_rows].astype(f32)
            gup_ref[:, cols] = gu_slots[
                t, :, units + i * down_rows : units + (i + 1) * down_rows
            ].astype(f32)
    whole = 4 * HEAD
    for j in range(CUBE // 2):
        pair = [qkv_slots[2 * j + i].astype(f32) for i in range(2)]
        gq_ref[:, j * whole : (j + 1) * whole] = sum(
            spread(clear_from(values, 2 * HEAD), whole, 2 * HEAD * i)
            for i, values in enumerate(pair)
        )
    for j in range(2):
        four = [qkv_slots[4 * j + i].astype(f32) for i in range(4)]
        for ref, start in ((gk_ref, 2 * HEAD), (gv_ref, 3 * HEAD)):
            ref[:, j * whole : (j + 1) * whole] = sum(
                spread(clear_from(lanes_at(values, start, HEAD), HEAD), whole, HEAD * i)
                for i, values in enumerate(four)
            )

    diagonal = lax.broadcasted_iota(jnp.int32, (rows, rows), 0) == lax.broadcasted_iota(
        jnp.int32, (rows, rows), 1
    )

    def gain_grad(pairs, norm_ref):
        total = sum(
            jnp.sum(weight[...].astype(f32) * grad[...], axis=1, keepdims=True)
            for weight, grad in pairs
        )
        row = jnp.sum(jnp.where(diagonal, total, 0.0), axis=0, keepdims=True)
        return row / norm_ref[...].astype(f32)

    attn_ref[...] = gain_grad(
        ((wq_ref, gq_ref), (wk_ref, gk_ref), (wv_ref, gv_ref)), norm_attn_ref
    )
    mlp_ref[...] = gain_grad(((wg_ref, gg_ref), (wu_ref, gup_ref)), norm_mlp_ref)


def per_device_any(
    n,
    layer_input,
    out_cotangent,
    lengths,
    norm_attn,
    w_query,
    w_key,
    w_value,
    w_out,
    norm_mlp,
    w_gate,
    w_up,
    w_down,
):
    cubes = n // (2 * CUBE)
    slots, width = layer_input.shape
    rows = w_query.shape[0]
    down_rows = w_down.shape[0]
    q_cols, kv_cols = w_query.shape[1] // CUBE, w_key.shape[1] // CUBE
    me = lax.axis_index("fsdp")
    core, place, cube = me % 2, (me // 2) % CUBE, me // (2 * CUBE)

    def swap(array, bits):
        return lax.ppermute(array, "fsdp", [(i, i ^ bits) for i in range(n)])

    def cube_gather(block):
        part = block.shape[1] // COLORS
        columns = []
        for color in range(COLORS):
            order = [(color + i) % 3 for i in range(3)]
            held, names = block[None, :, color * part : (color + 1) * part], [0]
            for bit in order:
                held = jnp.concatenate([held, swap(held, 2 << bit)], axis=0)
                names = names + [name ^ (1 << bit) for name in names]
            columns.append((held, names))
        return jnp.stack(
            [
                jnp.concatenate([held[names.index(s)] for held, names in columns], axis=1)
                for s in range(CUBE)
            ]
        )

    def cube_scatter(blocks):
        part = blocks.shape[2] // COLORS
        columns = []
        for color in range(COLORS):
            order = [(color + i) % 3 for i in range(3)]
            held = {s: blocks[s, :, color * part : (color + 1) * part] for s in range(CUBE)}
            for bit in order:
                send = [s for s in held if s & (1 << bit)]
                got = swap(jnp.stack([held[s] for s in send]), 2 << bit)
                for i, s in enumerate(send):
                    held[s ^ (1 << bit)] = held[s ^ (1 << bit)] + got[i]
                    del held[s]
            columns.append(held[0])
        return jnp.concatenate(columns, axis=1)

    def cube_exchange(blocks):
        return jnp.stack([blocks[0]] + [swap(blocks[s], 2 * s) for s in range(1, CUBE)])

    relative = jnp.arange(CUBE, dtype=jnp.int32) ^ place

    def by_place(blocks):
        return jnp.take(blocks, relative, axis=0, indices_are_sorted=False, unique_indices=True)

    def group_gather(block):
        held = jnp.stack([block] + [swap(block, 2 * CUBE * s) for s in range(1, cubes)])
        return jnp.stack([held, swap(held, 1)])

    owner = jnp.arange(n, dtype=jnp.int32)
    from_me = owner ^ me
    owner_entry = ((from_me % 2) * cubes + from_me // (2 * CUBE)) * CUBE + (from_me // 2) % CUBE
    pair = jnp.arange(2 * cubes, dtype=jnp.int32)
    pair_entry = ((pair % 2) ^ core) * cubes + ((pair // 2) ^ cube)

    def all_rows(block):
        held = group_gather(block).reshape(n, *block.shape[1:])
        return jnp.take(held, owner_entry, axis=0, unique_indices=True)

    small = jnp.concatenate(
        [norm_attn, norm_mlp, lengths[0].astype(bf16), jnp.zeros((LANES - 2 * rows - 1,), bf16)]
    )[None]
    bit = 1
    while bit < n:
        small = jnp.concatenate([small, swap(small, bit)], axis=0)
        bit *= 2
    cube_lengths = small[0 : 2 * CUBE : 2, 2 * rows].astype(jnp.int32)
    gains = jnp.take(small, from_me, axis=0)
    gain_attn = gains[:, :rows].reshape(width).astype(f32)
    gain_mlp = gains[:, rows : 2 * rows].reshape(width).astype(f32)
    cos, sin = rope_tables(slots)

    x_all = cube_gather(layer_input)
    own_qkv = jnp.concatenate(
        [
            w_query.reshape(rows, CUBE, q_cols),
            w_key.reshape(rows, CUBE, kv_cols),
            w_value.reshape(rows, CUBE, kv_cols),
        ],
        axis=2,
    ).transpose(1, 0, 2)
    w_qkv = all_rows(cube_exchange(by_place(own_qkv))).reshape(width, q_cols + 2 * kv_cols)
    w_qkv = jnp.pad(
        w_qkv.reshape(width, 4, HEAD), ((0, 0), (0, 0), (0, LANES - HEAD))
    ).reshape(width, 4 * LANES)

    out_held = jnp.stack([w_out] + [swap(w_out, 2 * CUBE * s) for s in range(1, cubes)])
    out_held = out_held.reshape(1, cubes, rows, width)
    for bit in range(3):
        out_held = jnp.concatenate([out_held, swap(out_held, 2 << bit)], axis=0)
    out_held = jnp.stack([out_held, swap(out_held, 1)])
    out_entry = ((from_me % 2) * CUBE + (from_me // 2) % CUBE) * cubes + from_me // (2 * CUBE)
    full_out = jnp.take(out_held.reshape(n, rows, width), out_entry, axis=0, unique_indices=True)
    full_out = jnp.pad(
        full_out.reshape(CUBE, q_cols, width), ((0, 0), (0, 2 * LANES - q_cols), (0, 0))
    ).reshape(CUBE * 2 * LANES, width)

    ff_cols = 2 * cubes * down_rows

    def by_hidden(weight):
        split = weight.reshape(rows, cubes, CUBE, 2, down_rows)
        return split.transpose(2, 0, 1, 3, 4).reshape(CUBE, rows, ff_cols)

    own_gate_up = jnp.concatenate([by_hidden(w_gate), by_hidden(w_up)], axis=2)
    w_gate_up = all_rows(cube_exchange(by_place(own_gate_up))).reshape(width, 2 * ff_cols)
    down_held = group_gather(w_down).reshape(2 * cubes, down_rows, width)
    down = jnp.take(down_held, pair_entry, axis=0, unique_indices=True).reshape(ff_cols, width)

    live = jnp.arange(slots, dtype=jnp.int32)[:, None] < lengths[0, 0]
    cotangent = jnp.where(live, out_cotangent, jnp.zeros_like(out_cotangent))
    g_all = cube_gather(cotangent).reshape(CUBE * slots, width)

    inputs = layer_input.astype(f32)
    unit_all, _ = rms_parts(x_all.reshape(CUBE * slots, width).astype(f32))
    normed_all = (unit_all * gain_attn).astype(bf16)
    qkv = matmul(normed_all, w_qkv).reshape(CUBE, slots, 4 * LANES)
    mixed = attend(cube_lengths, qkv, cos, sin)
    attended = by_place(cube_exchange(mixed)).transpose(1, 0, 2).reshape(slots, CUBE * 2 * LANES)
    residual = inputs + matmul(attended, full_out)
    unit_mlp, inv_mlp = rms_parts(residual)
    normed_mlp = cube_gather((unit_mlp * gain_mlp).astype(bf16)).reshape(CUBE * slots, width)

    gate_up = matmul(normed_mlp, w_gate_up)
    gate, up = gate_up[:, :ff_cols], gate_up[:, ff_cols:]
    sigmoid_gate = jax.nn.sigmoid(gate)
    hidden = (gate * sigmoid_gate * up).astype(bf16)
    grad_hidden = contract_last(g_all, down)
    grad_gate = (grad_hidden * up * sigmoid_gate * (1.0 + gate * (1.0 - sigmoid_gate))).astype(bf16)
    grad_up = (grad_hidden * gate * sigmoid_gate).astype(bf16)
    grad_gate_up = jnp.concatenate([grad_gate, grad_up], axis=1)
    grad_normed_mlp = cube_scatter(
        contract_last(grad_gate_up, w_gate_up).reshape(CUBE, slots, width)
    )
    grad_resid = cotangent.astype(f32) + rms_back(grad_normed_mlp, unit_mlp, inv_mlp, gain_mlp)
    grad_resid_low = grad_resid.astype(bf16)

    grad_attended = contract_last(grad_resid_low, full_out).astype(bf16)
    grad_blocks = by_place(grad_attended.reshape(slots, CUBE, 2 * LANES).transpose(1, 0, 2))
    grad_mixed = cube_exchange(grad_blocks)
    grad_qkv = attend_back(cube_lengths, qkv, grad_mixed, cos, sin).reshape(
        CUBE * slots, 4 * LANES
    )

    def low_sum(blocks):
        total = blocks[0]
        for s in range(1, CUBE):
            total = total + swap(blocks[s].astype(bf16), 2 * s).astype(f32)
        return total

    output = (
        residual + low_sum(matmul(hidden, down).reshape(CUBE, slots, width))
    ).astype(bf16)
    grad_normed = low_sum(contract_last(grad_qkv, w_qkv).reshape(CUBE, slots, width))
    unit_attn, inv_attn = rms_parts(inputs)
    grad_input = grad_resid + rms_back(grad_normed, unit_attn, inv_attn, gain_attn)

    def group_sum(blocks, core_axis):
        pick = functools.partial(
            lax.dynamic_index_in_dim, axis=core_axis + 1, keepdims=False
        )
        pair_total = pick(blocks, core) + swap(pick(blocks, 1 - core), 1)
        total = lax.dynamic_index_in_dim(pair_total, cube, axis=0, keepdims=False)
        for s in range(1, cubes):
            send = lax.dynamic_index_in_dim(pair_total, cube ^ s, axis=0, keepdims=False)
            total = total + swap(send.astype(bf16), 2 * CUBE * s).astype(f32)
        return total

    grad_down = group_sum(
        contract_first(hidden, g_all).reshape(cubes, 2, down_rows, width), 0
    )

    def to_owners(partial):
        cols = partial.shape[1]
        total = group_sum(partial.reshape(cubes, CUBE, 2, rows, cols), 1)
        return by_place(cube_exchange(by_place(total.astype(bf16)))).astype(f32)

    grad_gu = to_owners(contract_first(normed_mlp, grad_gate_up))

    def hidden_back(block):
        return block.reshape(CUBE, rows, cubes, 2, down_rows).transpose(1, 2, 0, 3, 4).reshape(
            rows, cubes * CUBE * 2 * down_rows
        )

    grad_w_gate, grad_w_up = hidden_back(grad_gu[:, :, :ff_cols]), hidden_back(grad_gu[:, :, ff_cols:])

    grad_w = to_owners(contract_first(normed_all, grad_qkv))
    grad_heads = grad_w.reshape(CUBE, rows, 4, LANES)[:, :, :, :HEAD].transpose(1, 2, 0, 3)
    grad_w_query = grad_heads[:, :2].transpose(0, 2, 1, 3).reshape(rows, CUBE * q_cols)
    grad_w_key = grad_heads[:, 2].reshape(rows, CUBE * kv_cols)
    grad_w_value = grad_heads[:, 3].reshape(rows, CUBE * kv_cols)

    resid_low_all = cube_gather(grad_resid_low).reshape(CUBE * slots, width)
    grad_out_part = contract_first(mixed.reshape(CUBE * slots, 2 * LANES), resid_low_all)[:q_cols]
    grad_out_sum = group_sum(grad_out_part.reshape(cubes, 2, rows, width), 0)
    moves = [
        (2 * CUBE * g + 2 * t + c, 2 * cubes * t + 2 * g + c)
        for g in range(cubes)
        for t in range(CUBE)
        for c in range(2)
    ]
    grad_w_out = lax.ppermute(grad_out_sum.astype(bf16), "fsdp", moves).astype(f32)

    def gain_grad(gain, pairs):
        total = sum(jnp.sum(weight.astype(f32) * grad, axis=1) for weight, grad in pairs)
        return total / gain.astype(f32)

    gain_attn_grad = gain_grad(
        norm_attn, [(w_query, grad_w_query), (w_key, grad_w_key), (w_value, grad_w_value)]
    )
    gain_mlp_grad = gain_grad(norm_mlp, [(w_gate, grad_w_gate), (w_up, grad_w_up)])
    return (
        output,
        grad_input,
        gain_attn_grad,
        grad_w_query,
        grad_w_key,
        grad_w_value,
        grad_w_out,
        gain_mlp_grad,
        grad_w_gate,
        grad_w_up,
        grad_down,
    )


def per_device_fast(
    n,
    layer_input,
    out_cotangent,
    lengths,
    norm_attn,
    w_query,
    w_key,
    w_value,
    w_out,
    norm_mlp,
    w_gate,
    w_up,
    w_down,
):
    cubes = n // (2 * CUBE)
    slots, width = layer_input.shape
    rows, down_rows = w_query.shape[0], w_down.shape[0]
    units, qkv_cols = 2 * cubes * down_rows, 4 * HEAD
    me = lax.axis_index("fsdp")
    own = jnp.arange(width, dtype=jnp.int32) // rows == me
    small = [jnp.where(own, jnp.tile(norm, n), 0).astype(f32) for norm in (norm_attn, norm_mlp)]
    small.append(jnp.where(jnp.arange(1024) == me, lengths[0], 0).astype(f32))
    small = jnp.concatenate(small).reshape(-1, LANES)
    cos, sin = rope_tables(slots)

    vmem = pl.BlockSpec(memory_space=pltpu.VMEM)
    smem = pl.BlockSpec(memory_space=pltpu.SMEM)
    hbm = pl.BlockSpec(memory_space=pl.ANY)
    outs = [
        ((slots, width), bf16),
        ((slots, width), f32),
        ((down_rows, width), f32),
        ((CUBE, rows, 2 * units), bf16),
        ((CUBE, rows, qkv_cols), bf16),
        ((rows, width), bf16),
    ]
    half = (2, CUBE // 2, rows, 2 * units)
    scratch = [
        ((CUBE, slots, width), bf16),
        ((CUBE, slots, 4 * LANES), bf16),
        ((CUBE, slots, 2 * LANES), bf16),
        ((slots, width), f32),
        ((CUBE, slots, width), bf16),
        ((cubes, CUBE, 2, rows, qkv_cols), bf16),
        ((2 * width // LANES + 8, LANES), f32),
        ((cubes, 2, 2, 2, 2, rows, width), bf16),
        ((cubes, CUBE, 2, rows, 2 * units), bf16),
        ((cubes, 2, down_rows, width), bf16),
        ((CUBE, slots, width), bf16),
        ((CUBE, slots, 2 * LANES), bf16),
        ((CUBE, slots, units), bf16),
        ((CUBE, slots, 2 * units), bf16),
        ((CUBE, slots, width), f32),
        ((CUBE - 1, slots, width), f32),
        ((cubes, 2, CUBE // 2, 2, rows, 2 * units), f32),
        ((cubes,) + half, f32),
        (half, bf16),
        (half, bf16),
        ((cubes, 2, down_rows, width), f32),
        ((cubes, down_rows, width), f32),
        ((down_rows, width), bf16),
        ((down_rows, width), bf16),
        ((CUBE, slots, qkv_cols), bf16),
    ]
    messages = 256
    parts = pl.pallas_call(
        functools.partial(layer_kernel, n),
        out_shape=[jax.ShapeDtypeStruct(*shape) for shape in outs],
        in_specs=[vmem, vmem, smem, vmem, vmem, vmem, vmem, hbm, vmem, vmem, hbm, vmem, vmem],
        out_specs=[vmem] * len(outs),
        scratch_shapes=[pltpu.VMEM(*shape) for shape in scratch]
        + [
            pltpu.SemaphoreType.DMA((messages,)),
            pltpu.SemaphoreType.DMA((messages,)),
            pltpu.SemaphoreType.DMA((2,)),
            pltpu.SemaphoreType.DMA((2,)),
            pltpu.SemaphoreType.REGULAR,
            pltpu.SemaphoreType.REGULAR,
            pltpu.SemaphoreType.REGULAR,
        ],
        compiler_params=pltpu.CompilerParams(
            collective_id=0, has_side_effects=True, vmem_limit_bytes=67043328
        ),
    )(
        layer_input, out_cotangent, lengths, small, w_query, w_key, w_value, w_out, w_gate, w_up,
        w_down, cos, sin,
    )
    finals = [
        ((slots, width), bf16),
        ((slots, width), f32),
        ((1, rows), f32),
        (w_query.shape, f32),
        (w_key.shape, f32),
        (w_value.shape, f32),
        (w_out.shape, f32),
        ((1, rows), f32),
        (w_gate.shape, f32),
        (w_up.shape, f32),
        (w_down.shape, f32),
    ]
    results = list(
        pl.pallas_call(
            functools.partial(finish_kernel, cubes),
            out_shape=[jax.ShapeDtypeStruct(*shape) for shape in finals],
            in_specs=[vmem] * 13,
            out_specs=[vmem] * len(finals),
        )(
            *parts, w_query, w_key, w_value, w_gate, w_up, norm_attn[None], norm_mlp[None]
        )
    )
    results[2], results[7] = results[2][0], results[7][0]
    return tuple(results)


def solution(mesh):
    n = mesh.shape["fsdp"]
    rows, vec = P("fsdp", None), P("fsdp")
    per_device = per_device_fast if n == 4 * CUBE else per_device_any
    return jax.shard_map(
        functools.partial(per_device, n),
        mesh=mesh,
        in_specs=(rows, rows, rows, vec, rows, rows, rows, rows, vec, rows, rows, rows),
        out_specs=(rows, rows, vec, rows, rows, rows, rows, vec, rows, rows, rows),
        check_vma=False,
    )
```

```python
import functools
import math

import jax
import jax.numpy as jnp
from jax import lax
from jax.experimental import pallas as pl
from jax.experimental.pallas import tpu as pltpu
from jax.sharding import PartitionSpec as P

HEADS = 16
KV_HEADS = 8
HEAD = 96
LANES = 128
CUBE = 8
COLORS = 3

eps_norm = 1e-05
rope_theta = 100000.0
masked_score = -1e30
score_scale = 1.0 / math.sqrt(HEAD)


bf16 = jnp.bfloat16
f32 = jnp.float32


def rope_tables(slot_count):
    half_width = HEAD // 2
    exponent = jnp.arange(half_width, dtype=f32) * (2.0 / HEAD)
    inverse = jnp.exp(-math.log(rope_theta) * exponent)
    angles = jnp.arange(slot_count, dtype=jnp.int32).astype(f32)[:, None] * inverse[None, :]
    pad = jnp.zeros((slot_count, LANES - HEAD), f32)
    cosine_tab = jnp.concatenate([jnp.cos(angles), jnp.cos(angles), pad], axis=-1)
    sine_tab = jnp.concatenate([jnp.sin(angles), jnp.sin(angles), pad], axis=-1)
    return cosine_tab, sine_tab


def rms_parts(values):
    inverse_rms = lax.rsqrt(jnp.mean(values * values, axis=-1, keepdims=True) + eps_norm)
    return values * inverse_rms, inverse_rms


def rms_back(grad_normed, unit_rows, inverse_rms, gain_vec):
    scaled = grad_normed * gain_vec
    return inverse_rms * (scaled - unit_rows * jnp.mean(scaled * unit_rows, axis=-1, keepdims=True))


def contract_last(left_side, right_side):
    return lax.dot_general(
        left_side, right_side, (((1,), (1,)), ((), ())), preferred_element_type=f32
    )


def contract_first(left_side, right_side):
    return lax.dot_general(
        left_side, right_side, (((0,), (0,)), ((), ())), preferred_element_type=f32
    )


def matmul(left_side, right_side):
    return jnp.dot(left_side, right_side, preferred_element_type=f32)


def _rot_half(t, lane):
    return jnp.where(
        lane < HEAD // 2, -pltpu.roll(t, LANES - HEAD // 2, 1), pltpu.roll(t, HEAD // 2, 1)
    )


def _rope(t, cos, sin, lane):
    return t * cos + _rot_half(t, lane) * sin


def _unrope(t, cos, sin, lane):
    return t * cos - _rot_half(t, lane) * sin


def _wide(v):
    return jnp.concatenate([v, jnp.zeros_like(v)], axis=1)


def _weights(q, k, visible, live):
    scores = jnp.where(visible, contract_last(q, k) * score_scale, masked_score)
    exponent = jnp.exp(scores - jnp.max(scores, axis=-1, keepdims=True))
    return jnp.where(live, exponent / jnp.sum(exponent, axis=-1, keepdims=True), 0.0)


def _masks(length, slots):
    row = lax.broadcasted_iota(jnp.int32, (slots, slots), 0)
    col = lax.broadcasted_iota(jnp.int32, (slots, slots), 1)
    live = row < length
    return (col <= row) & live & (col < length), live


def attend_kernel(len_ref, qkv_ref, cos_ref, sin_ref, o_ref):
    length = len_ref[pl.program_id(0)]
    slots = qkv_ref.shape[0]
    visible, live = _masks(length, slots)
    lane = lax.broadcasted_iota(jnp.int32, (slots, LANES), 1)
    cos, sin = cos_ref[...], sin_ref[...]
    k = _rope(qkv_ref[:, 2 * LANES : 3 * LANES], cos, sin, lane).astype(bf16)
    v = qkv_ref[:, 3 * LANES :]
    v_wide = _wide(v)
    mixed = None
    for h in range(2):
        q = _rope(qkv_ref[:, h * LANES : (h + 1) * LANES], cos, sin, lane).astype(bf16)
        weights = _weights(q, k, visible, live).astype(bf16)
        v_h = v_wide if h == 0 else pltpu.roll(v_wide, HEAD, 1)
        part = matmul(weights, v_h.astype(bf16))
        mixed = part if mixed is None else mixed + part
    o_ref[...] = mixed.astype(bf16)


def attend_back_kernel(len_ref, qkv_ref, do_ref, cos_ref, sin_ref, out_ref):
    length = len_ref[pl.program_id(0)]
    slots = qkv_ref.shape[0]
    visible, live = _masks(length, slots)
    lane = lax.broadcasted_iota(jnp.int32, (slots, LANES), 1)
    cos, sin = cos_ref[...], sin_ref[...]
    k = _rope(qkv_ref[:, 2 * LANES : 3 * LANES], cos, sin, lane).astype(bf16)
    v_wide = _wide(qkv_ref[:, 3 * LANES :])
    d_o = do_ref[...]
    grad_k = grad_v = None
    for h in range(2):
        q = _rope(qkv_ref[:, h * LANES : (h + 1) * LANES], cos, sin, lane).astype(bf16)
        weights = _weights(q, k, visible, live)
        v_h = v_wide if h == 0 else pltpu.roll(v_wide, HEAD, 1)
        grad_weights = contract_last(d_o, v_h.astype(bf16))
        row_inner = jnp.sum(weights * grad_weights, axis=-1, keepdims=True)
        grad_scores = (weights * (grad_weights - row_inner)).astype(bf16)
        grad_q = matmul(grad_scores, k) * score_scale
        out_ref[:, h * LANES : (h + 1) * LANES] = _unrope(grad_q, cos, sin, lane).astype(bf16)
        part_k = contract_first(grad_scores, q) * score_scale
        part_v = contract_first(weights.astype(bf16), d_o)
        if h == 1:
            part_v = pltpu.roll(part_v, 2 * LANES - HEAD, 1)
        part_v = part_v[:, :LANES]
        grad_k = part_k if grad_k is None else grad_k + part_k
        grad_v = part_v if grad_v is None else grad_v + part_v
    out_ref[:, 2 * LANES : 3 * LANES] = _unrope(grad_k, cos, sin, lane).astype(bf16)
    out_ref[:, 3 * LANES :] = jnp.where(lane < HEAD, grad_v, 0.0).astype(bf16)


def attend(lengths, qkv, cos, sin):
    blocks, slots, width = qkv.shape
    table = pl.BlockSpec((slots, LANES), lambda s, ln: (0, 0))
    return pl.pallas_call(
        attend_kernel,
        out_shape=jax.ShapeDtypeStruct((blocks, slots, 2 * LANES), bf16),
        grid_spec=pltpu.PrefetchScalarGridSpec(
            num_scalar_prefetch=1,
            grid=(blocks,),
            in_specs=[pl.BlockSpec((None, slots, width), lambda s, ln: (s, 0, 0)), table, table],
            out_specs=pl.BlockSpec((None, slots, 2 * LANES), lambda s, ln: (s, 0, 0)),
        ),
        cost_estimate=pl.CostEstimate(
            flops=blocks * 8 * slots * slots * LANES, bytes_accessed=blocks * slots * width * 6,
            transcendentals=blocks * 2 * slots * slots,
        ),
    )(lengths, qkv, cos, sin)


def attend_back(lengths, qkv, d_o, cos, sin):
    blocks, slots, width = qkv.shape
    table = pl.BlockSpec((slots, LANES), lambda s, ln: (0, 0))
    return pl.pallas_call(
        attend_back_kernel,
        out_shape=jax.ShapeDtypeStruct((blocks, slots, width), bf16),
        grid_spec=pltpu.PrefetchScalarGridSpec(
            num_scalar_prefetch=1,
            grid=(blocks,),
            in_specs=[
                pl.BlockSpec((None, slots, width), lambda s, ln: (s, 0, 0)),
                pl.BlockSpec((None, slots, 2 * LANES), lambda s, ln: (s, 0, 0)),
                table,
                table,
            ],
            out_specs=pl.BlockSpec((None, slots, width), lambda s, ln: (s, 0, 0)),
        ),
        cost_estimate=pl.CostEstimate(
            flops=blocks * 24 * slots * slots * LANES, bytes_accessed=blocks * slots * width * 8,
            transcendentals=blocks * 2 * slots * slots,
        ),
    )(lengths, qkv, d_o, cos, sin)


GATHER_WIDTHS = (3, 4, 5)
SCATTER_WIDTHS = (5, 4, 3)
OUT_WIDTHS = (6, 4, 2)
LOW_WIDTHS = (1, 5, 6)


class Mail:
    def __init__(self, n, send_sems, recv_sems):
        self.me = lax.axis_index("fsdp")
        self.send_sems, self.recv_sems = send_sems, recv_sems
        self.count, self.open = 0, []
        self.peers = {bits: self._peer(bits) for bits in range(1, n)}

    def _peer(self, bits):
        device, bit = self.me, 1
        while bit <= bits:
            if bits & bit:
                device = device + bit * (1 - 2 * ((self.me // bit) % 2))
            bit *= 2
        return device

    def enter(self, bits_list, away, others):
        barrier = pltpu.get_barrier_semaphore()

        @pl.when(away)
        def _():
            for device in others:
                pl.semaphore_signal(
                    barrier, inc=1, device_id=(device,), device_id_type=pl.DeviceIdType.MESH
                )

        for bits in bits_list:
            pl.semaphore_signal(
                barrier,
                inc=1,
                device_id=(self.peers[bits],),
                device_id_type=pl.DeviceIdType.MESH,
            )

        @pl.when(away)
        def _():
            pl.semaphore_wait(barrier, len(bits_list) + len(others))

        @pl.when(jnp.logical_not(away))
        def _():
            pl.semaphore_wait(barrier, len(bits_list))

    def make(self, src, dst, bits):
        copy = pltpu.make_async_remote_copy(
            src_ref=src,
            dst_ref=dst,
            send_sem=self.send_sems.at[self.count],
            recv_sem=self.recv_sems.at[self.count],
            device_id=(self.peers[bits],),
            device_id_type=pl.DeviceIdType.MESH,
        )
        self.count += 1
        self.open.append(copy)
        return copy

    def send(self, src, dst, bits):
        copy = self.make(src, dst, bits)
        copy.start()
        return copy

    def sent(self, copies):
        for copy in copies:
            copy.wait_send()
            self.open = [other for other in self.open if other is not copy]


def take(copies):
    for copy in copies:
        copy.wait_recv()


def xor_place(t, s):
    total = 0
    for bit in (1, 2, 4):
        total = total + bit * (((t // bit) % 2 + (s // bit) % 2) % 2)
    return total


def entry(s):
    if isinstance(s, int):
        return {3: 4, 4: 3}.get(s, s)
    return s + (s // 3) % 2 * (1 - s // 4) - (s // 4) * (1 - (s % 4 + 3) // 4)


def color_bits(color):
    return [1 << ((color + i) % 3) for i in range(3)]


def columns(ref, widths):
    starts = [sum(widths[:color]) for color in range(COLORS)]
    return lambda s, color: ref.at[
        entry(s), :, pl.ds(starts[color] * LANES, widths[color] * LANES)
    ]


class Gather:
    def __init__(self, mail, piece, absolute=False):
        self.mail, self.copies, self.stages = mail, {}, [[], [], []]

        def make(stage, color, slot, bit):
            dst = piece(slot if absolute else slot ^ bit, color)
            self.copies[color, slot ^ bit] = mail.make(piece(slot, color), dst, 2 * bit)
            self.stages[stage].append(self.copies[color, slot ^ bit])

        for i in range(3):
            for color in range(COLORS):
                make(0, color, 0, color_bits(color)[i])
        for color in range(COLORS):
            b1, b2, b3 = color_bits(color)
            make(1, color, b1, b2)
            make(1, color, b1, b3)
            make(2, color, b2, b3)
            make(2, color, b1 ^ b2, b3)

    def start(self):
        for copy in self.stages[0]:
            copy.start()

    def forward(self, stage):
        for color in range(COLORS):
            b1, b2, b3 = color_bits(color)
            for slot in ((b1,), (b2, b1 ^ b2))[stage - 1]:
                self.copies[color, slot].wait_recv()
        for copy in self.stages[stage]:
            copy.start()

    def sent(self):
        self.mail.sent(self.copies.values())

    def near(self):
        for color in range(COLORS):
            self.copies[color, color_bits(color)[2]].wait_recv()

    def far(self, colors=range(COLORS)):
        for color in colors:
            b1, b2, b3 = color_bits(color)
            for slot in (b1 ^ b3, b2 ^ b3, 7):
                self.copies[color, slot].wait_recv()


class Scatter:
    def __init__(self, mail, piece, got):
        self.mail, self.piece, self.got, self.copies = mail, piece, got, {}
        for color in range(COLORS):
            for bit in color_bits(color):
                for s in self._stage(color, bit):
                    self.copies[color, s] = mail.make(piece(s, color), got(s, color), 2 * bit)

    def _stage(self, color, bit):
        b1, b2, b3 = color_bits(color)
        if bit == b1:
            return [s for s in range(CUBE) if s & b1]
        return [b2, b2 ^ b3] if bit == b2 else [b3]

    def start(self, entries):
        for s in entries:
            for color in range(COLORS):
                if s & color_bits(color)[0]:
                    self.copies[color, s].start()

    def _add(self, color, s, bit):
        self.copies[color, s].wait_recv()
        here = self.piece(s ^ bit, color)
        here[...] = (here[...].astype(f32) + self.got(s, color)[...].astype(f32)).astype(here.dtype)

    def second(self):
        for color in range(COLORS):
            b1, b2, b3 = color_bits(color)
            for s in (b2, b2 ^ b3):
                self._add(color, b1 ^ s, b1)
                self.copies[color, s].start()

    def third(self):
        for color in range(COLORS):
            b1, b2, b3 = color_bits(color)
            self._add(color, b1 ^ b3, b1)
            self._add(color, b2 ^ b3, b2)
            self.copies[color, b3].start()

    def total(self, color):
        value = self.piece(0, color)[...].astype(f32)
        for s in color_bits(color):
            self.copies[color, s].wait_recv()
            value = value + self.got(s, color)[...].astype(f32)
        return value

    def sent(self):
        self.mail.sent(self.copies.values())


def lanes_at(values, start, width):
    low = start // LANES * LANES
    high = min(values.shape[1], -(-(start + width) // LANES) * LANES)
    window = values[:, low:high]
    if start > low:
        window = pltpu.roll(window, (high - low) - (start - low), 1)
    return window


def spread(values, width, shift):
    missing = width - values.shape[1]
    if missing > 0:
        values = jnp.concatenate(
            [values, jnp.zeros((values.shape[0], missing), values.dtype)], axis=1
        )
    return pltpu.roll(values, shift, 1) if shift else values


def clear_from(values, lane_count):
    lane = lax.broadcasted_iota(jnp.int32, values.shape, 1)
    return jnp.where(lane < lane_count, values, 0.0)


def heads_of(qkv):
    return [lanes_at(qkv, HEAD * j, HEAD)[:, :LANES] for j in range(4)]


def block_masks(slots, length):
    row = lax.broadcasted_iota(jnp.int32, (slots, slots), 0)
    col = lax.broadcasted_iota(jnp.int32, (slots, slots), 1)
    live = row.astype(f32) < length
    return (col <= row) & live, live


def lane_value(values, index):
    lane = lax.broadcasted_iota(jnp.int32, values.shape, 1)
    return jnp.sum(jnp.where(lane == index, values, 0.0), axis=1, keepdims=True)


def layer_kernel(
    n, x_ref, g_in, len_ref, small_ref, wq_ref, wk_ref, wv_ref, wo_ref, wg_ref, wu_ref, wd_ref,
    cos_ref, sin_ref,
    out_ref, grad_in, gd_ref, gu_slots, qkv_slots, wo_slot,
    h1_all, qkv_all, mixed_all, resid, h2_all, wqkv, gains,
    wout, wgu, wdown, g_all, o_slots, hidden, dgu, dh2, got,
    gu_grad, gu_got, gu_send, gu_far, wd_part, wd_got, wd_send, wd_far, dqkv,
    send_sems, recv_sems, local_sems, owner_sems, core_ready, far_ready, near_ready,
):
    cubes = n // (2 * CUBE)
    mail = Mail(n, send_sems, recv_sems)
    me = mail.me
    core, place, cube = me % 2, (me // 2) % CUBE, me // (2 * CUBE)
    pz, py, px = place // 4, (place // 2) % 2, place % 2
    other_core, other = 1 - core, 1 - cube
    slots, width = x_ref.shape
    rows, down_rows = wo_ref.shape[0], wd_ref.shape[0]
    units = hidden.shape[2]
    far_bits = 2 * CUBE
    owner = 2 * cubes * place + 2 * cube + core
    summed_at = far_bits * ((me // 2) % cubes) + 2 * (me // (2 * cubes)) + core
    away = owner != me
    mail.enter([2 * s for s in range(1, CUBE)] + [1, far_bits], away, [owner, summed_at])

    def small_at(i, low):
        return got.at[i, pl.ds(low, small_ref.shape[0]), pl.ds(0, LANES)]

    def small_add(copy, i, low):
        copy.wait_recv()
        gains[...] += small_at(i, low)[...]

    small_core = mail.send(small_ref, small_at(0, 32), 1)
    gains[...] = small_ref[...]

    h1_all[0] = x_ref[...]
    local = [
        pltpu.make_async_copy(wd_ref, wdown.at[cube, core], local_sems.at[0]),
        pltpu.make_async_copy(wo_ref, wout.at[cube, pz, py, px, core], local_sems.at[1]),
    ]
    for copy in local:
        copy.start()

    query, key, value = (ref[...].astype(f32) for ref in (wq_ref, wk_ref, wv_ref))
    for t in range(CUBE):
        whole = 4 * HEAD
        parts = (
            spread(clear_from(lanes_at(query, 2 * HEAD * t, 2 * HEAD), 2 * HEAD), whole, 0)
            + spread(clear_from(lanes_at(key, HEAD * t, HEAD), HEAD), whole, 2 * HEAD)
            + spread(clear_from(lanes_at(value, HEAD * t, HEAD), HEAD), whole, 3 * HEAD)
        )
        qkv_slots[t] = parts.astype(bf16)
    wqkv[cube, place, core] = qkv_slots[place]
    pack_cps = [
        mail.send(qkv_slots.at[xor_place(place, s)], wqkv.at[cube, place, core], 2 * s)
        for s in range(1, CUBE)
    ]
    small_core.wait_recv()
    mail.sent([small_core])
    gains[...] += small_at(0, 32)[...]
    small_far = mail.send(gains, small_at(1, 32), far_bits)

    x_mail = Gather(mail, columns(h1_all, GATHER_WIDTHS))
    x_mail.start()

    for t in range(CUBE):
        for i in range(2 * cubes):
            start = (((i // 2) * CUBE + t) * 2 + i % 2) * down_rows
            cols = slice(start, start + down_rows)
            gu_send[t // 4, t % 4, :, i * down_rows : (i + 1) * down_rows] = wg_ref[:, cols]
            gu_send[t // 4, t % 4, :, units + i * down_rows : units + (i + 1) * down_rows] = wu_ref[:, cols]
    wgu[cube, place, core] = gu_send[place // 4, place % 4]
    row = lax.broadcasted_iota(jnp.int32, (slots, width), 0)
    g_all[0] = jnp.where(row < len_ref[0, 0], g_in[...].astype(f32), 0.0).astype(bf16)
    small_far.wait_recv()
    mail.sent([small_far])
    gains[...] += small_at(1, 32)[...]
    small_cps = [mail.send(gains, small_at(s - 1, 0), 2 * s) for s in range(1, CUBE)]
    take(pack_cps)
    mail.sent(pack_cps)
    pack_far = mail.send(wqkv.at[cube, :, core], wqkv.at[cube, :, core], far_bits)
    pack_core = [mail.send(wqkv.at[cube, :, core], wqkv.at[cube, :, core], 1)]
    x_mail.forward(1)
    wo_cps = mail.send(wo_ref, wout.at[cube, pz, py, px, core], far_bits)
    gu_cps = [
        mail.send(
            gu_send.at[xor_place(place, s) // 4, xor_place(place, s) % 4],
            wgu.at[cube, place, core],
            2 * s,
        )
        for s in range(1, CUBE)
    ]
    x_mail.forward(2)
    wd_out = mail.send(wd_ref, wdown.at[cube, core], far_bits)
    take(small_cps)
    mail.sent(small_cps)
    for s in range(1, CUBE):
        gains[...] += small_at(s - 1, 0)[...]
    local[1].wait()
    wo_cps.wait_recv()

    def wo_piece(s, color):
        at = [(p + (s >> i) % 2) % 2 for i, p in ((2, pz), (1, py), (0, px))]
        widths = GATHER_WIDTHS
        start = sum(widths[:color])
        return wout.at[
            :, at[0], at[1], at[2], core, :, pl.ds(start * LANES, widths[color] * LANES)
        ]

    wo_mail = Gather(mail, wo_piece, absolute=True)
    pack_far.wait_recv()
    pack_core.append(mail.send(wqkv.at[other, :, core], wqkv.at[other, :, core], 1))
    x_mail.near()
    x_mail.far()
    wo_mail.start()
    g_mail = Gather(mail, columns(g_all, GATHER_WIDTHS))
    g_mail.start()
    take(pack_core)
    x_mail.sent()

    def row_of(first):
        return jnp.concatenate([gains[first + i : first + i + 1, :] for i in range(width // LANES)], axis=1)

    gain_attn, gain_mlp = row_of(0), row_of(width // LANES)
    lengths = gains[2 * (width // LANES) : 2 * (width // LANES) + 1, :]
    gu_out = mail.make(wgu.at[cube, :, core], wgu.at[cube, :, core], far_bits)

    def attention(s, carry):
        values = h1_all[s].astype(f32)
        normed = (rms_parts(values)[0] * gain_attn).astype(bf16)
        h1_all[s] = normed
        projected = heads_of(matmul(normed, wqkv[...].reshape(width, 4 * HEAD)))
        there = far_bits * cube + 2 * xor_place(place, entry(s)) + core
        visible, live = block_masks(slots, lane_value(lengths, there))
        lane = lax.broadcasted_iota(jnp.int32, (slots, LANES), 1)
        cos, sin = cos_ref[...], sin_ref[...]
        for j in range(3):
            qkv_all[s, :, j * LANES : (j + 1) * LANES] = _rope(projected[j], cos, sin, lane).astype(bf16)
        value = clear_from(projected[3], HEAD)
        qkv_all[s, :, 3 * LANES :] = value.astype(bf16)
        k = qkv_all[s, :, 2 * LANES : 3 * LANES]
        v_wide = _wide(value)
        mixed = None
        for h in range(2):
            q = qkv_all[s, :, h * LANES : (h + 1) * LANES]
            weights = _weights(q, k, visible, live).astype(bf16)
            v_h = pltpu.roll(v_wide, HEAD, 1) if h else v_wide
            part = matmul(weights, v_h.astype(bf16))
            mixed = part if mixed is None else mixed + part
        mixed_all[s] = mixed.astype(bf16)

        @pl.when(s == 4)
        def _():
            take(gu_cps)
            gu_out.start()

        @pl.when(s == 6)
        def _():
            wo_mail.forward(1)

        return carry

    lax.fori_loop(0, CUBE, attention, 0)

    o_cps = [mail.send(mixed_all.at[entry(s)], o_slots.at[place], 2 * s) for s in range(1, CUBE)]
    o_slots[place] = mixed_all[0]
    wo_mail.forward(2)
    local[0].wait()
    wd_out.wait_recv()
    wd_core = mail.send(wdown.at[:, core], wdown.at[:, core], 1)
    take(o_cps)
    g_mail.forward(1)
    wide = []
    for j in range(CUBE // 2):
        low = spread(o_slots[2 * j].astype(f32), 3 * LANES, 0)
        high = spread(o_slots[2 * j + 1].astype(f32), 3 * LANES, 2 * HEAD)
        wide.append((low + high).astype(bf16))
    attended = jnp.concatenate(wide, axis=1)
    wo_mail.near()
    wo_c = []
    for color in range(COLORS):
        wo_mail.far([color])
        start = sum(GATHER_WIDTHS[:color])
        part = wout.at[
            :, :, :, :, core, :, pl.ds(start * LANES, GATHER_WIDTHS[color] * LANES)
        ]
        wo_c.append(mail.send(part, part, 1))
    take(wo_c)
    step = 256
    for j in range(width // step):
        cols = slice(j * step, (j + 1) * step)
        weight = wout[:, :, :, :, :, :, cols].reshape(width, step)
        resid[:, cols] = x_ref[:, cols].astype(f32) + matmul(attended, weight)
    h2_all[0] = (rms_parts(resid[...])[0] * gain_mlp).astype(bf16)
    h2_mail = Gather(mail, columns(h2_all, GATHER_WIDTHS))
    h2_mail.start()
    g_mail.forward(2)
    h2_mail.forward(1)
    gu_out.wait_recv()
    gu_core = mail.send(wgu.at[:, :, core], wgu.at[:, :, core], 1)
    h2_mail.forward(2)
    wd_core.wait_recv()
    gu_core.wait_recv()
    g_mail.near()
    h2_mail.near()

    got_columns = columns(got, SCATTER_WIDTHS)
    back = Scatter(
        mail, columns(dh2, SCATTER_WIDTHS), lambda s, color: got_columns(entry(s - 1), color)
    )

    def feed_forward(half):
        step = 256
        tokens = CUBE // 2 * slots
        here = slice(half * CUBE // 2, (half + 1) * CUBE // 2)

        def split(values):
            return values.reshape(CUBE // 2, slots, values.shape[1])

        for j in range(units // step):
            cols = slice(j * step, (j + 1) * step)
            up_cols = slice(units + j * step, units + (j + 1) * step)
            lhs = h2_all[here].reshape(tokens, width)
            gate = matmul(lhs, wgu[:, :, :, :, cols].reshape(width, step))
            up = matmul(lhs, wgu[:, :, :, :, up_cols].reshape(width, step))
            down = wdown[...].reshape(units, width)[cols]
            grad_hidden = contract_last(g_all[here].reshape(tokens, width), down)
            sigmoid_gate = jax.nn.sigmoid(gate)
            silu = gate * sigmoid_gate
            hidden[here, :, cols] = split((silu * up).astype(bf16))
            dgu[here, :, cols] = split(
                (grad_hidden * up * sigmoid_gate * (1.0 + gate * (1.0 - sigmoid_gate))).astype(bf16)
            )
            dgu[here, :, up_cols] = split((grad_hidden * silu).astype(bf16))
        for j in range(4):
            part = width // 4
            weight = wgu[j // 2, (j % 2) * (CUBE // 2) : (j % 2 + 1) * (CUBE // 2)]
            grad = contract_last(
                dgu[here].reshape(tokens, 2 * units), weight.reshape(part, 2 * units)
            )
            dh2[here, :, j * part : (j + 1) * part] = split(grad)
        back.start([entry(i) for i in range(half * CUBE // 2, (half + 1) * CUBE // 2)])

    feed_forward(0)
    g_mail.far()
    h2_mail.far()
    feed_forward(1)

    g_mail.sent()
    h2_mail.sent()
    wo_mail.sent()
    mail.sent([wo_cps, *wo_c])
    d_all = dgu[...].reshape(CUBE * slots, 2 * units)
    chunk = width // 4
    for j in range(4):
        lhs = h2_all[:, :, j * chunk : (j + 1) * chunk].reshape(CUBE * slots, chunk)
        gu_grad[j // 2, j % 2] = contract_first(lhs, d_all).reshape(gu_grad.shape[2:])
    gu_own_cps = gu_cps
    gu_cps = gu_core_cps = mail.send(gu_grad.at[:, :, :, other_core], gu_got, 1)
    hid_all = hidden[...].reshape(CUBE * slots, units)
    for j in range(4):
        cols = slice(j * chunk, (j + 1) * chunk)
        g_cols = g_all[:, :, cols].reshape(CUBE * slots, chunk)
        wd_part[:, :, :, cols] = contract_first(hid_all, g_cols).reshape(cubes, 2, down_rows, chunk)
    wd_cps = wd_core_cps = mail.send(wd_part.at[:, other_core], wd_got, 1)
    for i in range(2):
        half = slice(i * CUBE // 2, (i + 1) * CUBE // 2)
        lhs = hidden[half].reshape(CUBE // 2 * slots, units)
        for j in range(4):
            cols = slice(j * chunk, (j + 1) * chunk)
            part = matmul(lhs, wdown[:, :, :, cols].reshape(units, chunk))
            h2_all[half, :, cols] = part.reshape(CUBE // 2, slots, chunk).astype(bf16)
    gu_cps.wait_recv()
    mail.sent(gu_own_cps)
    gu_send[...] = (gu_grad[other, :, :, core] + gu_got[other]).astype(bf16)
    gu_cps = gu_far_cps = mail.send(gu_send, gu_far, far_bits)
    wd_cps.wait_recv()
    wd_send[...] = (wd_part[other, core] + wd_got[other]).astype(bf16)
    wd_cps = wd_far_cps = mail.send(wd_send, wd_far, far_bits)

    def out_got(s, color):
        if color == 1:
            return hidden.at[entry(s)]
        start, part = ((0, 768), None, (768, 256))[color]
        return dgu.at[entry(s), :, pl.ds(start, part)]

    out_piece = columns(h2_all, OUT_WIDTHS)
    out_mail = Scatter(mail, out_piece, out_got)
    for bit in (1, 2, 4):
        pl.semaphore_signal(
            near_ready,
            inc=1,
            device_id=(mail.peers[2 * bit],),
            device_id_type=pl.DeviceIdType.MESH,
        )
    back.second()
    pl.semaphore_wait(near_ready, 3)
    out_mail.start(range(CUBE))
    back.third()

    unit, inverse = rms_parts(resid[...])
    for color in range(COLORS):
        columns(dh2, SCATTER_WIDTHS)(0, color)[...] = back.total(color)
    grad_in[...] = g_all[0].astype(f32) + rms_back(dh2[0], unit, inverse, gain_mlp)
    low = grad_in[...].astype(bf16)
    g_all[0] = low
    for t in range(CUBE):
        weight = wout[t // 4, (t // 2) % 2, t % 2].reshape(2 * HEAD, width)
        dqkv[t, :, : 2 * LANES] = spread(contract_last(low, weight), 2 * LANES, 0).astype(bf16)
    do_cps = [
        mail.send(dqkv.at[xor_place(place, s), :, pl.ds(0, 2 * LANES)], o_slots.at[entry(s)], 2 * s)
        for s in range(1, CUBE)
    ]
    o_slots[0] = dqkv[place, :, : 2 * LANES]
    out_mail.second()

    gu_cps.wait_recv()
    mail.sent([gu_far_cps])
    gu_send[...] = (
        gu_grad[cube, :, :, core] + gu_got[cube] + gu_far[...].astype(f32)
    ).astype(bf16)
    wd_cps.wait_recv()
    gd_ref[...] = wd_part[cube, core] + wd_got[cube] + wd_far[...].astype(f32)
    for ready, bits in ((core_ready, 1), (far_ready, far_bits)):
        pl.semaphore_signal(
            ready, inc=1, device_id=(mail.peers[bits],), device_id_type=pl.DeviceIdType.MESH
        )
    gu_cps = [
        mail.send(
            gu_send.at[xor_place(place, s) // 4, xor_place(place, s) % 4], gu_slots.at[place], 2 * s
        )
        for s in range(1, CUBE)
    ]
    gu_slots[place] = gu_send[place // 4, place % 4]
    take(do_cps)
    mail.sent(do_cps)
    low_mail = Gather(mail, columns(g_all, LOW_WIDTHS))
    low_mail.start()

    def attention_back(s, carry):
        there = far_bits * cube + 2 * xor_place(place, entry(s)) + core
        visible, live = block_masks(slots, lane_value(lengths, there))
        lane = lax.broadcasted_iota(jnp.int32, (slots, LANES), 1)
        cos, sin = cos_ref[...], sin_ref[...]
        k = qkv_all[s, :, 2 * LANES : 3 * LANES]
        v_wide = _wide(qkv_all[s, :, 3 * LANES :].astype(f32))
        grad_o = o_slots[s]
        grad_k = grad_v = total = None
        for h in range(2):
            q = qkv_all[s, :, h * LANES : (h + 1) * LANES]
            weights = _weights(q, k, visible, live)
            v_h = pltpu.roll(v_wide, HEAD, 1) if h else v_wide
            grad_weights = contract_last(grad_o, v_h.astype(bf16))
            row_inner = jnp.sum(weights * grad_weights, axis=-1, keepdims=True)
            grad_scores = (weights * (grad_weights - row_inner)).astype(bf16)
            grad_q = _unrope(matmul(grad_scores, k) * score_scale, cos, sin, lane)
            part_k = contract_first(grad_scores, q) * score_scale
            part_v = contract_first(weights.astype(bf16), grad_o)
            if h:
                part_v = pltpu.roll(part_v, 2 * LANES - HEAD, 1)
            part_v = part_v[:, :LANES]
            grad_q = spread(grad_q, 4 * HEAD, h * HEAD)
            total = grad_q if total is None else total + grad_q
            grad_k = part_k if grad_k is None else grad_k + part_k
            grad_v = part_v if grad_v is None else grad_v + part_v
        total = total + spread(_unrope(grad_k, cos, sin, lane), 4 * HEAD, 2 * HEAD)
        total = total + spread(clear_from(grad_v, HEAD), 4 * HEAD, 3 * HEAD)
        dqkv[s] = total.astype(bf16)

        return carry

    lax.fori_loop(0, CUBE, attention_back, 0)
    out_mail.third()

    pl.semaphore_wait(core_ready, 1)
    mail.sent([gu_core_cps, wd_core_cps])
    qkv_all_grad = dqkv[...].reshape(CUBE * slots, 4 * HEAD)
    narrow = slice(0, 4 * HEAD)
    for j in range(4):
        lhs = h1_all[:, :, j * chunk : (j + 1) * chunk].reshape(CUBE * slots, chunk)
        gu_grad[j // 2, j % 2, :, :, :, narrow] = contract_first(lhs, qkv_all_grad).reshape(
            CUBE // 2, 2, rows, 4 * HEAD
        )
    qkv_cps = mail.send(
        gu_grad.at[:, :, :, other_core, :, narrow], gu_got.at[:, :, :, :, narrow], 1
    )
    for i in range(2):
        half = slice(i * CUBE // 2, (i + 1) * CUBE // 2)
        lhs = dqkv[half].reshape(CUBE // 2 * slots, 4 * HEAD)
        for j in range(2):
            part = width // 2
            grad = contract_last(lhs, wqkv[j].reshape(part, 4 * HEAD))
            h1_all[half, :, j * part : (j + 1) * part] = grad.reshape(
                CUBE // 2, slots, part
            ).astype(bf16)

    cuts = (0, 48, 96, slots)

    def in_piece(s, color):
        return h1_all.at[entry(s), pl.ds(cuts[color], cuts[color + 1] - cuts[color])]

    def in_got(s, color):
        i = COLORS * s + color
        slot = wout.at[i // 16, (i // 8) % 2, (i // 4) % 2, (i // 2) % 2, i % 2]
        return slot.at[pl.ds(0, cuts[color + 1] - cuts[color])]

    in_mail = Scatter(mail, in_piece, in_got)
    in_mail.start(range(CUBE))
    qkv_cps.wait_recv()
    pl.semaphore_wait(far_ready, 1)
    mail.sent([*gu_cps, wd_far_cps])
    gu_send[:, :, :, narrow] = (
        gu_grad[other, :, :, core, :, narrow] + gu_got[other, :, :, :, narrow]
    ).astype(bf16)
    qkv_cps = mail.send(
        gu_send.at[:, :, :, narrow], gu_far.at[:, :, :, narrow], far_bits
    )
    low_mail.forward(1)
    low_mail.forward(2)
    in_mail.second()

    low_mail.near()
    low_mail.far()
    mixed = mixed_all[...].reshape(CUBE * slots, 2 * LANES)
    for j in range(4):
        cols = slice(j * chunk, (j + 1) * chunk)
        g_cols = g_all[:, :, cols].reshape(CUBE * slots, chunk)
        wd_part[:, :, :rows, cols] = contract_first(mixed, g_cols)[: 2 * HEAD].reshape(
            cubes, 2, rows, chunk
        )
    wo_cps = mail.send(wd_part.at[:, other_core, pl.ds(0, rows)], wd_got.at[:, pl.ds(0, rows)], 1)
    wo_cps.wait_recv()
    wd_send[:rows] = (wd_part[other, core, :rows] + wd_got[other, :rows]).astype(bf16)
    wo_cps = mail.send(wd_send.at[pl.ds(0, rows)], wd_far.at[pl.ds(0, rows)], far_bits)
    qkv_cps.wait_recv()
    gu_far[:, :, :, narrow] = (
        gu_grad[cube, :, :, core, :, narrow]
        + gu_got[cube, :, :, :, narrow]
        + gu_far[:, :, :, narrow].astype(f32)
    ).astype(bf16)
    qkv_cps = [
        mail.send(
            gu_far.at[xor_place(place, s) // 4, xor_place(place, s) % 4, :, narrow],
            qkv_slots.at[place],
            2 * s,
        )
        for s in range(1, CUBE)
    ]
    qkv_slots[place] = gu_far[place // 4, place % 4, :, narrow]
    in_mail.third()
    wo_cps.wait_recv()
    wd_far[:rows] = (
        wd_part[cube, core, :rows] + wd_got[cube, :rows] + wd_far[:rows].astype(f32)
    ).astype(bf16)
    wo_copy = pltpu.make_async_remote_copy(
        src_ref=wd_far.at[pl.ds(0, rows)],
        dst_ref=wo_slot,
        send_sem=owner_sems.at[0],
        recv_sem=owner_sems.at[1],
        device_id=(owner,),
        device_id_type=pl.DeviceIdType.MESH,
    )

    @pl.when(away)
    def _():
        wo_copy.start()

    @pl.when(owner == me)
    def _():
        wo_slot[...] = wd_far[:rows]

    take(gu_cps)
    take(qkv_cps)

    @pl.when(away)
    def _():
        wo_copy.wait_recv()
        wo_copy.wait_send()

    unit, inverse = rms_parts(x_ref[...].astype(f32))
    for color in range(COLORS):
        dh2[0, cuts[color] : cuts[color + 1]] = in_mail.total(color)
    grad_in[...] += rms_back(dh2[0], unit, inverse, gain_attn)
    for color in range(COLORS):
        low = sum(OUT_WIDTHS[:color]) * LANES
        here = slice(low, low + OUT_WIDTHS[color] * LANES)
        out_ref[:, here] = (resid[:, here] + out_mail.total(color)).astype(bf16)
    mail.sent(mail.open)


def finish_kernel(
    cubes, out_in, grad_in, gd_in, gu_slots, qkv_slots, wo_slot, wq_ref, wk_ref, wv_ref, wg_ref,
    wu_ref, norm_attn_ref, norm_mlp_ref,
    out_ref, grad_ref, attn_ref, gq_ref, gk_ref, gv_ref, go_ref, mlp_ref, gg_ref, gup_ref, gd_ref,
):
    rows, units = wg_ref.shape[0], gu_slots.shape[2] // 2
    down_rows = units // (2 * cubes)
    out_ref[...] = out_in[...]
    grad_ref[...] = grad_in[...]
    gd_ref[...] = gd_in[...]
    go_ref[...] = wo_slot[...].astype(f32)
    for t in range(CUBE):
        for i in range(2 * cubes):
            start = (((i // 2) * CUBE + t) * 2 + i % 2) * down_rows
            cols = slice(start, start + down_rows)
            gg_ref[:, cols] = gu_slots[t, :, i * down_rows : (i + 1) * down_rows].astype(f32)
            gup_ref[:, cols] = gu_slots[
                t, :, units + i * down_rows : units + (i + 1) * down_rows
            ].astype(f32)
    whole = 4 * HEAD
    for j in range(CUBE // 2):
        pair = [qkv_slots[2 * j + i].astype(f32) for i in range(2)]
        gq_ref[:, j * whole : (j + 1) * whole] = sum(
            spread(clear_from(values, 2 * HEAD), whole, 2 * HEAD * i)
            for i, values in enumerate(pair)
        )
    for j in range(2):
        four = [qkv_slots[4 * j + i].astype(f32) for i in range(4)]
        for ref, start in ((gk_ref, 2 * HEAD), (gv_ref, 3 * HEAD)):
            ref[:, j * whole : (j + 1) * whole] = sum(
                spread(clear_from(lanes_at(values, start, HEAD), HEAD), whole, HEAD * i)
                for i, values in enumerate(four)
            )

    diagonal = lax.broadcasted_iota(jnp.int32, (rows, rows), 0) == lax.broadcasted_iota(
        jnp.int32, (rows, rows), 1
    )

    def gain_grad(pairs, norm_ref):
        total = sum(
            jnp.sum(weight[...].astype(f32) * grad[...], axis=1, keepdims=True)
            for weight, grad in pairs
        )
        row = jnp.sum(jnp.where(diagonal, total, 0.0), axis=0, keepdims=True)
        return row / norm_ref[...].astype(f32)

    attn_ref[...] = gain_grad(
        ((wq_ref, gq_ref), (wk_ref, gk_ref), (wv_ref, gv_ref)), norm_attn_ref
    )
    mlp_ref[...] = gain_grad(((wg_ref, gg_ref), (wu_ref, gup_ref)), norm_mlp_ref)


def per_device_any(
    n,
    layer_input,
    out_cotangent,
    lengths,
    norm_attn,
    w_query,
    w_key,
    w_value,
    w_out,
    norm_mlp,
    w_gate,
    w_up,
    w_down,
):
    cubes = n // (2 * CUBE)
    slots, width = layer_input.shape
    rows = w_query.shape[0]
    down_rows = w_down.shape[0]
    q_cols, kv_cols = w_query.shape[1] // CUBE, w_key.shape[1] // CUBE
    me = lax.axis_index("fsdp")
    core, place, cube = me % 2, (me // 2) % CUBE, me // (2 * CUBE)

    def swap(array, bits):
        return lax.ppermute(array, "fsdp", [(i, i ^ bits) for i in range(n)])

    def cube_gather(block):
        part = block.shape[1] // COLORS
        columns = []
        for color in range(COLORS):
            order = [(color + i) % 3 for i in range(3)]
            held, names = block[None, :, color * part : (color + 1) * part], [0]
            for bit in order:
                held = jnp.concatenate([held, swap(held, 2 << bit)], axis=0)
                names = names + [name ^ (1 << bit) for name in names]
            columns.append((held, names))
        return jnp.stack(
            [
                jnp.concatenate([held[names.index(s)] for held, names in columns], axis=1)
                for s in range(CUBE)
            ]
        )

    def cube_scatter(blocks):
        part = blocks.shape[2] // COLORS
        columns = []
        for color in range(COLORS):
            order = [(color + i) % 3 for i in range(3)]
            held = {s: blocks[s, :, color * part : (color + 1) * part] for s in range(CUBE)}
            for bit in order:
                send = [s for s in held if s & (1 << bit)]
                got = swap(jnp.stack([held[s] for s in send]), 2 << bit)
                for i, s in enumerate(send):
                    held[s ^ (1 << bit)] = held[s ^ (1 << bit)] + got[i]
                    del held[s]
            columns.append(held[0])
        return jnp.concatenate(columns, axis=1)

    def cube_exchange(blocks):
        return jnp.stack([blocks[0]] + [swap(blocks[s], 2 * s) for s in range(1, CUBE)])

    relative = jnp.arange(CUBE, dtype=jnp.int32) ^ place

    def by_place(blocks):
        return jnp.take(blocks, relative, axis=0, indices_are_sorted=False, unique_indices=True)

    def group_gather(block):
        held = jnp.stack([block] + [swap(block, 2 * CUBE * s) for s in range(1, cubes)])
        return jnp.stack([held, swap(held, 1)])

    owner = jnp.arange(n, dtype=jnp.int32)
    from_me = owner ^ me
    owner_entry = ((from_me % 2) * cubes + from_me // (2 * CUBE)) * CUBE + (from_me // 2) % CUBE
    pair = jnp.arange(2 * cubes, dtype=jnp.int32)
    pair_entry = ((pair % 2) ^ core) * cubes + ((pair // 2) ^ cube)

    def all_rows(block):
        held = group_gather(block).reshape(n, *block.shape[1:])
        return jnp.take(held, owner_entry, axis=0, unique_indices=True)

    small = jnp.concatenate(
        [norm_attn, norm_mlp, lengths[0].astype(bf16), jnp.zeros((LANES - 2 * rows - 1,), bf16)]
    )[None]
    bit = 1
    while bit < n:
        small = jnp.concatenate([small, swap(small, bit)], axis=0)
        bit *= 2
    cube_lengths = small[0 : 2 * CUBE : 2, 2 * rows].astype(jnp.int32)
    gains = jnp.take(small, from_me, axis=0)
    gain_attn = gains[:, :rows].reshape(width).astype(f32)
    gain_mlp = gains[:, rows : 2 * rows].reshape(width).astype(f32)
    cos, sin = rope_tables(slots)

    x_all = cube_gather(layer_input)
    own_qkv = jnp.concatenate(
        [
            w_query.reshape(rows, CUBE, q_cols),
            w_key.reshape(rows, CUBE, kv_cols),
            w_value.reshape(rows, CUBE, kv_cols),
        ],
        axis=2,
    ).transpose(1, 0, 2)
    w_qkv = all_rows(cube_exchange(by_place(own_qkv))).reshape(width, q_cols + 2 * kv_cols)
    w_qkv = jnp.pad(
        w_qkv.reshape(width, 4, HEAD), ((0, 0), (0, 0), (0, LANES - HEAD))
    ).reshape(width, 4 * LANES)

    out_held = jnp.stack([w_out] + [swap(w_out, 2 * CUBE * s) for s in range(1, cubes)])
    out_held = out_held.reshape(1, cubes, rows, width)
    for bit in range(3):
        out_held = jnp.concatenate([out_held, swap(out_held, 2 << bit)], axis=0)
    out_held = jnp.stack([out_held, swap(out_held, 1)])
    out_entry = ((from_me % 2) * CUBE + (from_me // 2) % CUBE) * cubes + from_me // (2 * CUBE)
    full_out = jnp.take(out_held.reshape(n, rows, width), out_entry, axis=0, unique_indices=True)
    full_out = jnp.pad(
        full_out.reshape(CUBE, q_cols, width), ((0, 0), (0, 2 * LANES - q_cols), (0, 0))
    ).reshape(CUBE * 2 * LANES, width)

    ff_cols = 2 * cubes * down_rows

    def by_hidden(weight):
        split = weight.reshape(rows, cubes, CUBE, 2, down_rows)
        return split.transpose(2, 0, 1, 3, 4).reshape(CUBE, rows, ff_cols)

    own_gate_up = jnp.concatenate([by_hidden(w_gate), by_hidden(w_up)], axis=2)
    w_gate_up = all_rows(cube_exchange(by_place(own_gate_up))).reshape(width, 2 * ff_cols)
    down_held = group_gather(w_down).reshape(2 * cubes, down_rows, width)
    down = jnp.take(down_held, pair_entry, axis=0, unique_indices=True).reshape(ff_cols, width)

    live = jnp.arange(slots, dtype=jnp.int32)[:, None] < lengths[0, 0]
    cotangent = jnp.where(live, out_cotangent, jnp.zeros_like(out_cotangent))
    g_all = cube_gather(cotangent).reshape(CUBE * slots, width)

    inputs = layer_input.astype(f32)
    unit_all, _ = rms_parts(x_all.reshape(CUBE * slots, width).astype(f32))
    normed_all = (unit_all * gain_attn).astype(bf16)
    qkv = matmul(normed_all, w_qkv).reshape(CUBE, slots, 4 * LANES)
    mixed = attend(cube_lengths, qkv, cos, sin)
    attended = by_place(cube_exchange(mixed)).transpose(1, 0, 2).reshape(slots, CUBE * 2 * LANES)
    residual = inputs + matmul(attended, full_out)
    unit_mlp, inv_mlp = rms_parts(residual)
    normed_mlp = cube_gather((unit_mlp * gain_mlp).astype(bf16)).reshape(CUBE * slots, width)

    gate_up = matmul(normed_mlp, w_gate_up)
    gate, up = gate_up[:, :ff_cols], gate_up[:, ff_cols:]
    sigmoid_gate = jax.nn.sigmoid(gate)
    hidden = (gate * sigmoid_gate * up).astype(bf16)
    grad_hidden = contract_last(g_all, down)
    grad_gate = (grad_hidden * up * sigmoid_gate * (1.0 + gate * (1.0 - sigmoid_gate))).astype(bf16)
    grad_up = (grad_hidden * gate * sigmoid_gate).astype(bf16)
    grad_gate_up = jnp.concatenate([grad_gate, grad_up], axis=1)
    grad_normed_mlp = cube_scatter(
        contract_last(grad_gate_up, w_gate_up).reshape(CUBE, slots, width)
    )
    grad_resid = cotangent.astype(f32) + rms_back(grad_normed_mlp, unit_mlp, inv_mlp, gain_mlp)
    grad_resid_low = grad_resid.astype(bf16)

    grad_attended = contract_last(grad_resid_low, full_out).astype(bf16)
    grad_blocks = by_place(grad_attended.reshape(slots, CUBE, 2 * LANES).transpose(1, 0, 2))
    grad_mixed = cube_exchange(grad_blocks)
    grad_qkv = attend_back(cube_lengths, qkv, grad_mixed, cos, sin).reshape(
        CUBE * slots, 4 * LANES
    )

    def low_sum(blocks):
        total = blocks[0]
        for s in range(1, CUBE):
            total = total + swap(blocks[s].astype(bf16), 2 * s).astype(f32)
        return total

    output = (
        residual + low_sum(matmul(hidden, down).reshape(CUBE, slots, width))
    ).astype(bf16)
    grad_normed = low_sum(contract_last(grad_qkv, w_qkv).reshape(CUBE, slots, width))
    unit_attn, inv_attn = rms_parts(inputs)
    grad_input = grad_resid + rms_back(grad_normed, unit_attn, inv_attn, gain_attn)

    def group_sum(blocks, core_axis):
        pick = functools.partial(
            lax.dynamic_index_in_dim, axis=core_axis + 1, keepdims=False
        )
        pair_total = pick(blocks, core) + swap(pick(blocks, 1 - core), 1)
        total = lax.dynamic_index_in_dim(pair_total, cube, axis=0, keepdims=False)
        for s in range(1, cubes):
            send = lax.dynamic_index_in_dim(pair_total, cube ^ s, axis=0, keepdims=False)
            total = total + swap(send.astype(bf16), 2 * CUBE * s).astype(f32)
        return total

    grad_down = group_sum(
        contract_first(hidden, g_all).reshape(cubes, 2, down_rows, width), 0
    )

    def to_owners(partial):
        cols = partial.shape[1]
        total = group_sum(partial.reshape(cubes, CUBE, 2, rows, cols), 1)
        return by_place(cube_exchange(by_place(total.astype(bf16)))).astype(f32)

    grad_gu = to_owners(contract_first(normed_mlp, grad_gate_up))

    def hidden_back(block):
        return block.reshape(CUBE, rows, cubes, 2, down_rows).transpose(1, 2, 0, 3, 4).reshape(
            rows, cubes * CUBE * 2 * down_rows
        )

    grad_w_gate, grad_w_up = hidden_back(grad_gu[:, :, :ff_cols]), hidden_back(grad_gu[:, :, ff_cols:])

    grad_w = to_owners(contract_first(normed_all, grad_qkv))
    grad_heads = grad_w.reshape(CUBE, rows, 4, LANES)[:, :, :, :HEAD].transpose(1, 2, 0, 3)
    grad_w_query = grad_heads[:, :2].transpose(0, 2, 1, 3).reshape(rows, CUBE * q_cols)
    grad_w_key = grad_heads[:, 2].reshape(rows, CUBE * kv_cols)
    grad_w_value = grad_heads[:, 3].reshape(rows, CUBE * kv_cols)

    resid_low_all = cube_gather(grad_resid_low).reshape(CUBE * slots, width)
    grad_out_part = contract_first(mixed.reshape(CUBE * slots, 2 * LANES), resid_low_all)[:q_cols]
    grad_out_sum = group_sum(grad_out_part.reshape(cubes, 2, rows, width), 0)
    moves = [
        (2 * CUBE * g + 2 * t + c, 2 * cubes * t + 2 * g + c)
        for g in range(cubes)
        for t in range(CUBE)
        for c in range(2)
    ]
    grad_w_out = lax.ppermute(grad_out_sum.astype(bf16), "fsdp", moves).astype(f32)

    def gain_grad(gain, pairs):
        total = sum(jnp.sum(weight.astype(f32) * grad, axis=1) for weight, grad in pairs)
        return total / gain.astype(f32)

    gain_attn_grad = gain_grad(
        norm_attn, [(w_query, grad_w_query), (w_key, grad_w_key), (w_value, grad_w_value)]
    )
    gain_mlp_grad = gain_grad(norm_mlp, [(w_gate, grad_w_gate), (w_up, grad_w_up)])
    return (
        output,
        grad_input,
        gain_attn_grad,
        grad_w_query,
        grad_w_key,
        grad_w_value,
        grad_w_out,
        gain_mlp_grad,
        grad_w_gate,
        grad_w_up,
        grad_down,
    )


def per_device_fast(
    n,
    layer_input,
    out_cotangent,
    lengths,
    norm_attn,
    w_query,
    w_key,
    w_value,
    w_out,
    norm_mlp,
    w_gate,
    w_up,
    w_down,
):
    cubes = n // (2 * CUBE)
    slots, width = layer_input.shape
    rows, down_rows = w_query.shape[0], w_down.shape[0]
    units, qkv_cols = 2 * cubes * down_rows, 4 * HEAD
    me = lax.axis_index("fsdp")
    own = jnp.arange(width, dtype=jnp.int32) // rows == me
    small = [jnp.where(own, jnp.tile(norm, n), 0).astype(f32) for norm in (norm_attn, norm_mlp)]
    small.append(jnp.where(jnp.arange(1024) == me, lengths[0], 0).astype(f32))
    small = jnp.concatenate(small).reshape(-1, LANES)
    cos, sin = rope_tables(slots)

    vmem = pl.BlockSpec(memory_space=pltpu.VMEM)
    smem = pl.BlockSpec(memory_space=pltpu.SMEM)
    hbm = pl.BlockSpec(memory_space=pl.ANY)
    outs = [
        ((slots, width), bf16),
        ((slots, width), f32),
        ((down_rows, width), f32),
        ((CUBE, rows, 2 * units), bf16),
        ((CUBE, rows, qkv_cols), bf16),
        ((rows, width), bf16),
    ]
    half = (2, CUBE // 2, rows, 2 * units)
    scratch = [
        ((CUBE, slots, width), bf16),
        ((CUBE, slots, 4 * LANES), bf16),
        ((CUBE, slots, 2 * LANES), bf16),
        ((slots, width), f32),
        ((CUBE, slots, width), bf16),
        ((cubes, CUBE, 2, rows, qkv_cols), bf16),
        ((2 * width // LANES + 8, LANES), f32),
        ((cubes, 2, 2, 2, 2, rows, width), bf16),
        ((cubes, CUBE, 2, rows, 2 * units), bf16),
        ((cubes, 2, down_rows, width), bf16),
        ((CUBE, slots, width), bf16),
        ((CUBE, slots, 2 * LANES), bf16),
        ((CUBE, slots, units), bf16),
        ((CUBE, slots, 2 * units), bf16),
        ((CUBE, slots, width), f32),
        ((CUBE - 1, slots, width), f32),
        ((cubes, 2, CUBE // 2, 2, rows, 2 * units), f32),
        ((cubes,) + half, f32),
        (half, bf16),
        (half, bf16),
        ((cubes, 2, down_rows, width), f32),
        ((cubes, down_rows, width), f32),
        ((down_rows, width), bf16),
        ((down_rows, width), bf16),
        ((CUBE, slots, qkv_cols), bf16),
    ]
    messages = 256
    parts = pl.pallas_call(
        functools.partial(layer_kernel, n),
        out_shape=[jax.ShapeDtypeStruct(*shape) for shape in outs],
        in_specs=[vmem, vmem, smem, vmem, vmem, vmem, vmem, hbm, vmem, vmem, hbm, vmem, vmem],
        out_specs=[vmem] * len(outs),
        scratch_shapes=[pltpu.VMEM(*shape) for shape in scratch]
        + [
            pltpu.SemaphoreType.DMA((messages,)),
            pltpu.SemaphoreType.DMA((messages,)),
            pltpu.SemaphoreType.DMA((2,)),
            pltpu.SemaphoreType.DMA((2,)),
            pltpu.SemaphoreType.REGULAR,
            pltpu.SemaphoreType.REGULAR,
            pltpu.SemaphoreType.REGULAR,
        ],
        compiler_params=pltpu.CompilerParams(
            collective_id=0, has_side_effects=True, vmem_limit_bytes=67043328
        ),
    )(
        layer_input, out_cotangent, lengths, small, w_query, w_key, w_value, w_out, w_gate, w_up,
        w_down, cos, sin,
    )
    finals = [
        ((slots, width), bf16),
        ((slots, width), f32),
        ((1, rows), f32),
        (w_query.shape, f32),
        (w_key.shape, f32),
        (w_value.shape, f32),
        (w_out.shape, f32),
        ((1, rows), f32),
        (w_gate.shape, f32),
        (w_up.shape, f32),
        (w_down.shape, f32),
    ]
    results = list(
        pl.pallas_call(
            functools.partial(finish_kernel, cubes),
            out_shape=[jax.ShapeDtypeStruct(*shape) for shape in finals],
            in_specs=[vmem] * 13,
            out_specs=[vmem] * len(finals),
        )(
            *parts, w_query, w_key, w_value, w_gate, w_up, norm_attn[None], norm_mlp[None]
        )
    )
    results[2], results[7] = results[2][0], results[7][0]
    return tuple(results)


def solution(mesh):
    n = mesh.shape["fsdp"]
    rows, vec = P("fsdp", None), P("fsdp")
    per_device = per_device_fast if n == 4 * CUBE else per_device_any
    return jax.shard_map(
        functools.partial(per_device, n),
        mesh=mesh,
        in_specs=(rows, rows, rows, vec, rows, rows, rows, rows, vec, rows, rows, rows),
        out_specs=(rows, rows, vec, rows, rows, rows, rows, vec, rows, rows, rows),
        check_vma=False,
    )
```

```python
import functools
import math

import jax
import jax.numpy as jnp
from jax import lax
from jax.experimental import pallas as pl
from jax.experimental.pallas import tpu as pltpu
from jax.sharding import PartitionSpec as P

HEADS = 16
KV_HEADS = 8
HEAD = 96
LANES = 128
CUBE = 8
COLORS = 3

eps_norm = 1e-05
rope_theta = 100000.0
masked_score = -1e30
score_scale = 1.0 / math.sqrt(HEAD)


bf16 = jnp.bfloat16
f32 = jnp.float32


def rope_tables(slot_count):
    half_width = HEAD // 2
    exponent = jnp.arange(half_width, dtype=f32) * (2.0 / HEAD)
    inverse = jnp.exp(-math.log(rope_theta) * exponent)
    angles = jnp.arange(slot_count, dtype=jnp.int32).astype(f32)[:, None] * inverse[None, :]
    pad = jnp.zeros((slot_count, LANES - HEAD), f32)
    cosine_tab = jnp.concatenate([jnp.cos(angles), jnp.cos(angles), pad], axis=-1)
    sine_tab = jnp.concatenate([jnp.sin(angles), jnp.sin(angles), pad], axis=-1)
    return cosine_tab, sine_tab


def rms_parts(values):
    inverse_rms = lax.rsqrt(jnp.mean(values * values, axis=-1, keepdims=True) + eps_norm)
    return values * inverse_rms, inverse_rms


def rms_back(grad_normed, unit_rows, inverse_rms, gain_vec):
    scaled = grad_normed * gain_vec
    return inverse_rms * (scaled - unit_rows * jnp.mean(scaled * unit_rows, axis=-1, keepdims=True))


def contract_last(left_side, right_side):
    return lax.dot_general(
        left_side, right_side, (((1,), (1,)), ((), ())), preferred_element_type=f32
    )


def contract_first(left_side, right_side):
    return lax.dot_general(
        left_side, right_side, (((0,), (0,)), ((), ())), preferred_element_type=f32
    )


def matmul(left_side, right_side):
    return jnp.dot(left_side, right_side, preferred_element_type=f32)


def _rot_half(t, lane):
    return jnp.where(
        lane < HEAD // 2, -pltpu.roll(t, LANES - HEAD // 2, 1), pltpu.roll(t, HEAD // 2, 1)
    )


def _rope(t, cos, sin, lane):
    return t * cos + _rot_half(t, lane) * sin


def _unrope(t, cos, sin, lane):
    return t * cos - _rot_half(t, lane) * sin


def _wide(v):
    return jnp.concatenate([v, jnp.zeros_like(v)], axis=1)


def _weights(q, k, visible, live):
    scores = jnp.where(visible, contract_last(q, k) * score_scale, masked_score)
    exponent = jnp.exp(scores - jnp.max(scores, axis=-1, keepdims=True))
    return jnp.where(live, exponent / jnp.sum(exponent, axis=-1, keepdims=True), 0.0)


def _masks(length, slots):
    row = lax.broadcasted_iota(jnp.int32, (slots, slots), 0)
    col = lax.broadcasted_iota(jnp.int32, (slots, slots), 1)
    live = row < length
    return (col <= row) & live & (col < length), live


def attend_kernel(len_ref, qkv_ref, cos_ref, sin_ref, o_ref):
    length = len_ref[pl.program_id(0)]
    slots = qkv_ref.shape[0]
    visible, live = _masks(length, slots)
    lane = lax.broadcasted_iota(jnp.int32, (slots, LANES), 1)
    cos, sin = cos_ref[...], sin_ref[...]
    k = _rope(qkv_ref[:, 2 * LANES : 3 * LANES], cos, sin, lane).astype(bf16)
    v = qkv_ref[:, 3 * LANES :]
    v_wide = _wide(v)
    mixed = None
    for h in range(2):
        q = _rope(qkv_ref[:, h * LANES : (h + 1) * LANES], cos, sin, lane).astype(bf16)
        weights = _weights(q, k, visible, live).astype(bf16)
        v_h = v_wide if h == 0 else pltpu.roll(v_wide, HEAD, 1)
        part = matmul(weights, v_h.astype(bf16))
        mixed = part if mixed is None else mixed + part
    o_ref[...] = mixed.astype(bf16)


def attend_back_kernel(len_ref, qkv_ref, do_ref, cos_ref, sin_ref, out_ref):
    length = len_ref[pl.program_id(0)]
    slots = qkv_ref.shape[0]
    visible, live = _masks(length, slots)
    lane = lax.broadcasted_iota(jnp.int32, (slots, LANES), 1)
    cos, sin = cos_ref[...], sin_ref[...]
    k = _rope(qkv_ref[:, 2 * LANES : 3 * LANES], cos, sin, lane).astype(bf16)
    v_wide = _wide(qkv_ref[:, 3 * LANES :])
    d_o = do_ref[...]
    grad_k = grad_v = None
    for h in range(2):
        q = _rope(qkv_ref[:, h * LANES : (h + 1) * LANES], cos, sin, lane).astype(bf16)
        weights = _weights(q, k, visible, live)
        v_h = v_wide if h == 0 else pltpu.roll(v_wide, HEAD, 1)
        grad_weights = contract_last(d_o, v_h.astype(bf16))
        row_inner = jnp.sum(weights * grad_weights, axis=-1, keepdims=True)
        grad_scores = (weights * (grad_weights - row_inner)).astype(bf16)
        grad_q = matmul(grad_scores, k) * score_scale
        out_ref[:, h * LANES : (h + 1) * LANES] = _unrope(grad_q, cos, sin, lane).astype(bf16)
        part_k = contract_first(grad_scores, q) * score_scale
        part_v = contract_first(weights.astype(bf16), d_o)
        if h == 1:
            part_v = pltpu.roll(part_v, 2 * LANES - HEAD, 1)
        part_v = part_v[:, :LANES]
        grad_k = part_k if grad_k is None else grad_k + part_k
        grad_v = part_v if grad_v is None else grad_v + part_v
    out_ref[:, 2 * LANES : 3 * LANES] = _unrope(grad_k, cos, sin, lane).astype(bf16)
    out_ref[:, 3 * LANES :] = jnp.where(lane < HEAD, grad_v, 0.0).astype(bf16)


def attend(lengths, qkv, cos, sin):
    blocks, slots, width = qkv.shape
    table = pl.BlockSpec((slots, LANES), lambda s, ln: (0, 0))
    return pl.pallas_call(
        attend_kernel,
        out_shape=jax.ShapeDtypeStruct((blocks, slots, 2 * LANES), bf16),
        grid_spec=pltpu.PrefetchScalarGridSpec(
            num_scalar_prefetch=1,
            grid=(blocks,),
            in_specs=[pl.BlockSpec((None, slots, width), lambda s, ln: (s, 0, 0)), table, table],
            out_specs=pl.BlockSpec((None, slots, 2 * LANES), lambda s, ln: (s, 0, 0)),
        ),
        cost_estimate=pl.CostEstimate(
            flops=blocks * 8 * slots * slots * LANES, bytes_accessed=blocks * slots * width * 6,
            transcendentals=blocks * 2 * slots * slots,
        ),
    )(lengths, qkv, cos, sin)


def attend_back(lengths, qkv, d_o, cos, sin):
    blocks, slots, width = qkv.shape
    table = pl.BlockSpec((slots, LANES), lambda s, ln: (0, 0))
    return pl.pallas_call(
        attend_back_kernel,
        out_shape=jax.ShapeDtypeStruct((blocks, slots, width), bf16),
        grid_spec=pltpu.PrefetchScalarGridSpec(
            num_scalar_prefetch=1,
            grid=(blocks,),
            in_specs=[
                pl.BlockSpec((None, slots, width), lambda s, ln: (s, 0, 0)),
                pl.BlockSpec((None, slots, 2 * LANES), lambda s, ln: (s, 0, 0)),
                table,
                table,
            ],
            out_specs=pl.BlockSpec((None, slots, width), lambda s, ln: (s, 0, 0)),
        ),
        cost_estimate=pl.CostEstimate(
            flops=blocks * 24 * slots * slots * LANES, bytes_accessed=blocks * slots * width * 8,
            transcendentals=blocks * 2 * slots * slots,
        ),
    )(lengths, qkv, d_o, cos, sin)


GATHER_WIDTHS = (3, 4, 5)
SCATTER_WIDTHS = (5, 4, 3)
OUT_WIDTHS = (6, 4, 2)
LOW_WIDTHS = (3, 4, 5)


class Mail:
    def __init__(self, n, send_sems, recv_sems):
        self.me = lax.axis_index("fsdp")
        self.send_sems, self.recv_sems = send_sems, recv_sems
        self.count, self.open = 0, []
        self.peers = {bits: self._peer(bits) for bits in range(1, n)}

    def _peer(self, bits):
        device, bit = self.me, 1
        while bit <= bits:
            if bits & bit:
                device = device + bit * (1 - 2 * ((self.me // bit) % 2))
            bit *= 2
        return device

    def enter(self, bits_list, away, others):
        barrier = pltpu.get_barrier_semaphore()

        @pl.when(away)
        def _():
            for device in others:
                pl.semaphore_signal(
                    barrier, inc=1, device_id=(device,), device_id_type=pl.DeviceIdType.MESH
                )

        for bits in bits_list:
            pl.semaphore_signal(
                barrier,
                inc=1,
                device_id=(self.peers[bits],),
                device_id_type=pl.DeviceIdType.MESH,
            )

        @pl.when(away)
        def _():
            pl.semaphore_wait(barrier, len(bits_list) + len(others))

        @pl.when(jnp.logical_not(away))
        def _():
            pl.semaphore_wait(barrier, len(bits_list))

    def make(self, src, dst, bits):
        copy = pltpu.make_async_remote_copy(
            src_ref=src,
            dst_ref=dst,
            send_sem=self.send_sems.at[self.count],
            recv_sem=self.recv_sems.at[self.count],
            device_id=(self.peers[bits],),
            device_id_type=pl.DeviceIdType.MESH,
        )
        self.count += 1
        self.open.append(copy)
        return copy

    def send(self, src, dst, bits):
        copy = self.make(src, dst, bits)
        copy.start()
        return copy

    def sent(self, copies):
        for copy in copies:
            copy.wait_send()
            self.open = [other for other in self.open if other is not copy]


def take(copies):
    for copy in copies:
        copy.wait_recv()


def xor_place(t, s):
    total = 0
    for bit in (1, 2, 4):
        total = total + bit * (((t // bit) % 2 + (s // bit) % 2) % 2)
    return total


def entry(s):
    if isinstance(s, int):
        return {3: 4, 4: 3}.get(s, s)
    return s + (s // 3) % 2 * (1 - s // 4) - (s // 4) * (1 - (s % 4 + 3) // 4)


def color_bits(color):
    return [1 << ((color + i) % 3) for i in range(3)]


def columns(ref, widths):
    starts = [sum(widths[:color]) for color in range(COLORS)]
    return lambda s, color: ref.at[
        entry(s), :, pl.ds(starts[color] * LANES, widths[color] * LANES)
    ]


class Gather:
    def __init__(self, mail, piece, absolute=False):
        self.mail, self.copies, self.stages = mail, {}, [[], [], []]

        def make(stage, color, slot, bit):
            dst = piece(slot if absolute else slot ^ bit, color)
            self.copies[color, slot ^ bit] = mail.make(piece(slot, color), dst, 2 * bit)
            self.stages[stage].append(self.copies[color, slot ^ bit])

        for i in range(3):
            for color in range(COLORS):
                make(0, color, 0, color_bits(color)[i])
        for color in range(COLORS):
            b1, b2, b3 = color_bits(color)
            make(1, color, b1, b2)
            make(1, color, b1, b3)
            make(2, color, b2, b3)
            make(2, color, b1 ^ b2, b3)

    def start(self):
        for copy in self.stages[0]:
            copy.start()

    def forward(self, stage):
        for color in range(COLORS):
            b1, b2, b3 = color_bits(color)
            for slot in ((b1,), (b2, b1 ^ b2))[stage - 1]:
                self.copies[color, slot].wait_recv()
        for copy in self.stages[stage]:
            copy.start()

    def sent(self):
        self.mail.sent(self.copies.values())

    def near(self):
        for color in range(COLORS):
            self.copies[color, color_bits(color)[2]].wait_recv()

    def far(self, colors=range(COLORS)):
        for color in colors:
            b1, b2, b3 = color_bits(color)
            for slot in (b1 ^ b3, b2 ^ b3, 7):
                self.copies[color, slot].wait_recv()


class Scatter:
    def __init__(self, mail, piece, got):
        self.mail, self.piece, self.got, self.copies = mail, piece, got, {}
        for color in range(COLORS):
            for bit in color_bits(color):
                for s in self._stage(color, bit):
                    self.copies[color, s] = mail.make(piece(s, color), got(s, color), 2 * bit)

    def _stage(self, color, bit):
        b1, b2, b3 = color_bits(color)
        if bit == b1:
            return [s for s in range(CUBE) if s & b1]
        return [b2, b2 ^ b3] if bit == b2 else [b3]

    def start(self, entries):
        for s in entries:
            for color in range(COLORS):
                if s & color_bits(color)[0]:
                    self.copies[color, s].start()

    def _add(self, color, s, bit):
        self.copies[color, s].wait_recv()
        here = self.piece(s ^ bit, color)
        here[...] = (here[...].astype(f32) + self.got(s, color)[...].astype(f32)).astype(here.dtype)

    def second(self):
        for color in range(COLORS):
            b1, b2, b3 = color_bits(color)
            for s in (b2, b2 ^ b3):
                self._add(color, b1 ^ s, b1)
                self.copies[color, s].start()

    def third(self):
        for color in range(COLORS):
            b1, b2, b3 = color_bits(color)
            self._add(color, b1 ^ b3, b1)
            self._add(color, b2 ^ b3, b2)
            self.copies[color, b3].start()

    def total(self, color):
        value = self.piece(0, color)[...].astype(f32)
        for s in color_bits(color):
            self.copies[color, s].wait_recv()
            value = value + self.got(s, color)[...].astype(f32)
        return value

    def sent(self):
        self.mail.sent(self.copies.values())


def lanes_at(values, start, width):
    low = start // LANES * LANES
    high = min(values.shape[1], -(-(start + width) // LANES) * LANES)
    window = values[:, low:high]
    if start > low:
        window = pltpu.roll(window, (high - low) - (start - low), 1)
    return window


def spread(values, width, shift):
    missing = width - values.shape[1]
    if missing > 0:
        values = jnp.concatenate(
            [values, jnp.zeros((values.shape[0], missing), values.dtype)], axis=1
        )
    return pltpu.roll(values, shift, 1) if shift else values


def clear_from(values, lane_count):
    lane = lax.broadcasted_iota(jnp.int32, values.shape, 1)
    return jnp.where(lane < lane_count, values, 0.0)


def heads_of(qkv):
    return [lanes_at(qkv, HEAD * j, HEAD)[:, :LANES] for j in range(4)]


def block_masks(slots, length):
    row = lax.broadcasted_iota(jnp.int32, (slots, slots), 0)
    col = lax.broadcasted_iota(jnp.int32, (slots, slots), 1)
    live = row.astype(f32) < length
    return (col <= row) & live, live


def lane_value(values, index):
    lane = lax.broadcasted_iota(jnp.int32, values.shape, 1)
    return jnp.sum(jnp.where(lane == index, values, 0.0), axis=1, keepdims=True)


def layer_kernel(
    n, x_ref, g_in, len_ref, small_ref, wq_ref, wk_ref, wv_ref, wo_ref, wg_ref, wu_ref, wd_ref,
    cos_ref, sin_ref,
    out_ref, grad_in, gd_ref, gu_slots, qkv_slots, wo_slot,
    h1_all, qkv_all, mixed_all, resid, h2_all, wqkv, gains,
    wout, wgu, wdown, g_all, o_slots, hidden, dgu, dh2, got,
    gu_grad, gu_got, gu_send, gu_far, wd_part, wd_got, wd_send, wd_far, dqkv,
    send_sems, recv_sems, local_sems, owner_sems, core_ready, far_ready, near_ready,
):
    cubes = n // (2 * CUBE)
    mail = Mail(n, send_sems, recv_sems)
    me = mail.me
    core, place, cube = me % 2, (me // 2) % CUBE, me // (2 * CUBE)
    pz, py, px = place // 4, (place // 2) % 2, place % 2
    other_core, other = 1 - core, 1 - cube
    slots, width = x_ref.shape
    rows, down_rows = wo_ref.shape[0], wd_ref.shape[0]
    units = hidden.shape[2]
    far_bits = 2 * CUBE
    owner = 2 * cubes * place + 2 * cube + core
    summed_at = far_bits * ((me // 2) % cubes) + 2 * (me // (2 * cubes)) + core
    away = owner != me
    mail.enter([2 * s for s in range(1, CUBE)] + [1, far_bits], away, [owner, summed_at])

    def small_at(i, low):
        return got.at[i, pl.ds(low, small_ref.shape[0]), pl.ds(0, LANES)]

    def small_add(copy, i, low):
        copy.wait_recv()
        gains[...] += small_at(i, low)[...]

    small_core = mail.send(small_ref, small_at(0, 32), 1)
    gains[...] = small_ref[...]

    h1_all[0] = x_ref[...]
    local = [
        pltpu.make_async_copy(wd_ref, wdown.at[cube, core], local_sems.at[0]),
        pltpu.make_async_copy(wo_ref, wout.at[cube, pz, py, px, core], local_sems.at[1]),
    ]
    for copy in local:
        copy.start()

    query, key, value = (ref[...].astype(f32) for ref in (wq_ref, wk_ref, wv_ref))
    for t in range(CUBE):
        whole = 4 * HEAD
        parts = (
            spread(clear_from(lanes_at(query, 2 * HEAD * t, 2 * HEAD), 2 * HEAD), whole, 0)
            + spread(clear_from(lanes_at(key, HEAD * t, HEAD), HEAD), whole, 2 * HEAD)
            + spread(clear_from(lanes_at(value, HEAD * t, HEAD), HEAD), whole, 3 * HEAD)
        )
        qkv_slots[t] = parts.astype(bf16)
    wqkv[cube, place, core] = qkv_slots[place]
    pack_cps = [
        mail.send(qkv_slots.at[xor_place(place, s)], wqkv.at[cube, place, core], 2 * s)
        for s in range(1, CUBE)
    ]
    small_core.wait_recv()
    mail.sent([small_core])
    gains[...] += small_at(0, 32)[...]
    small_far = mail.send(gains, small_at(1, 32), far_bits)

    x_mail = Gather(mail, columns(h1_all, GATHER_WIDTHS))
    x_mail.start()

    for t in range(CUBE):
        for i in range(2 * cubes):
            start = (((i // 2) * CUBE + t) * 2 + i % 2) * down_rows
            cols = slice(start, start + down_rows)
            gu_send[t // 4, t % 4, :, i * down_rows : (i + 1) * down_rows] = wg_ref[:, cols]
            gu_send[t // 4, t % 4, :, units + i * down_rows : units + (i + 1) * down_rows] = wu_ref[:, cols]
    wgu[cube, place, core] = gu_send[place // 4, place % 4]
    row = lax.broadcasted_iota(jnp.int32, (slots, width), 0)
    g_all[0] = jnp.where(row < len_ref[0, 0], g_in[...].astype(f32), 0.0).astype(bf16)
    small_far.wait_recv()
    mail.sent([small_far])
    gains[...] += small_at(1, 32)[...]
    small_cps = [mail.send(gains, small_at(s - 1, 0), 2 * s) for s in range(1, CUBE)]
    take(pack_cps)
    mail.sent(pack_cps)
    pack_far = mail.send(wqkv.at[cube, :, core], wqkv.at[cube, :, core], far_bits)
    pack_core = [mail.send(wqkv.at[cube, :, core], wqkv.at[cube, :, core], 1)]
    x_mail.forward(1)
    wo_cps = mail.send(wo_ref, wout.at[cube, pz, py, px, core], far_bits)
    gu_cps = [
        mail.send(
            gu_send.at[xor_place(place, s) // 4, xor_place(place, s) % 4],
            wgu.at[cube, place, core],
            2 * s,
        )
        for s in range(1, CUBE)
    ]
    x_mail.forward(2)
    wd_out = mail.send(wd_ref, wdown.at[cube, core], far_bits)
    take(small_cps)
    mail.sent(small_cps)
    for s in range(1, CUBE):
        gains[...] += small_at(s - 1, 0)[...]
    local[1].wait()
    wo_cps.wait_recv()

    def wo_piece(s, color):
        at = [(p + (s >> i) % 2) % 2 for i, p in ((2, pz), (1, py), (0, px))]
        widths = GATHER_WIDTHS
        start = sum(widths[:color])
        return wout.at[
            :, at[0], at[1], at[2], core, :, pl.ds(start * LANES, widths[color] * LANES)
        ]

    wo_mail = Gather(mail, wo_piece, absolute=True)
    pack_far.wait_recv()
    pack_core.append(mail.send(wqkv.at[other, :, core], wqkv.at[other, :, core], 1))
    x_mail.near()
    x_mail.far()
    wo_mail.start()
    g_mail = Gather(mail, columns(g_all, GATHER_WIDTHS))
    g_mail.start()
    take(pack_core)
    x_mail.sent()

    def row_of(first):
        return jnp.concatenate([gains[first + i : first + i + 1, :] for i in range(width // LANES)], axis=1)

    gain_attn, gain_mlp = row_of(0), row_of(width // LANES)
    lengths = gains[2 * (width // LANES) : 2 * (width // LANES) + 1, :]
    gu_out = mail.make(wgu.at[cube, :, core], wgu.at[cube, :, core], far_bits)

    def attention(s, carry):
        values = h1_all[s].astype(f32)
        normed = (rms_parts(values)[0] * gain_attn).astype(bf16)
        h1_all[s] = normed
        projected = heads_of(matmul(normed, wqkv[...].reshape(width, 4 * HEAD)))
        there = far_bits * cube + 2 * xor_place(place, entry(s)) + core
        visible, live = block_masks(slots, lane_value(lengths, there))
        lane = lax.broadcasted_iota(jnp.int32, (slots, LANES), 1)
        cos, sin = cos_ref[...], sin_ref[...]
        for j in range(3):
            qkv_all[s, :, j * LANES : (j + 1) * LANES] = _rope(projected[j], cos, sin, lane).astype(bf16)
        value = clear_from(projected[3], HEAD)
        qkv_all[s, :, 3 * LANES :] = value.astype(bf16)
        k = qkv_all[s, :, 2 * LANES : 3 * LANES]
        v_wide = _wide(value)
        mixed = None
        for h in range(2):
            q = qkv_all[s, :, h * LANES : (h + 1) * LANES]
            weights = _weights(q, k, visible, live).astype(bf16)
            v_h = pltpu.roll(v_wide, HEAD, 1) if h else v_wide
            part = matmul(weights, v_h.astype(bf16))
            mixed = part if mixed is None else mixed + part
        mixed_all[s] = mixed.astype(bf16)

        @pl.when(s == 4)
        def _():
            take(gu_cps)
            gu_out.start()

        @pl.when(s == 6)
        def _():
            wo_mail.forward(1)

        return carry

    lax.fori_loop(0, CUBE, attention, 0)

    o_cps = [mail.send(mixed_all.at[entry(s)], o_slots.at[place], 2 * s) for s in range(1, CUBE)]
    o_slots[place] = mixed_all[0]
    wo_mail.forward(2)
    local[0].wait()
    wd_out.wait_recv()
    wd_core = mail.send(wdown.at[:, core], wdown.at[:, core], 1)
    take(o_cps)
    g_mail.forward(1)
    wide = []
    for j in range(CUBE // 2):
        low = spread(o_slots[2 * j].astype(f32), 3 * LANES, 0)
        high = spread(o_slots[2 * j + 1].astype(f32), 3 * LANES, 2 * HEAD)
        wide.append((low + high).astype(bf16))
    attended = jnp.concatenate(wide, axis=1)
    wo_mail.near()
    wo_c = []
    for color in range(COLORS):
        wo_mail.far([color])
        start = sum(GATHER_WIDTHS[:color])
        part = wout.at[
            :, :, :, :, core, :, pl.ds(start * LANES, GATHER_WIDTHS[color] * LANES)
        ]
        wo_c.append(mail.send(part, part, 1))
    take(wo_c)
    step = 256
    for j in range(width // step):
        cols = slice(j * step, (j + 1) * step)
        weight = wout[:, :, :, :, :, :, cols].reshape(width, step)
        resid[:, cols] = x_ref[:, cols].astype(f32) + matmul(attended, weight)
    h2_all[0] = (rms_parts(resid[...])[0] * gain_mlp).astype(bf16)
    h2_mail = Gather(mail, columns(h2_all, GATHER_WIDTHS))
    h2_mail.start()
    g_mail.forward(2)
    h2_mail.forward(1)
    gu_out.wait_recv()
    gu_core = mail.send(wgu.at[:, :, core], wgu.at[:, :, core], 1)
    h2_mail.forward(2)
    wd_core.wait_recv()
    gu_core.wait_recv()
    g_mail.near()
    h2_mail.near()

    got_columns = columns(got, SCATTER_WIDTHS)
    back = Scatter(
        mail, columns(dh2, SCATTER_WIDTHS), lambda s, color: got_columns(entry(s - 1), color)
    )

    def feed_forward(half):
        step = 256
        tokens = CUBE // 2 * slots
        here = slice(half * CUBE // 2, (half + 1) * CUBE // 2)

        def split(values):
            return values.reshape(CUBE // 2, slots, values.shape[1])

        for j in range(units // step):
            cols = slice(j * step, (j + 1) * step)
            up_cols = slice(units + j * step, units + (j + 1) * step)
            lhs = h2_all[here].reshape(tokens, width)
            gate = matmul(lhs, wgu[:, :, :, :, cols].reshape(width, step))
            up = matmul(lhs, wgu[:, :, :, :, up_cols].reshape(width, step))
            down = wdown[...].reshape(units, width)[cols]
            grad_hidden = contract_last(g_all[here].reshape(tokens, width), down)
            sigmoid_gate = jax.nn.sigmoid(gate)
            silu = gate * sigmoid_gate
            hidden[here, :, cols] = split((silu * up).astype(bf16))
            dgu[here, :, cols] = split(
                (grad_hidden * up * sigmoid_gate * (1.0 + gate * (1.0 - sigmoid_gate))).astype(bf16)
            )
            dgu[here, :, up_cols] = split((grad_hidden * silu).astype(bf16))
        for j in range(4):
            part = width // 4
            weight = wgu[j // 2, (j % 2) * (CUBE // 2) : (j % 2 + 1) * (CUBE // 2)]
            grad = contract_last(
                dgu[here].reshape(tokens, 2 * units), weight.reshape(part, 2 * units)
            )
            dh2[here, :, j * part : (j + 1) * part] = split(grad)
        back.start([entry(i) for i in range(half * CUBE // 2, (half + 1) * CUBE // 2)])

    feed_forward(0)
    g_mail.far()
    h2_mail.far()
    feed_forward(1)

    g_mail.sent()
    h2_mail.sent()
    wo_mail.sent()
    mail.sent([wo_cps, *wo_c])
    d_all = dgu[...].reshape(CUBE * slots, 2 * units)
    chunk = width // 4
    for j in range(4):
        lhs = h2_all[:, :, j * chunk : (j + 1) * chunk].reshape(CUBE * slots, chunk)
        gu_grad[j // 2, j % 2] = contract_first(lhs, d_all).reshape(gu_grad.shape[2:])
    gu_own_cps = gu_cps
    gu_cps = gu_core_cps = mail.send(gu_grad.at[:, :, :, other_core], gu_got, 1)
    hid_all = hidden[...].reshape(CUBE * slots, units)
    for j in range(4):
        cols = slice(j * chunk, (j + 1) * chunk)
        g_cols = g_all[:, :, cols].reshape(CUBE * slots, chunk)
        wd_part[:, :, :, cols] = contract_first(hid_all, g_cols).reshape(cubes, 2, down_rows, chunk)
    wd_cps = wd_core_cps = mail.send(wd_part.at[:, other_core], wd_got, 1)
    for i in range(2):
        half = slice(i * CUBE // 2, (i + 1) * CUBE // 2)
        lhs = hidden[half].reshape(CUBE // 2 * slots, units)
        for j in range(4):
            cols = slice(j * chunk, (j + 1) * chunk)
            part = matmul(lhs, wdown[:, :, :, cols].reshape(units, chunk))
            h2_all[half, :, cols] = part.reshape(CUBE // 2, slots, chunk).astype(bf16)
    gu_cps.wait_recv()
    mail.sent(gu_own_cps)
    gu_send[...] = (gu_grad[other, :, :, core] + gu_got[other]).astype(bf16)
    gu_cps = gu_far_cps = mail.send(gu_send, gu_far, far_bits)
    wd_cps.wait_recv()
    wd_send[...] = (wd_part[other, core] + wd_got[other]).astype(bf16)
    wd_cps = wd_far_cps = mail.send(wd_send, wd_far, far_bits)

    def out_got(s, color):
        if color == 1:
            return hidden.at[entry(s)]
        start, part = ((0, 768), None, (768, 256))[color]
        return dgu.at[entry(s), :, pl.ds(start, part)]

    out_piece = columns(h2_all, OUT_WIDTHS)
    out_mail = Scatter(mail, out_piece, out_got)
    for bit in (1, 2, 4):
        pl.semaphore_signal(
            near_ready,
            inc=1,
            device_id=(mail.peers[2 * bit],),
            device_id_type=pl.DeviceIdType.MESH,
        )
    back.second()
    pl.semaphore_wait(near_ready, 3)
    out_mail.start(range(CUBE))
    back.third()

    unit, inverse = rms_parts(resid[...])
    for color in range(COLORS):
        columns(dh2, SCATTER_WIDTHS)(0, color)[...] = back.total(color)
    grad_in[...] = g_all[0].astype(f32) + rms_back(dh2[0], unit, inverse, gain_mlp)
    low = grad_in[...].astype(bf16)
    g_all[0] = low
    for t in range(CUBE):
        weight = wout[t // 4, (t // 2) % 2, t % 2].reshape(2 * HEAD, width)
        dqkv[t, :, : 2 * LANES] = spread(contract_last(low, weight), 2 * LANES, 0).astype(bf16)
    do_cps = [
        mail.send(dqkv.at[xor_place(place, s), :, pl.ds(0, 2 * LANES)], o_slots.at[entry(s)], 2 * s)
        for s in range(1, CUBE)
    ]
    o_slots[0] = dqkv[place, :, : 2 * LANES]
    out_mail.second()

    gu_cps.wait_recv()
    mail.sent([gu_far_cps])
    gu_send[...] = (
        gu_grad[cube, :, :, core] + gu_got[cube] + gu_far[...].astype(f32)
    ).astype(bf16)
    wd_cps.wait_recv()
    gd_ref[...] = wd_part[cube, core] + wd_got[cube] + wd_far[...].astype(f32)
    for ready, bits in ((core_ready, 1), (far_ready, far_bits)):
        pl.semaphore_signal(
            ready, inc=1, device_id=(mail.peers[bits],), device_id_type=pl.DeviceIdType.MESH
        )
    gu_cps = [
        mail.send(
            gu_send.at[xor_place(place, s) // 4, xor_place(place, s) % 4], gu_slots.at[place], 2 * s
        )
        for s in range(1, CUBE)
    ]
    gu_slots[place] = gu_send[place // 4, place % 4]
    take(do_cps)
    mail.sent(do_cps)
    low_mail = Gather(mail, columns(g_all, LOW_WIDTHS))
    low_mail.start()

    def attention_back(s, carry):
        there = far_bits * cube + 2 * xor_place(place, entry(s)) + core
        visible, live = block_masks(slots, lane_value(lengths, there))
        lane = lax.broadcasted_iota(jnp.int32, (slots, LANES), 1)
        cos, sin = cos_ref[...], sin_ref[...]
        k = qkv_all[s, :, 2 * LANES : 3 * LANES]
        v_wide = _wide(qkv_all[s, :, 3 * LANES :].astype(f32))
        grad_o = o_slots[s]
        grad_k = grad_v = total = None
        for h in range(2):
            q = qkv_all[s, :, h * LANES : (h + 1) * LANES]
            weights = _weights(q, k, visible, live)
            v_h = pltpu.roll(v_wide, HEAD, 1) if h else v_wide
            grad_weights = contract_last(grad_o, v_h.astype(bf16))
            row_inner = jnp.sum(weights * grad_weights, axis=-1, keepdims=True)
            grad_scores = (weights * (grad_weights - row_inner)).astype(bf16)
            grad_q = _unrope(matmul(grad_scores, k) * score_scale, cos, sin, lane)
            part_k = contract_first(grad_scores, q) * score_scale
            part_v = contract_first(weights.astype(bf16), grad_o)
            if h:
                part_v = pltpu.roll(part_v, 2 * LANES - HEAD, 1)
            part_v = part_v[:, :LANES]
            grad_q = spread(grad_q, 4 * HEAD, h * HEAD)
            total = grad_q if total is None else total + grad_q
            grad_k = part_k if grad_k is None else grad_k + part_k
            grad_v = part_v if grad_v is None else grad_v + part_v
        total = total + spread(_unrope(grad_k, cos, sin, lane), 4 * HEAD, 2 * HEAD)
        total = total + spread(clear_from(grad_v, HEAD), 4 * HEAD, 3 * HEAD)
        dqkv[s] = total.astype(bf16)

        return carry

    lax.fori_loop(0, CUBE, attention_back, 0)
    out_mail.third()

    pl.semaphore_wait(core_ready, 1)
    mail.sent([gu_core_cps, wd_core_cps])
    qkv_all_grad = dqkv[...].reshape(CUBE * slots, 4 * HEAD)
    narrow = slice(0, 4 * HEAD)
    for j in range(4):
        lhs = h1_all[:, :, j * chunk : (j + 1) * chunk].reshape(CUBE * slots, chunk)
        gu_grad[j // 2, j % 2, :, :, :, narrow] = contract_first(lhs, qkv_all_grad).reshape(
            CUBE // 2, 2, rows, 4 * HEAD
        )
    qkv_cps = mail.send(
        gu_grad.at[:, :, :, other_core, :, narrow], gu_got.at[:, :, :, :, narrow], 1
    )
    for i in range(2):
        half = slice(i * CUBE // 2, (i + 1) * CUBE // 2)
        lhs = dqkv[half].reshape(CUBE // 2 * slots, 4 * HEAD)
        for j in range(2):
            part = width // 2
            grad = contract_last(lhs, wqkv[j].reshape(part, 4 * HEAD))
            h1_all[half, :, j * part : (j + 1) * part] = grad.reshape(
                CUBE // 2, slots, part
            ).astype(bf16)

    cuts = (0, 48, 96, slots)

    def in_piece(s, color):
        return h1_all.at[entry(s), pl.ds(cuts[color], cuts[color + 1] - cuts[color])]

    def in_got(s, color):
        i = COLORS * s + color
        slot = wout.at[i // 16, (i // 8) % 2, (i // 4) % 2, (i // 2) % 2, i % 2]
        return slot.at[pl.ds(0, cuts[color + 1] - cuts[color])]

    in_mail = Scatter(mail, in_piece, in_got)
    in_mail.start(range(CUBE))
    qkv_cps.wait_recv()
    pl.semaphore_wait(far_ready, 1)
    mail.sent([*gu_cps, wd_far_cps])
    gu_send[:, :, :, narrow] = (
        gu_grad[other, :, :, core, :, narrow] + gu_got[other, :, :, :, narrow]
    ).astype(bf16)
    qkv_cps = mail.send(
        gu_send.at[:, :, :, narrow], gu_far.at[:, :, :, narrow], far_bits
    )
    low_mail.forward(1)
    low_mail.forward(2)
    in_mail.second()

    low_mail.near()
    low_mail.far()
    mixed = mixed_all[...].reshape(CUBE * slots, 2 * LANES)
    for j in range(4):
        cols = slice(j * chunk, (j + 1) * chunk)
        g_cols = g_all[:, :, cols].reshape(CUBE * slots, chunk)
        wd_part[:, :, :rows, cols] = contract_first(mixed, g_cols)[: 2 * HEAD].reshape(
            cubes, 2, rows, chunk
        )
    wo_cps = mail.send(wd_part.at[:, other_core, pl.ds(0, rows)], wd_got.at[:, pl.ds(0, rows)], 1)
    wo_cps.wait_recv()
    wd_send[:rows] = (wd_part[other, core, :rows] + wd_got[other, :rows]).astype(bf16)
    wo_cps = mail.send(wd_send.at[pl.ds(0, rows)], wd_far.at[pl.ds(0, rows)], far_bits)
    qkv_cps.wait_recv()
    gu_far[:, :, :, narrow] = (
        gu_grad[cube, :, :, core, :, narrow]
        + gu_got[cube, :, :, :, narrow]
        + gu_far[:, :, :, narrow].astype(f32)
    ).astype(bf16)
    qkv_cps = [
        mail.send(
            gu_far.at[xor_place(place, s) // 4, xor_place(place, s) % 4, :, narrow],
            qkv_slots.at[place],
            2 * s,
        )
        for s in range(1, CUBE)
    ]
    qkv_slots[place] = gu_far[place // 4, place % 4, :, narrow]
    in_mail.third()
    wo_cps.wait_recv()
    wd_far[:rows] = (
        wd_part[cube, core, :rows] + wd_got[cube, :rows] + wd_far[:rows].astype(f32)
    ).astype(bf16)
    wo_copy = pltpu.make_async_remote_copy(
        src_ref=wd_far.at[pl.ds(0, rows)],
        dst_ref=wo_slot,
        send_sem=owner_sems.at[0],
        recv_sem=owner_sems.at[1],
        device_id=(owner,),
        device_id_type=pl.DeviceIdType.MESH,
    )

    @pl.when(away)
    def _():
        wo_copy.start()

    @pl.when(owner == me)
    def _():
        wo_slot[...] = wd_far[:rows]

    take(gu_cps)
    take(qkv_cps)

    @pl.when(away)
    def _():
        wo_copy.wait_recv()
        wo_copy.wait_send()

    unit, inverse = rms_parts(x_ref[...].astype(f32))
    for color in range(COLORS):
        dh2[0, cuts[color] : cuts[color + 1]] = in_mail.total(color)
    grad_in[...] += rms_back(dh2[0], unit, inverse, gain_attn)
    for color in range(COLORS):
        low = sum(OUT_WIDTHS[:color]) * LANES
        here = slice(low, low + OUT_WIDTHS[color] * LANES)
        out_ref[:, here] = (resid[:, here] + out_mail.total(color)).astype(bf16)
    mail.sent(mail.open)


def finish_kernel(
    cubes, out_in, grad_in, gd_in, gu_slots, qkv_slots, wo_slot, wq_ref, wk_ref, wv_ref, wg_ref,
    wu_ref, norm_attn_ref, norm_mlp_ref,
    out_ref, grad_ref, attn_ref, gq_ref, gk_ref, gv_ref, go_ref, mlp_ref, gg_ref, gup_ref, gd_ref,
):
    rows, units = wg_ref.shape[0], gu_slots.shape[2] // 2
    down_rows = units // (2 * cubes)
    out_ref[...] = out_in[...]
    grad_ref[...] = grad_in[...]
    gd_ref[...] = gd_in[...]
    go_ref[...] = wo_slot[...].astype(f32)
    for t in range(CUBE):
        for i in range(2 * cubes):
            start = (((i // 2) * CUBE + t) * 2 + i % 2) * down_rows
            cols = slice(start, start + down_rows)
            gg_ref[:, cols] = gu_slots[t, :, i * down_rows : (i + 1) * down_rows].astype(f32)
            gup_ref[:, cols] = gu_slots[
                t, :, units + i * down_rows : units + (i + 1) * down_rows
            ].astype(f32)
    whole = 4 * HEAD
    for j in range(CUBE // 2):
        pair = [qkv_slots[2 * j + i].astype(f32) for i in range(2)]
        gq_ref[:, j * whole : (j + 1) * whole] = sum(
            spread(clear_from(values, 2 * HEAD), whole, 2 * HEAD * i)
            for i, values in enumerate(pair)
        )
    for j in range(2):
        four = [qkv_slots[4 * j + i].astype(f32) for i in range(4)]
        for ref, start in ((gk_ref, 2 * HEAD), (gv_ref, 3 * HEAD)):
            ref[:, j * whole : (j + 1) * whole] = sum(
                spread(clear_from(lanes_at(values, start, HEAD), HEAD), whole, HEAD * i)
                for i, values in enumerate(four)
            )

    diagonal = lax.broadcasted_iota(jnp.int32, (rows, rows), 0) == lax.broadcasted_iota(
        jnp.int32, (rows, rows), 1
    )

    def gain_grad(pairs, norm_ref):
        total = sum(
            jnp.sum(weight[...].astype(f32) * grad[...], axis=1, keepdims=True)
            for weight, grad in pairs
        )
        row = jnp.sum(jnp.where(diagonal, total, 0.0), axis=0, keepdims=True)
        return row / norm_ref[...].astype(f32)

    attn_ref[...] = gain_grad(
        ((wq_ref, gq_ref), (wk_ref, gk_ref), (wv_ref, gv_ref)), norm_attn_ref
    )
    mlp_ref[...] = gain_grad(((wg_ref, gg_ref), (wu_ref, gup_ref)), norm_mlp_ref)


def per_device_any(
    n,
    layer_input,
    out_cotangent,
    lengths,
    norm_attn,
    w_query,
    w_key,
    w_value,
    w_out,
    norm_mlp,
    w_gate,
    w_up,
    w_down,
):
    cubes = n // (2 * CUBE)
    slots, width = layer_input.shape
    rows = w_query.shape[0]
    down_rows = w_down.shape[0]
    q_cols, kv_cols = w_query.shape[1] // CUBE, w_key.shape[1] // CUBE
    me = lax.axis_index("fsdp")
    core, place, cube = me % 2, (me // 2) % CUBE, me // (2 * CUBE)

    def swap(array, bits):
        return lax.ppermute(array, "fsdp", [(i, i ^ bits) for i in range(n)])

    def cube_gather(block):
        part = block.shape[1] // COLORS
        columns = []
        for color in range(COLORS):
            order = [(color + i) % 3 for i in range(3)]
            held, names = block[None, :, color * part : (color + 1) * part], [0]
            for bit in order:
                held = jnp.concatenate([held, swap(held, 2 << bit)], axis=0)
                names = names + [name ^ (1 << bit) for name in names]
            columns.append((held, names))
        return jnp.stack(
            [
                jnp.concatenate([held[names.index(s)] for held, names in columns], axis=1)
                for s in range(CUBE)
            ]
        )

    def cube_scatter(blocks):
        part = blocks.shape[2] // COLORS
        columns = []
        for color in range(COLORS):
            order = [(color + i) % 3 for i in range(3)]
            held = {s: blocks[s, :, color * part : (color + 1) * part] for s in range(CUBE)}
            for bit in order:
                send = [s for s in held if s & (1 << bit)]
                got = swap(jnp.stack([held[s] for s in send]), 2 << bit)
                for i, s in enumerate(send):
                    held[s ^ (1 << bit)] = held[s ^ (1 << bit)] + got[i]
                    del held[s]
            columns.append(held[0])
        return jnp.concatenate(columns, axis=1)

    def cube_exchange(blocks):
        return jnp.stack([blocks[0]] + [swap(blocks[s], 2 * s) for s in range(1, CUBE)])

    relative = jnp.arange(CUBE, dtype=jnp.int32) ^ place

    def by_place(blocks):
        return jnp.take(blocks, relative, axis=0, indices_are_sorted=False, unique_indices=True)

    def group_gather(block):
        held = jnp.stack([block] + [swap(block, 2 * CUBE * s) for s in range(1, cubes)])
        return jnp.stack([held, swap(held, 1)])

    owner = jnp.arange(n, dtype=jnp.int32)
    from_me = owner ^ me
    owner_entry = ((from_me % 2) * cubes + from_me // (2 * CUBE)) * CUBE + (from_me // 2) % CUBE
    pair = jnp.arange(2 * cubes, dtype=jnp.int32)
    pair_entry = ((pair % 2) ^ core) * cubes + ((pair // 2) ^ cube)

    def all_rows(block):
        held = group_gather(block).reshape(n, *block.shape[1:])
        return jnp.take(held, owner_entry, axis=0, unique_indices=True)

    small = jnp.concatenate(
        [norm_attn, norm_mlp, lengths[0].astype(bf16), jnp.zeros((LANES - 2 * rows - 1,), bf16)]
    )[None]
    bit = 1
    while bit < n:
        small = jnp.concatenate([small, swap(small, bit)], axis=0)
        bit *= 2
    cube_lengths = small[0 : 2 * CUBE : 2, 2 * rows].astype(jnp.int32)
    gains = jnp.take(small, from_me, axis=0)
    gain_attn = gains[:, :rows].reshape(width).astype(f32)
    gain_mlp = gains[:, rows : 2 * rows].reshape(width).astype(f32)
    cos, sin = rope_tables(slots)

    x_all = cube_gather(layer_input)
    own_qkv = jnp.concatenate(
        [
            w_query.reshape(rows, CUBE, q_cols),
            w_key.reshape(rows, CUBE, kv_cols),
            w_value.reshape(rows, CUBE, kv_cols),
        ],
        axis=2,
    ).transpose(1, 0, 2)
    w_qkv = all_rows(cube_exchange(by_place(own_qkv))).reshape(width, q_cols + 2 * kv_cols)
    w_qkv = jnp.pad(
        w_qkv.reshape(width, 4, HEAD), ((0, 0), (0, 0), (0, LANES - HEAD))
    ).reshape(width, 4 * LANES)

    out_held = jnp.stack([w_out] + [swap(w_out, 2 * CUBE * s) for s in range(1, cubes)])
    out_held = out_held.reshape(1, cubes, rows, width)
    for bit in range(3):
        out_held = jnp.concatenate([out_held, swap(out_held, 2 << bit)], axis=0)
    out_held = jnp.stack([out_held, swap(out_held, 1)])
    out_entry = ((from_me % 2) * CUBE + (from_me // 2) % CUBE) * cubes + from_me // (2 * CUBE)
    full_out = jnp.take(out_held.reshape(n, rows, width), out_entry, axis=0, unique_indices=True)
    full_out = jnp.pad(
        full_out.reshape(CUBE, q_cols, width), ((0, 0), (0, 2 * LANES - q_cols), (0, 0))
    ).reshape(CUBE * 2 * LANES, width)

    ff_cols = 2 * cubes * down_rows

    def by_hidden(weight):
        split = weight.reshape(rows, cubes, CUBE, 2, down_rows)
        return split.transpose(2, 0, 1, 3, 4).reshape(CUBE, rows, ff_cols)

    own_gate_up = jnp.concatenate([by_hidden(w_gate), by_hidden(w_up)], axis=2)
    w_gate_up = all_rows(cube_exchange(by_place(own_gate_up))).reshape(width, 2 * ff_cols)
    down_held = group_gather(w_down).reshape(2 * cubes, down_rows, width)
    down = jnp.take(down_held, pair_entry, axis=0, unique_indices=True).reshape(ff_cols, width)

    live = jnp.arange(slots, dtype=jnp.int32)[:, None] < lengths[0, 0]
    cotangent = jnp.where(live, out_cotangent, jnp.zeros_like(out_cotangent))
    g_all = cube_gather(cotangent).reshape(CUBE * slots, width)

    inputs = layer_input.astype(f32)
    unit_all, _ = rms_parts(x_all.reshape(CUBE * slots, width).astype(f32))
    normed_all = (unit_all * gain_attn).astype(bf16)
    qkv = matmul(normed_all, w_qkv).reshape(CUBE, slots, 4 * LANES)
    mixed = attend(cube_lengths, qkv, cos, sin)
    attended = by_place(cube_exchange(mixed)).transpose(1, 0, 2).reshape(slots, CUBE * 2 * LANES)
    residual = inputs + matmul(attended, full_out)
    unit_mlp, inv_mlp = rms_parts(residual)
    normed_mlp = cube_gather((unit_mlp * gain_mlp).astype(bf16)).reshape(CUBE * slots, width)

    gate_up = matmul(normed_mlp, w_gate_up)
    gate, up = gate_up[:, :ff_cols], gate_up[:, ff_cols:]
    sigmoid_gate = jax.nn.sigmoid(gate)
    hidden = (gate * sigmoid_gate * up).astype(bf16)
    grad_hidden = contract_last(g_all, down)
    grad_gate = (grad_hidden * up * sigmoid_gate * (1.0 + gate * (1.0 - sigmoid_gate))).astype(bf16)
    grad_up = (grad_hidden * gate * sigmoid_gate).astype(bf16)
    grad_gate_up = jnp.concatenate([grad_gate, grad_up], axis=1)
    grad_normed_mlp = cube_scatter(
        contract_last(grad_gate_up, w_gate_up).reshape(CUBE, slots, width)
    )
    grad_resid = cotangent.astype(f32) + rms_back(grad_normed_mlp, unit_mlp, inv_mlp, gain_mlp)
    grad_resid_low = grad_resid.astype(bf16)

    grad_attended = contract_last(grad_resid_low, full_out).astype(bf16)
    grad_blocks = by_place(grad_attended.reshape(slots, CUBE, 2 * LANES).transpose(1, 0, 2))
    grad_mixed = cube_exchange(grad_blocks)
    grad_qkv = attend_back(cube_lengths, qkv, grad_mixed, cos, sin).reshape(
        CUBE * slots, 4 * LANES
    )

    def low_sum(blocks):
        total = blocks[0]
        for s in range(1, CUBE):
            total = total + swap(blocks[s].astype(bf16), 2 * s).astype(f32)
        return total

    output = (
        residual + low_sum(matmul(hidden, down).reshape(CUBE, slots, width))
    ).astype(bf16)
    grad_normed = low_sum(contract_last(grad_qkv, w_qkv).reshape(CUBE, slots, width))
    unit_attn, inv_attn = rms_parts(inputs)
    grad_input = grad_resid + rms_back(grad_normed, unit_attn, inv_attn, gain_attn)

    def group_sum(blocks, core_axis):
        pick = functools.partial(
            lax.dynamic_index_in_dim, axis=core_axis + 1, keepdims=False
        )
        pair_total = pick(blocks, core) + swap(pick(blocks, 1 - core), 1)
        total = lax.dynamic_index_in_dim(pair_total, cube, axis=0, keepdims=False)
        for s in range(1, cubes):
            send = lax.dynamic_index_in_dim(pair_total, cube ^ s, axis=0, keepdims=False)
            total = total + swap(send.astype(bf16), 2 * CUBE * s).astype(f32)
        return total

    grad_down = group_sum(
        contract_first(hidden, g_all).reshape(cubes, 2, down_rows, width), 0
    )

    def to_owners(partial):
        cols = partial.shape[1]
        total = group_sum(partial.reshape(cubes, CUBE, 2, rows, cols), 1)
        return by_place(cube_exchange(by_place(total.astype(bf16)))).astype(f32)

    grad_gu = to_owners(contract_first(normed_mlp, grad_gate_up))

    def hidden_back(block):
        return block.reshape(CUBE, rows, cubes, 2, down_rows).transpose(1, 2, 0, 3, 4).reshape(
            rows, cubes * CUBE * 2 * down_rows
        )

    grad_w_gate, grad_w_up = hidden_back(grad_gu[:, :, :ff_cols]), hidden_back(grad_gu[:, :, ff_cols:])

    grad_w = to_owners(contract_first(normed_all, grad_qkv))
    grad_heads = grad_w.reshape(CUBE, rows, 4, LANES)[:, :, :, :HEAD].transpose(1, 2, 0, 3)
    grad_w_query = grad_heads[:, :2].transpose(0, 2, 1, 3).reshape(rows, CUBE * q_cols)
    grad_w_key = grad_heads[:, 2].reshape(rows, CUBE * kv_cols)
    grad_w_value = grad_heads[:, 3].reshape(rows, CUBE * kv_cols)

    resid_low_all = cube_gather(grad_resid_low).reshape(CUBE * slots, width)
    grad_out_part = contract_first(mixed.reshape(CUBE * slots, 2 * LANES), resid_low_all)[:q_cols]
    grad_out_sum = group_sum(grad_out_part.reshape(cubes, 2, rows, width), 0)
    moves = [
        (2 * CUBE * g + 2 * t + c, 2 * cubes * t + 2 * g + c)
        for g in range(cubes)
        for t in range(CUBE)
        for c in range(2)
    ]
    grad_w_out = lax.ppermute(grad_out_sum.astype(bf16), "fsdp", moves).astype(f32)

    def gain_grad(gain, pairs):
        total = sum(jnp.sum(weight.astype(f32) * grad, axis=1) for weight, grad in pairs)
        return total / gain.astype(f32)

    gain_attn_grad = gain_grad(
        norm_attn, [(w_query, grad_w_query), (w_key, grad_w_key), (w_value, grad_w_value)]
    )
    gain_mlp_grad = gain_grad(norm_mlp, [(w_gate, grad_w_gate), (w_up, grad_w_up)])
    return (
        output,
        grad_input,
        gain_attn_grad,
        grad_w_query,
        grad_w_key,
        grad_w_value,
        grad_w_out,
        gain_mlp_grad,
        grad_w_gate,
        grad_w_up,
        grad_down,
    )


def per_device_fast(
    n,
    layer_input,
    out_cotangent,
    lengths,
    norm_attn,
    w_query,
    w_key,
    w_value,
    w_out,
    norm_mlp,
    w_gate,
    w_up,
    w_down,
):
    cubes = n // (2 * CUBE)
    slots, width = layer_input.shape
    rows, down_rows = w_query.shape[0], w_down.shape[0]
    units, qkv_cols = 2 * cubes * down_rows, 4 * HEAD
    me = lax.axis_index("fsdp")
    own = jnp.arange(width, dtype=jnp.int32) // rows == me
    small = [jnp.where(own, jnp.tile(norm, n), 0).astype(f32) for norm in (norm_attn, norm_mlp)]
    small.append(jnp.where(jnp.arange(1024) == me, lengths[0], 0).astype(f32))
    small = jnp.concatenate(small).reshape(-1, LANES)
    cos, sin = rope_tables(slots)

    vmem = pl.BlockSpec(memory_space=pltpu.VMEM)
    smem = pl.BlockSpec(memory_space=pltpu.SMEM)
    hbm = pl.BlockSpec(memory_space=pl.ANY)
    outs = [
        ((slots, width), bf16),
        ((slots, width), f32),
        ((down_rows, width), f32),
        ((CUBE, rows, 2 * units), bf16),
        ((CUBE, rows, qkv_cols), bf16),
        ((rows, width), bf16),
    ]
    half = (2, CUBE // 2, rows, 2 * units)
    scratch = [
        ((CUBE, slots, width), bf16),
        ((CUBE, slots, 4 * LANES), bf16),
        ((CUBE, slots, 2 * LANES), bf16),
        ((slots, width), f32),
        ((CUBE, slots, width), bf16),
        ((cubes, CUBE, 2, rows, qkv_cols), bf16),
        ((2 * width // LANES + 8, LANES), f32),
        ((cubes, 2, 2, 2, 2, rows, width), bf16),
        ((cubes, CUBE, 2, rows, 2 * units), bf16),
        ((cubes, 2, down_rows, width), bf16),
        ((CUBE, slots, width), bf16),
        ((CUBE, slots, 2 * LANES), bf16),
        ((CUBE, slots, units), bf16),
        ((CUBE, slots, 2 * units), bf16),
        ((CUBE, slots, width), f32),
        ((CUBE - 1, slots, width), f32),
        ((cubes, 2, CUBE // 2, 2, rows, 2 * units), f32),
        ((cubes,) + half, f32),
        (half, bf16),
        (half, bf16),
        ((cubes, 2, down_rows, width), f32),
        ((cubes, down_rows, width), f32),
        ((down_rows, width), bf16),
        ((down_rows, width), bf16),
        ((CUBE, slots, qkv_cols), bf16),
    ]
    messages = 256
    parts = pl.pallas_call(
        functools.partial(layer_kernel, n),
        out_shape=[jax.ShapeDtypeStruct(*shape) for shape in outs],
        in_specs=[vmem, vmem, smem, vmem, vmem, vmem, vmem, hbm, vmem, vmem, hbm, vmem, vmem],
        out_specs=[vmem] * len(outs),
        scratch_shapes=[pltpu.VMEM(*shape) for shape in scratch]
        + [
            pltpu.SemaphoreType.DMA((messages,)),
            pltpu.SemaphoreType.DMA((messages,)),
            pltpu.SemaphoreType.DMA((2,)),
            pltpu.SemaphoreType.DMA((2,)),
            pltpu.SemaphoreType.REGULAR,
            pltpu.SemaphoreType.REGULAR,
            pltpu.SemaphoreType.REGULAR,
        ],
        compiler_params=pltpu.CompilerParams(
            collective_id=0, has_side_effects=True, vmem_limit_bytes=67043328
        ),
    )(
        layer_input, out_cotangent, lengths, small, w_query, w_key, w_value, w_out, w_gate, w_up,
        w_down, cos, sin,
    )
    finals = [
        ((slots, width), bf16),
        ((slots, width), f32),
        ((1, rows), f32),
        (w_query.shape, f32),
        (w_key.shape, f32),
        (w_value.shape, f32),
        (w_out.shape, f32),
        ((1, rows), f32),
        (w_gate.shape, f32),
        (w_up.shape, f32),
        (w_down.shape, f32),
    ]
    results = list(
        pl.pallas_call(
            functools.partial(finish_kernel, cubes),
            out_shape=[jax.ShapeDtypeStruct(*shape) for shape in finals],
            in_specs=[vmem] * 13,
            out_specs=[vmem] * len(finals),
        )(
            *parts, w_query, w_key, w_value, w_gate, w_up, norm_attn[None], norm_mlp[None]
        )
    )
    results[2], results[7] = results[2][0], results[7][0]
    return tuple(results)


def solution(mesh):
    n = mesh.shape["fsdp"]
    rows, vec = P("fsdp", None), P("fsdp")
    per_device = per_device_fast if n == 4 * CUBE else per_device_any
    return jax.shard_map(
        functools.partial(per_device, n),
        mesh=mesh,
        in_specs=(rows, rows, rows, vec, rows, rows, rows, rows, vec, rows, rows, rows),
        out_specs=(rows, rows, vec, rows, rows, rows, rows, vec, rows, rows, rows),
        check_vma=False,
    )
```
